32 devices in a mesh: gx: 4 (over y, core), gy: 4 (over z), gz: 2 (over x).
Axes of the slice: x: 2, y: 2, z: 4, core: 2. Of those that a mesh axis runs over, the one named last changes fastest.
Arguments:
- residual: float32 [32, 128, 256], P('gx', 'gy', 'gz'), may hold values from -32 to 32
- direction: float32 [32, 128, 256], P('gx', 'gy', 'gz'), may hold values from -32 to 32
- diagonal: float32 [32, 128, 256], P('gx', 'gy', 'gz'), may hold values from 0.5 to 2
- recycled: bfloat16 [16, 32, 128, 256], P(None, 'gx', 'gy', 'gz'), may hold values from -6 to 6
- recycled_images: bfloat16 [16, 32, 128, 256], P(None, 'gx', 'gy', 'gz'), may hold values from -0.0014648438 to 0.0014648438
- coupling_inverse: float32 [16, 16], replicated, may hold values from -1 to 3, as said below
Outputs:
- solution_delta: float32 [32, 128, 256], P('gx', 'gy', 'gz')
- new_residual: float32 [32, 128, 256], P('gx', 'gy', 'gz')
- new_direction: float32 [32, 128, 256], P('gx', 'gy', 'gz')
The draws below stay inside these ranges and needn't reach their ends.
Inputs may be any that keep to these rules, and one draw needn't show every extreme that they name: `coupling_inverse`: symmetric.
All inputs are finite; a program needn't handle non-finite values.
Results may differ from the reference program's by a relative error of at most 0.0028.
Values sent between devices are 32-bit elements; how exact they have to be, the bound alone decides.
No kernel may reach another device: no remote copies, remote signals or barrier semaphores. Data moves between devices by JAX's collectives and lax.ppermute only.
A program may use at most 64 MiB of HBM per device.

```python
import jax
import jax.numpy as jnp
import numpy as np
from jax import lax

S = 4
RECYCLED = 16
BASIS = 9
NX = 32
NY = 128
NZ = 256


def position_scale():
    along_x = 1.0 + 2.0 * jnp.arange(NX, dtype=jnp.float32) / NX
    along_y = 1.0 + 2.0 * jnp.arange(NY, dtype=jnp.float32) / NY
    along_z = 1.0 + 2.0 * jnp.arange(NZ, dtype=jnp.float32) / NZ
    return jnp.sqrt(along_x[:, None, None] * along_y[None, :, None] * along_z[None, None, :])


def field_draw(key, salt):
    subkey = jax.random.fold_in(key, salt)
    values = jnp.clip(jax.random.normal(subkey, (NX, NY, NZ), jnp.float32), -6.0, 6.0)
    return values * position_scale()


def draw_residual(key, part):
    return field_draw(key, 101)


def draw_direction(key, part):
    return field_draw(key, 202)


def draw_coupling_inverse(key, part):
    first_key = jax.random.fold_in(key, 303)
    second_key = jax.random.fold_in(key, 404)
    leading = jax.random.uniform(first_key, (RECYCLED,), jnp.float32, 0.5, 2.0)
    spread = jnp.clip(jax.random.normal(second_key, (RECYCLED, RECYCLED), jnp.float32), -3.0, 3.0) * 0.08
    return jnp.diag(leading) + spread + spread.T


def block_levels(own_key, extent, cuts, least, high):
    def one(axis_at, blocks):
        steps = jax.random.uniform(jax.random.fold_in(jax.random.fold_in(own_key, 6), axis_at), (blocks,), jnp.float32, least / len(cuts), high / len(cuts))
        return jnp.repeat(jnp.exp(steps), extent[axis_at] // blocks).reshape((-1,) + (1,) * (len(extent) - axis_at - 1))

    loudness = one(*cuts[0])
    for cut in cuts[1:]:
        loudness = loudness * one(*cut)
    return loudness


def centred(rng, shape, scale, limit, split=(), kind=jnp.bfloat16):
    level = block_levels(rng, shape, split, -0.22, 0.18) if split else 1.0
    result = jax.random.normal(rng, shape, jnp.float32) * scale * level
    return jnp.minimum(jnp.maximum(result, -limit), limit).astype(kind)


def setup_inputs(seed: int = 0) -> dict:
    keys = jax.random.split(jax.random.key(seed), 7)
    residual = draw_residual(jax.random.fold_in(keys[6], 71), 0)
    direction = draw_direction(jax.random.fold_in(keys[6], 71), 0)
    diagonal = jnp.clip(0.5 + 1.5 * jax.random.uniform(keys[2], (NX, NY, NZ), jnp.float32) ** block_levels(keys[2], (NX, NY, NZ), ((0, 4), (1, 4), (2, 2)), -0.2, 0.2), 0.5, 2.0)
    recycled = centred(keys[3], (RECYCLED, NX, NY, NZ), 1.0, 6.0, ((1, 4), (2, 4), (3, 2)))
    recycled_images = centred(keys[4], (RECYCLED, NX, NY, NZ), (RECYCLED * NX * NY * NZ) ** -0.5, 0.0014648438, ((1, 4), (2, 4), (3, 2)))
    coupling_inverse = draw_coupling_inverse(jax.random.fold_in(keys[6], 71), 0)
    return {"residual": residual, "direction": direction, "diagonal": diagonal, "recycled": recycled, "recycled_images": recycled_images, "coupling_inverse": coupling_inverse}


center = 7.25
half_width = 6.75


def neighbours_sum(values):
    beside_all = jnp.roll(values, -1, 1) + jnp.roll(values, 1, 1)
    beside_all = beside_all + jnp.roll(values, -1, 2) + jnp.roll(values, 1, 2)
    beside_all = beside_all + jnp.roll(values, -1, 3) + jnp.roll(values, 1, 3)
    return beside_all


def chebyshev_next(current, beside_all, diagonal, earlier):
    mapped = (6.0 + diagonal) * current - beside_all
    scaled = (mapped - center * current) / half_width
    if earlier is None:
        return scaled
    return 2.0 * scaled - earlier


def recurrence_matrix():
    recurrence = np.zeros((BASIS, BASIS), np.float32)
    for offset, length in ((0, S + 1), (S + 1, S)):
        recurrence[offset, offset] = center
        recurrence[offset + 1, offset] = half_width
        for column in range(1, length - 1):
            recurrence[offset + column + 1, offset + column] = half_width / 2
            recurrence[offset + column, offset + column] = center
            recurrence[offset + column - 1, offset + column] = half_width / 2
    return jnp.asarray(recurrence, dtype=jnp.float32)


def coordinates(totals, coupling_inverse):
    precise = lax.Precision.HIGHEST
    gram_block = totals[:BASIS]
    projections = totals[BASIS:]
    recurrence = recurrence_matrix()
    counter = jnp.arange(BASIS)
    residue = (counter == S + 1).astype(jnp.float32)
    search = (counter == 0).astype(jnp.float32)
    update = jnp.zeros((BASIS,), jnp.float32)
    norm_now = jnp.dot(residue, jnp.dot(gram_block, residue, precision=precise), precision=precise)
    for iteration in range(S):
        mapped = jnp.dot(recurrence, search, precision=precise)
        step_size = norm_now / jnp.dot(search, jnp.dot(gram_block, mapped, precision=precise), precision=precise)
        update = update + step_size * search
        residue = residue - step_size * mapped
        norm_next = jnp.dot(residue, jnp.dot(gram_block, residue, precision=precise), precision=precise)
        search = residue + (norm_next / norm_now) * search
        norm_now = norm_next
    weights = jnp.dot(coupling_inverse, jnp.dot(projections, residue, precision=precise), precision=precise)
    return update, residue, search, weights.astype(jnp.bfloat16)


def reference(residual, direction, diagonal, recycled, recycled_images, coupling_inverse):
    precise = lax.Precision.HIGHEST
    current = jnp.stack([direction, residual])
    earlier = None
    search_basis = [direction]
    residue_basis = [residual]
    for iteration in range(S):
        if iteration == S - 1:
            current = current[:1]
            earlier = earlier[:1]
        beside_all = neighbours_sum(current)
        following = chebyshev_next(current, beside_all, diagonal, earlier)
        earlier, current = current, following
        search_basis.append(following[0])
        if following.shape[0] > 1:
            residue_basis.append(following[1])
    basis = jnp.stack(search_basis + residue_basis)
    basis_flat = basis.reshape(BASIS, -1)
    gram_block = lax.dot_general(basis_flat, basis_flat, (((1,), (1,)), ((), ())), precision=precise, preferred_element_type=jnp.float32)
    rounded = basis_flat.astype(jnp.bfloat16)
    images = recycled_images.reshape(RECYCLED, -1)
    projections = lax.dot_general(images, rounded, (((1,), (1,)), ((), ())), preferred_element_type=jnp.float32)
    totals = jnp.concatenate([gram_block, projections], 0)
    update, residue, search, weights = coordinates(totals, coupling_inverse)
    shape = residual.shape
    solution_delta = jnp.dot(update, basis_flat, precision=precise).reshape(shape)
    new_residual = jnp.dot(residue, basis_flat, precision=precise).reshape(shape)
    correction = jnp.dot(weights, recycled.reshape(RECYCLED, -1), preferred_element_type=jnp.float32)
    new_direction = (jnp.dot(search, basis_flat, precision=precise) - correction).reshape(shape)
    return solution_delta, new_residual, new_direction
```

```python
import jax
import jax.numpy as jnp
from jax import lax
from jax.experimental import pallas as pl
from jax.experimental.pallas import tpu as pltpu
from jax.sharding import PartitionSpec as P

S = 4
BASIS = 9
RECYCLED = 16
LANES = 128
PROJECTED = 16
SECOND = 32
AXES = ("gx", "gy", "gz")


center = 7.25
half_width = 6.75


def extended(block, sides, width):
    for axis, dim in sides:
        count = lax.axis_size(axis)
        forward = [(i, i + 1) for i in range(count - 1)]
        forward.append((count - 1, 0))
        backward = [(target, source) for source, target in forward]
        low = lax.ppermute(
            lax.slice_in_dim(block, block.shape[dim] - width, None, axis=dim), axis, forward
        )
        high = lax.ppermute(lax.slice_in_dim(block, 0, width, axis=dim), axis, backward)
        block = jnp.concatenate([low, block, high], axis=dim)
    return block


def inside(padded):
    centre_cells = padded[:, 1:-1, 1:-1, 1:-1]
    beside_all = padded[:, 2:, 1:-1, 1:-1] + padded[:, :-2, 1:-1, 1:-1]
    beside_all = beside_all + padded[:, 1:-1, 2:, 1:-1] + padded[:, 1:-1, :-2, 1:-1]
    beside_all = beside_all + padded[:, 1:-1, 1:-1, 2:] + padded[:, 1:-1, 1:-1, :-2]
    return (centre_cells, beside_all)


def trim_margin(values, margin):
    if margin == 0:
        return values
    return values[..., margin:-margin, margin:-margin, margin:-margin]


def chebyshev_next(current, beside_all, diagonal, earlier):
    mapped = (6.0 + diagonal) * current - beside_all
    scaled = (mapped - center * current) / half_width
    if earlier is None:
        return scaled
    return 2.0 * scaled - earlier


def finish_kernel(parts, coupling, basis, recycled, delta_out, residual_out, direction_out):
    rows = 16
    total = jnp.sum(parts[...], axis=0)
    lane = lax.broadcasted_iota(jnp.int32, (rows, LANES), 1)
    row = lax.broadcasted_iota(jnp.int32, (rows, LANES), 0)
    table = jnp.concatenate([total, pltpu.roll(total, LANES - SECOND, 1)], axis=0)
    gram = jnp.where(lane < BASIS, table, 0.0)
    images = jnp.where(lane < RECYCLED, pltpu.roll(table, LANES - PROJECTED, 1), 0.0)

    def bands(index):
        first = (index == 0) | (index == S + 1)
        last = (index == S) | (index >= BASIS - 1)
        before_last = (index == S - 1) | (index == BASIS - 2)
        second = (index == 1) | (index == S + 2)
        middle = jnp.where(last, 0.0, center)
        below = jnp.where(first | (index >= BASIS), 0.0, jnp.where(second, half_width, half_width / 2))
        above = jnp.where(last | before_last, 0.0, half_width / 2)
        return (middle, below, above)

    by_row = bands(row)
    by_lane = bands(lane)

    def apply(coefficients, values, axis, size):
        middle, below, above = coefficients
        return (
            middle * values
            + below * pltpu.roll(values, 1, axis)
            + above * pltpu.roll(values, size - 1, axis)
        )

    def form(down, across):
        product = gram * down * across
        return jnp.sum(jnp.sum(product, axis=0, keepdims=True), axis=1, keepdims=True)

    residue = [(row == S + 1).astype(jnp.float32), (lane == S + 1).astype(jnp.float32)]
    search = [(row == 0).astype(jnp.float32), (lane == 0).astype(jnp.float32)]
    update = jnp.zeros((rows, LANES), jnp.float32)
    norm_now = form(residue[0], residue[1])
    for iteration in range(S):
        mapped = [apply(by_row, search[0], 0, rows), apply(by_lane, search[1], 1, LANES)]
        step_size = norm_now / form(search[0], mapped[1])
        update = update + step_size * search[0]
        residue = [residue[0] - step_size * mapped[0], residue[1] - step_size * mapped[1]]
        norm_next = form(residue[0], residue[1])
        ratio = norm_next / norm_now
        search = [residue[0] + ratio * search[0], residue[1] + ratio * search[1]]
        norm_now = norm_next
    projected = jnp.sum(images * residue[0], axis=0, keepdims=True)[:, :RECYCLED]
    weights = jnp.sum(coupling[...] * projected, axis=1, keepdims=True)
    weights = jnp.broadcast_to(weights.astype(jnp.bfloat16).astype(jnp.float32), (RECYCLED, LANES))
    for plane in range(delta_out.shape[0]):
        delta = 0.0
        left = 0.0
        ahead = 0.0
        for field in range(BASIS):
            values = basis[field, plane]
            delta = delta + update[field : field + 1] * values
            left = left + residue[0][field : field + 1] * values
            ahead = ahead + search[0][field : field + 1] * values
        correction = 0.0
        for vector in range(RECYCLED):
            correction = correction + weights[vector : vector + 1] * recycled[vector, plane].astype(jnp.float32)
        delta_out[plane] = delta
        residual_out[plane] = left
        direction_out[plane] = ahead - correction


def body(residual, direction, diagonal, recycled, recycled_images, coupling_inverse):
    precise = lax.Precision.HIGHEST
    search_basis = [direction]
    residue_basis = [residual]
    earlier = None
    packed = jnp.stack([direction, residual, diagonal])
    padded = extended(packed, (("gx", 1), ("gy", 2), ("gz", 3)), S)
    wide_diag = padded[2]
    current = padded[:2]
    for iteration in range(S):
        if iteration == S - 1:
            current = current[:1]
            earlier = earlier[:1]
        centre_cells, beside_all = inside(current)
        margin = S - iteration - 1
        local_diag = trim_margin(wide_diag, iteration + 1)
        previous = None if earlier is None else trim_margin(earlier, 2)
        following = chebyshev_next(centre_cells, beside_all, local_diag, previous)
        earlier, current = (current, following)
        search_basis.append(trim_margin(following[0], margin))
        if following.shape[0] > 1:
            residue_basis.append(trim_margin(following[1], margin))
    basis = jnp.stack(search_basis + residue_basis)
    basis_flat = basis.reshape(basis.shape[0], -1)
    gram_block = lax.dot_general(
        basis_flat,
        basis_flat,
        (((1,), (1,)), ((), ())),
        precision=precise,
        preferred_element_type=jnp.float32,
    )
    rounded = basis_flat.astype(jnp.bfloat16)
    images = recycled_images.reshape(recycled_images.shape[0], -1)
    projections = lax.dot_general(
        images, rounded, (((1,), (1,)), ((), ())), preferred_element_type=jnp.float32
    )
    table = jnp.zeros((BASIS, LANES), jnp.float32)
    table = table.at[:, :BASIS].set(gram_block).at[:, PROJECTED : PROJECTED + RECYCLED].set(projections.T)
    last = jnp.roll(table[BASIS - 1 :], SECOND, 1)
    table = table[: BASIS - 1] + jnp.pad(last, ((0, BASIS - 2), (0, 0)))
    devices = lax.axis_size(AXES)
    parts = lax.all_to_all(jnp.broadcast_to(table[None], (devices, BASIS - 1, LANES)), AXES, 0, 0)
    field = jax.ShapeDtypeStruct(residual.shape, jnp.float32)
    in_vmem = pl.BlockSpec(memory_space=pltpu.VMEM)
    return pl.pallas_call(
        finish_kernel,
        out_shape=(field, field, field),
        in_specs=[in_vmem] * 4,
        out_specs=(in_vmem, in_vmem, in_vmem),
        name="finish",
    )(parts, coupling_inverse, basis, recycled)


def solution(mesh):
    in_specs = (
        P("gx", "gy", "gz"),
        P("gx", "gy", "gz"),
        P("gx", "gy", "gz"),
        P(None, "gx", "gy", "gz"),
        P(None, "gx", "gy", "gz"),
        P(),
    )
    out_specs = (P("gx", "gy", "gz"), P("gx", "gy", "gz"), P("gx", "gy", "gz"))
    return jax.shard_map(body, mesh=mesh, in_specs=in_specs, out_specs=out_specs, check_vma=False)
```

```python
import jax
import jax.numpy as jnp
from jax import lax
from jax.experimental import pallas as pl
from jax.experimental.pallas import tpu as pltpu
from jax.sharding import PartitionSpec as P

S = 4
BASIS = 9
RECYCLED = 16
LANES = 128
TILE = 8
AXES = ("gx", "gy", "gz")

RIM = 2 * S
SIDE = RIM * S


center = 7.25
half_width = 6.75


def lanes_of(rows):
    return lax.broadcasted_iota(jnp.int32, (rows, LANES), 1)


def rows_of(rows):
    return lax.broadcasted_iota(jnp.int32, (rows, LANES), 0)


def turn(values, shift, axis):
    shift = shift % values.shape[axis]
    return pltpu.roll(values, shift, axis) if shift else values


def rim_kernel(direction, residual, diagonal, coupling, rim_out, after_out, before_out, coupling_out):
    planes, rows, _ = direction.shape
    lane = lanes_of(rows)
    after = jnp.zeros((rows, LANES), jnp.float32)
    before = jnp.zeros((rows, LANES), jnp.float32)
    for field, source in enumerate((direction, residual, diagonal)):
        rim = jnp.zeros((rows, LANES), jnp.float32)
        for plane in range(planes):
            base = SIDE + RIM * plane
            values = source[plane]
            place = lane - base
            rim = jnp.where((place >= 0) & (place < S), turn(values, base, 1), rim)
            rim = jnp.where((place >= S) & (place < RIM), turn(values, base + RIM, 1), rim)
        rim_out[field] = rim
        mine = (lane >= SIDE * field) & (lane < SIDE * (field + 1))
        after = jnp.where(mine, turn(rim, SIDE * field - RIM * planes, 1), after)
        before = jnp.where(mine, turn(rim, SIDE * field - SIDE, 1), before)
    after_out[...] = after
    before_out[...] = before
    vector = lax.broadcasted_iota(jnp.int32, (RECYCLED, LANES), 0)
    spread = (lanes_of(RECYCLED) == 16 * (vector % 8) + 8 * (vector // 8)).astype(jnp.float32)
    coupling_out[...] = jnp.dot(
        coupling[...], spread, precision=lax.Precision.HIGHEST, preferred_element_type=jnp.float32
    )


def plane_of(own, low, high, field, x):
    planes = own.shape[0]
    first = (0, S, 2 * S - 1)[field]
    width = (S, S - 1, S - 1)[field]
    if x < 0:
        return low[first + width + x]
    if x >= planes:
        return high[first + x - planes]
    return own[x]


def groups_of(planes):
    found = []
    for field in range(3):
        reach = (S, S - 1, S - 1)[field]
        for x in range(1 - reach, planes + reach - 1):
            found.append((field, x))
    return found + [(field, None) for field in range(3)]


def edge_kernel(
    parity, direction, residual, diagonal, low, high, rim_next, rim_before, rim_low_next, rim_low_before, rim_high_next, rim_high_before, first_out, second_out, rim_out
):
    planes, rows, _ = direction.shape
    lane = lanes_of(rows)
    nearer = lane % RIM < S
    low_rim = jnp.where(nearer, rim_low_next[...], rim_low_before[...])
    high_rim = jnp.where(nearer, rim_high_next[...], rim_high_before[...])
    for field in range(3):
        rim = jnp.where(nearer, rim_next[field], rim_before[field])
        rim = jnp.where(lane < SIDE, turn(low_rim, -SIDE * field, 1), rim)
        rim = jnp.where(lane >= SIDE + RIM * planes, turn(high_rim, SIDE + RIM * planes - SIDE * field, 1), rim)
        rim_out[field] = rim
    fields = (direction, residual, diagonal)
    row = rows_of(TILE)

    def ends(group):
        field, x = group
        values = rim_out[field] if x is None else plane_of(fields[field], low, high, field, x)
        return values[:TILE], values[rows - TILE :]

    even = parity[0] == 0
    groups = groups_of(planes)
    for tile in range(first_out.shape[0]):
        start, end = ends(groups[2 * tile])
        if 2 * tile + 1 < len(groups):
            start_too, end_too = ends(groups[2 * tile + 1])
        else:
            start_too, end_too = start, end
        lower = jnp.where(row < S, start, turn(start_too, S, 0))
        upper = jnp.where(row < S, turn(end, S, 0), end_too)
        first_out[tile] = jnp.where(even, upper, lower)
        second_out[tile] = jnp.where(even, lower, upper)


def basis_kernel(
    parity, direction, residual, diagonal, low, high, rims, first, second, images, basis_out, parts_out, walk, trail, weight
):
    planes, rows, _ = direction.shape
    ring = rows + 2 * S
    fields = (direction, residual, diagonal)
    row = rows_of(TILE)
    lane = lanes_of(ring)
    place = lane % RIM
    even = parity[0] == 0
    halo = {}
    groups = groups_of(planes)
    for tile in range(first.shape[0]):
        above = jnp.where(even, first[tile], second[tile])
        below = jnp.where(even, second[tile], first[tile])
        halo[groups[2 * tile]] = jnp.where(row < S, above, turn(below, S, 0))
        if 2 * tile + 1 < len(groups):
            halo[groups[2 * tile + 1]] = jnp.where(row < S, turn(above, S, 0), below)
    nothing = jnp.zeros((TILE, LANES), jnp.float32)

    def whole(field, x):
        if x is None:
            inner = rims[field]
        else:
            inner = plane_of(fields[field], low, high, field, x)
        return jnp.concatenate([inner, halo.get((field, x), nothing)], axis=0)

    def scaled(values):
        return (values - (center - 6.0)) * (2.0 / half_width)

    def facing(rim):
        return jnp.where(place == 1, turn(rim, 2 - RIM, 1), rim)

    def ends_of(values, x, gathered):
        base = RIM * (x + S)
        here = (lane == base) | (lane == base + 1)
        return jnp.where(here, turn(values, base + 1, 1), gathered)

    for x in range(1 - S, planes + S - 1):
        weight[x + S] = scaled(whole(2, x))
    weight_rim = scaled(whole(2, None))

    def step(level, history, offset, x, rim_facing, own):
        at = x + S
        values = history[level, at]
        across = turn(rim_facing, -(RIM * at + 1), 1)
        beside = history[level, at - 1] + history[level, at + 1]
        beside = beside + (turn(values, 1, 0) + turn(values, ring - 1, 0))
        beside = beside + jnp.where(lane == 0, across, turn(values, 1, 1))
        beside = beside + jnp.where(lane == LANES - 1, across, turn(values, LANES - 1, 1))
        following = weight[at] * values - (2.0 / half_width) * beside
        if level == 0:
            following = 0.5 * following
        else:
            following = following - history[level - 1, at]
        if 0 <= x < planes:
            basis_out[offset + level, x] = following[:rows]
        if not own:
            history[level + 1, at] = following
        return following

    def rim_step(level, rims_so_far, gathered):
        rim = rims_so_far[level]
        beside = turn(rim, RIM, 1) + turn(rim, -RIM, 1)
        beside = beside + (turn(rim, 1, 0) + turn(rim, ring - 1, 0))
        beside = beside + jnp.where(place == 0, gathered, turn(rim, 1, 1))
        beside = beside + jnp.where(place == RIM - 1, turn(gathered, RIM - 2, 1), turn(rim, -1, 1))
        following = weight_rim * rim - (2.0 / half_width) * beside
        if level == 0:
            return 0.5 * following
        return following - rims_so_far[level - 1]

    for field, history, offset, length in ((0, walk, 0, S), (1, trail, S, S - 1)):
        gathered = jnp.zeros((ring, LANES), jnp.float32)
        for x in range(-length, planes + length):
            values = whole(field, x)
            history[0, x + S] = values
            gathered = ends_of(values, x, gathered)
        rims_so_far = [whole(field, None)]
        for level in range(length):
            rim_facing = facing(rims_so_far[level])
            reach = length - 1 - level
            own = reach == 0
            gathered_next = jnp.zeros((ring, LANES), jnp.float32)
            for x in range(-reach, planes + reach):
                following = step(level, history, offset, x, rim_facing, own)
                if not own:
                    gathered_next = ends_of(following, x, gathered_next)
            if not own:
                rims_so_far.append(rim_step(level, rims_so_far, gathered))
                gathered = gathered_next

    def field_of(index):
        if index == 0:
            return direction
        if index == S + 1:
            return residual
        return basis_out.at[index - 1 if index <= S else index - 2]

    members = [field_of(index) for index in range(BASIS)]
    pairs = [(i, j) for i in range(BASIS) for j in range(i, BASIS)]
    sums = {}
    for x in range(planes):
        for start in range(0, rows, TILE):
            values = [member[x, start : start + TILE] for member in members]
            for i, j in pairs:
                product = values[i] * values[j]
                sums[i, j] = sums[i, j] + product if (i, j) in sums else product

    half = 16
    total = jnp.zeros((BASIS * half, RECYCLED * half), jnp.float32)
    for x in range(planes):
        rounded = []
        against = []
        for start in range(0, rows, half):
            rounded.append(
                jnp.concatenate([member[x, start : start + half].astype(jnp.bfloat16) for member in members], axis=0)
            )
            against.append(images[:, x, start : start + half, :].reshape(RECYCLED * half, LANES))
        total = total + lax.dot_general(
            jnp.concatenate(rounded, axis=1),
            jnp.concatenate(against, axis=1),
            (((1,), (1,)), ((), ())),
            preferred_element_type=jnp.float32,
        )
    wide = (BASIS * half, RECYCLED * half)
    same = (
        lax.broadcasted_iota(jnp.int32, wide, 0) % half == lax.broadcasted_iota(jnp.int32, wide, 1) % half
    )
    total = jnp.where(same, total, 0.0)
    spot = lanes_of(TILE)
    table = jnp.zeros((TILE, LANES), jnp.float32)
    for index in range(BASIS):
        line = jnp.sum(total[half * index : half * (index + 1)], axis=0, keepdims=True)
        line = jnp.concatenate([line[:, :LANES], line[:, LANES:]], axis=0)
        line = jnp.broadcast_to(line[:, None, :], (2, TILE, LANES)).reshape(2 * TILE, LANES)
        for shift in (1, 2, 4, 8):
            line = line + turn(line, -shift, 1)
        line = jnp.where(
            spot % 16 == 0, line[:TILE], jnp.where(spot % 16 == 8, turn(line[TILE:], 8, 1), 0.0)
        )
        if index < TILE:
            table = jnp.where((row == index) & (spot % 8 == 0), line, table)
        else:
            table = jnp.where((row == 0) & (spot % 8 == 4), turn(line, 4, 1), table)

    def lane_of(index):
        return jnp.where(index <= S, 1 + 16 * index, 9 + 16 * (index - S - 1))

    for j in range(BASIS):
        column = jnp.zeros((TILE, LANES), jnp.float32)
        for i in range(TILE):
            summed = jnp.sum(sums[min(i, j), max(i, j)], axis=0, keepdims=True)
            column = jnp.where(row == i, summed, column)
        column = jnp.sum(column, axis=1, keepdims=True)
        at = 1 + 16 * j if j <= S else 9 + 16 * (j - S - 1)
        table = jnp.where(spot == at, column, table)
        if j == BASIS - 1:
            table = jnp.where(spot == lane_of(row) + 4, column, table)
    corner = jnp.sum(jnp.sum(sums[BASIS - 1, BASIS - 1], axis=0, keepdims=True), axis=1, keepdims=True)
    table = jnp.where((row == 0) & (spot == 9 + 16 * (BASIS - 2 - S) + 4), corner, table)
    for device in range(parts_out.shape[0]):
        parts_out[device] = table


def bands(position, length):
    inside = (position >= 0) & (position < length)
    middle = jnp.where(inside & (position < length - 1), center, 0.0)
    below = jnp.where(position == 1, half_width, half_width / 2)
    below = jnp.where(inside & (position >= 1), below, 0.0)
    above = jnp.where(inside & (position < length - 2), half_width / 2, 0.0)
    return (middle, below, above)


def finish_kernel(parts, coupling, direction, residual, basis, recycled, delta_out, residual_out, direction_out):
    height = 16
    total = jnp.sum(parts[...], axis=0)
    spot = lanes_of(TILE)
    last = jnp.sum(jnp.where(spot % 8 >= 4, total, 0.0), axis=0, keepdims=True)
    last = turn(jnp.broadcast_to(last, (TILE, LANES)), -4, 1)
    table = jnp.concatenate([total, jnp.where(rows_of(TILE) == 0, last, 0.0)], axis=0)
    lane = lanes_of(height)
    row = rows_of(height)
    gram = jnp.where(lane % 8 == 1, table, 0.0)
    images = jnp.where(lane % 8 == 0, table, 0.0)
    by_row = bands(jnp.where(row <= S, row, row - S - 1), jnp.where(row <= S, S + 1, S))
    leading = lane % 16 < 8
    by_lane = bands(lane // 16, jnp.where(leading, S + 1, S))

    def apply(coefficients, values, axis, stride):
        middle, below, above = coefficients
        return middle * values + below * turn(values, stride, axis) + above * turn(values, -stride, axis)

    def form(down, across):
        product = gram * down * across
        return jnp.sum(jnp.sum(product, axis=0, keepdims=True), axis=1, keepdims=True)

    residue = [(row == S + 1).astype(jnp.float32), ((lane // 16 == 0) & ~leading).astype(jnp.float32)]
    search = [(row == 0).astype(jnp.float32), ((lane // 16 == 0) & leading).astype(jnp.float32)]
    update = jnp.zeros((height, LANES), jnp.float32)
    norm_now = form(residue[0], residue[1])
    for iteration in range(S):
        mapped = [apply(by_row, search[0], 0, 1), apply(by_lane, search[1], 1, 16)]
        step_size = norm_now / form(search[0], mapped[1])
        update = update + step_size * search[0]
        residue = [residue[0] - step_size * mapped[0], residue[1] - step_size * mapped[1]]
        norm_next = form(residue[0], residue[1])
        ratio = norm_next / norm_now
        search = [residue[0] + ratio * search[0], residue[1] + ratio * search[1]]
        norm_now = norm_next
    projected = jnp.sum(images * residue[0], axis=0, keepdims=True)
    weights = jnp.sum(coupling[...] * projected, axis=1, keepdims=True)
    weights = jnp.broadcast_to(weights.astype(jnp.bfloat16).astype(jnp.float32), (RECYCLED, LANES))
    for plane in range(delta_out.shape[0]):
        delta = 0.0
        left = 0.0
        ahead = 0.0
        for field in range(BASIS):
            if field == 0:
                values = direction[plane]
            elif field == S + 1:
                values = residual[plane]
            else:
                values = basis[field - 1 if field <= S else field - 2, plane]
            delta = delta + update[field : field + 1] * values
            left = left + residue[0][field : field + 1] * values
            ahead = ahead + search[0][field : field + 1] * values
        correction = 0.0
        for vector in range(RECYCLED):
            correction = correction + weights[vector : vector + 1] * recycled[vector, plane].astype(jnp.float32)
        delta_out[plane] = delta
        residual_out[plane] = left
        direction_out[plane] = ahead - correction


def shifted(values, shifts):
    axes = tuple(shifts)
    counts = [lax.axis_size(axis) for axis in axes]
    pairs = [(0, 0)]
    for axis, count in zip(axes, counts):
        pairs = [
            (source * count + i, target * count + (i + shifts[axis]) % count)
            for source, target in pairs
            for i in range(count)
        ]
    return lax.ppermute(values, axes, pairs)


def call(kernel, out_shape, operands, name, scratch=(), limit=16):
    in_vmem = pl.BlockSpec(memory_space=pltpu.VMEM)
    in_smem = pl.BlockSpec(memory_space=pltpu.SMEM)
    return pl.pallas_call(
        kernel,
        out_shape=tuple(jax.ShapeDtypeStruct(shape, jnp.float32) for shape in out_shape),
        in_specs=[in_smem if operand.dtype == jnp.int32 else in_vmem for operand in operands],
        out_specs=(in_vmem,) * len(out_shape),
        scratch_shapes=list(scratch),
        compiler_params=pltpu.CompilerParams(vmem_limit_bytes=limit * 1024 * 1024),
        name=name,
    )(*operands)


def body(residual, direction, diagonal, recycled, recycled_images, coupling_inverse):
    planes, rows, columns = residual.shape
    if columns != LANES or rows % 16 or RIM * (planes + 2 * S) != LANES or lax.axis_size("gy") % 2:
        raise ValueError("unsupported block")
    fields = (direction, residual, diagonal)
    reach = (S, S - 1, S - 1)
    upper = jnp.concatenate([field[planes - width :] for field, width in zip(fields, reach)])
    lower = jnp.concatenate([field[:width] for field, width in zip(fields, reach)])
    low = shifted(upper, {"gx": 1})
    high = shifted(lower, {"gx": -1})
    rim, rim_after, rim_before, coupling = call(
        rim_kernel,
        [(3, rows, LANES), (rows, LANES), (rows, LANES), (RECYCLED, LANES)],
        (*fields, coupling_inverse),
        "rim",
    )
    sides = (-1,) if lax.axis_size("gz") == 2 else (-1, 1)
    rims = [shifted(rim, {"gz": side}) for side in sides]
    low_rims = [shifted(rim_after, {"gx": 1, "gz": side}) for side in sides]
    high_rims = [shifted(rim_before, {"gx": -1, "gz": side}) for side in sides]
    parity = (lax.axis_index("gy") % 2).astype(jnp.int32).reshape(1)
    tiles = (len(groups_of(planes)) + 1) // 2
    first, second, whole_rims = call(
        edge_kernel,
        [(tiles, TILE, LANES), (tiles, TILE, LANES), (3, rows, LANES)],
        (parity, *fields, low, high, rims[0], rims[-1], low_rims[0], low_rims[-1], high_rims[0], high_rims[-1]),
        "edge",
    )
    count = lax.axis_size("gy")
    first = lax.ppermute(first, "gy", [(i, i ^ 1) for i in range(count)])
    second = lax.ppermute(second, "gy", [(i, (i - 1 + 2 * (i % 2)) % count) for i in range(count)])
    devices = lax.axis_size(AXES)
    ring = rows + 2 * S
    basis, parts = call(
        basis_kernel,
        [(BASIS - 2, planes, rows, LANES), (devices, TILE, LANES)],
        (parity, *fields, low, high, whole_rims, first, second, recycled_images),
        "basis",
        [
            pltpu.VMEM((S, planes + 2 * S, ring, LANES), jnp.float32),
            pltpu.VMEM((S - 1, planes + 2 * S, ring, LANES), jnp.float32),
            pltpu.VMEM((planes + 2 * S, ring, LANES), jnp.float32),
        ],
    )
    parts = lax.all_to_all(parts, AXES, 0, 0)
    return call(
        finish_kernel,
        [residual.shape] * 3,
        (parts, coupling, direction, residual, basis, recycled),
        "finish",
    )


def solution(mesh):
    in_specs = (
        P("gx", "gy", "gz"),
        P("gx", "gy", "gz"),
        P("gx", "gy", "gz"),
        P(None, "gx", "gy", "gz"),
        P(None, "gx", "gy", "gz"),
        P(),
    )
    out_specs = (P("gx", "gy", "gz"), P("gx", "gy", "gz"), P("gx", "gy", "gz"))
    return jax.shard_map(body, mesh=mesh, in_specs=in_specs, out_specs=out_specs, check_vma=False)
```

```python
import jax
import jax.numpy as jnp
import numpy as np
from jax import lax
from jax.experimental import pallas as pl
from jax.experimental.pallas import tpu as pltpu
from jax.sharding import PartitionSpec as P

S = 4
BASIS = 9
RECYCLED = 16
LANES = 128
TILE = 8
AXES = ("gx", "gy", "gz")

RIM = 2 * S
SIDE = RIM * S


center = 7.25
half_width = 6.75


def lanes_of(rows):
    return lax.broadcasted_iota(jnp.int32, (rows, LANES), 1)


def rows_of(rows):
    return lax.broadcasted_iota(jnp.int32, (rows, LANES), 0)


def turn(values, shift, axis):
    shift = shift % values.shape[axis]
    return pltpu.roll(values, shift, axis) if shift else values


def rim_kernel(direction, residual, diagonal, coupling, rim_out, after_out, before_out, coupling_out):
    planes, rows, _ = direction.shape
    lane = lanes_of(rows)
    after = jnp.zeros((rows, LANES), jnp.float32)
    before = jnp.zeros((rows, LANES), jnp.float32)
    for field, source in enumerate((direction, residual, diagonal)):
        rim = jnp.zeros((rows, LANES), jnp.float32)
        for plane in range(planes):
            base = SIDE + RIM * plane
            values = source[plane]
            place = lane - base
            rim = jnp.where((place >= 0) & (place < S), turn(values, base, 1), rim)
            rim = jnp.where((place >= S) & (place < RIM), turn(values, base + RIM, 1), rim)
        rim_out[field] = rim
        mine = (lane >= SIDE * field) & (lane < SIDE * (field + 1))
        after = jnp.where(mine, turn(rim, SIDE * field - RIM * planes, 1), after)
        before = jnp.where(mine, turn(rim, SIDE * field - SIDE, 1), before)
    after_out[...] = after
    before_out[...] = before
    vector = lax.broadcasted_iota(jnp.int32, (RECYCLED, LANES), 0)
    spread = (lanes_of(RECYCLED) == 16 * (vector % 8) + 8 * (vector // 8)).astype(jnp.float32)
    coupling_out[...] = jnp.dot(
        coupling[...], spread, precision=lax.Precision.HIGHEST, preferred_element_type=jnp.float32
    )


def plane_of(own, low, high, field, x):
    planes = own.shape[0]
    first = (0, S, 2 * S - 1)[field]
    width = (S, S - 1, S - 1)[field]
    if x < 0:
        return low[first + width + x]
    if x >= planes:
        return high[first + x - planes]
    return own[x]


def packing(planes):
    pieces = []
    for field in range(3):
        reach = (S, S - 1, S - 1)[field]
        for x in range(1 - reach, planes + reach - 1):
            pieces.append((reach - max(0, -x, x - planes + 1), field, x))
        pieces.append((reach - 1, field, None))
    pieces.sort(key=lambda piece: -piece[0])
    tiles = []
    for count, field, x in pieces:
        for tile in tiles:
            used = sum(piece[0] for piece in tile)
            if used + count <= TILE:
                tile.append((count, field, x, used))
                break
        else:
            tiles.append([(count, field, x, 0)])
    return tiles


def edge_kernel(
    parity, direction, residual, diagonal, low, high, rim_next, rim_before, rim_low_next, rim_low_before, rim_high_next, rim_high_before, first_out, second_out, rim_out
):
    planes, rows, _ = direction.shape
    lane = lanes_of(rows)
    nearer = lane % RIM < S
    low_rim = jnp.where(nearer, rim_low_next[...], rim_low_before[...])
    high_rim = jnp.where(nearer, rim_high_next[...], rim_high_before[...])
    for field in range(3):
        rim = jnp.where(nearer, rim_next[field], rim_before[field])
        rim = jnp.where(lane < SIDE, turn(low_rim, -SIDE * field, 1), rim)
        rim = jnp.where(lane >= SIDE + RIM * planes, turn(high_rim, SIDE + RIM * planes - SIDE * field, 1), rim)
        rim_out[field] = rim
    fields = (direction, residual, diagonal)
    row = rows_of(TILE)

    even = parity[0] == 0
    for index, tile in enumerate(packing(planes)):
        lower = jnp.zeros((TILE, LANES), jnp.float32)
        upper = jnp.zeros((TILE, LANES), jnp.float32)
        for count, field, x, offset in tile:
            values = rim_out[field] if x is None else plane_of(fields[field], low, high, field, x)
            mine = (row >= offset) & (row < offset + count)
            lower = jnp.where(mine, turn(values[:TILE], offset, 0), lower)
            upper = jnp.where(mine, turn(values[rows - TILE :], offset + count, 0), upper)
        first_out[index] = jnp.where(even, upper, lower)
        second_out[index] = jnp.where(even, lower, upper)


def shift_matrices():
    source = np.arange(LANES)[:, None]
    target = np.arange(LANES)[None, :]
    along = np.abs(source - target) == 1
    ends = ((target % RIM == 0) & (source == LANES - 1)) | ((target % RIM == RIM - 1) & (source == 0))
    facing = ((target == 0) & (source % RIM == RIM - 1)) | ((target == LANES - 1) & (source % RIM == 0))
    around = (np.abs(source - target) == RIM) | (along & (source // RIM == target // RIM))
    inner = np.concatenate([along, ends], 1)
    outer = np.concatenate([facing, np.zeros_like(facing)], 1)
    return (
        jnp.asarray(np.concatenate([inner, inner, outer, outer]), jnp.bfloat16),
        jnp.asarray(np.concatenate([around, around]), jnp.bfloat16),
    )


def split(values):
    leading = values.astype(jnp.bfloat16)
    return leading, (values - leading.astype(jnp.float32)).astype(jnp.bfloat16)


def products():
    found = []
    for one, other, count in ((0, 0, 2 * S + 1), (S + 1, S + 1, 2 * S - 1), (0, S + 1, 2 * S)):
        found.append([(one + (m + 1) // 2, other + m // 2) for m in range(count)])
    return found


def basis_kernel(
    parity, direction, residual, diagonal, low, high, rims, first, second, images, shifts, rim_shifts, basis_out, parts_out, walk, trail, weight, left
):
    planes, rows, _ = direction.shape
    ring = rows + 2 * S
    fields = (direction, residual, diagonal)
    row = rows_of(TILE)
    lane = lanes_of(ring)
    even = parity[0] == 0
    halo = {}
    for index, tile in enumerate(packing(planes)):
        above = jnp.where(even, first[index], second[index])
        below = jnp.where(even, second[index], first[index])
        for count, field, x, offset in tile:
            halo[field, x] = jnp.where(row < S, turn(above, -offset, 0), turn(below, -offset - count, 0))
    nothing = jnp.zeros((TILE, LANES), jnp.float32)

    def whole(field, x):
        if x is None:
            inner = rims[field]
        else:
            inner = plane_of(fields[field], low, high, field, x)
        return jnp.concatenate([inner, halo.get((field, x), nothing)], axis=0)

    def scaled(values):
        return (values - (center - 6.0)) * (2.0 / half_width)

    for x in range(1 - S, planes + S - 1):
        weight[x + S] = scaled(whole(2, x))
    weight_rim = scaled(whole(2, None))
    chains = ((0, walk, 0, S), (1, trail, S, S - 1))
    rim_levels = {}
    for field, history, offset, length in chains:
        for x in range(-length, planes + length):
            history[0, x + S] = whole(field, x)
        rim_levels[field] = [whole(field, None)]

    def advance(values, before, factor, beside):
        following = factor * values - (2.0 / half_width) * beside
        return 0.5 * following if before is None else following - before

    for level in range(S):
        work = []
        for field, history, offset, length in chains:
            reach = length - 1 - level
            if reach < 0:
                continue
            lead, rest = split(rim_levels[field][level])
            lead = lead.astype(jnp.float32)
            rest = rest.astype(jnp.float32)
            for x in range(-reach, planes + reach, 2):
                pair = jnp.concatenate([history[level, x + S], history[level, x + S + 1]], axis=0)
                parts = list(split(pair))
                for facing in (lead, rest):
                    slots = [jnp.where(lane // RIM == x + S + k, facing, 0.0) for k in range(2)]
                    parts.append(jnp.concatenate(slots, axis=0).astype(jnp.bfloat16))
                for index, part in enumerate(parts):
                    left[ring * len(work) : ring * (len(work) + 2), LANES * index : LANES * (index + 1)] = part
                work.append((field, history, offset, reach, x))
                work.append((field, history, offset, reach, x + 1))
        moved = jnp.dot(left[: ring * len(work)], shifts[...], preferred_element_type=jnp.float32)
        gathered = {}
        for index, (field, history, offset, reach, x) in enumerate(work):
            at = x + S
            here = moved[ring * index : ring * (index + 1)]
            values = history[level, at]
            beside = here[:, :LANES] + (history[level, at - 1] + history[level, at + 1])
            beside = beside + (turn(values, 1, 0) + turn(values, -1, 0))
            before = None if level == 0 else history[level - 1, at]
            following = advance(values, before, weight[at], beside)
            if 0 <= x < planes:
                basis_out[offset + level, x] = following[:rows]
            if reach:
                history[level + 1, at] = following
                gathered[field] = jnp.where(lane // RIM == at, here[:, LANES:], gathered.get(field, 0.0))
        for field in gathered:
            levels = rim_levels[field]
            rim = levels[level]
            beside = jnp.dot(
                jnp.concatenate(split(rim), axis=1), rim_shifts[...], preferred_element_type=jnp.float32
            )
            beside = beside + (turn(rim, 1, 0) + turn(rim, -1, 0)) + gathered[field]
            levels.append(advance(rim, None if level == 0 else levels[level - 1], weight_rim, beside))

    def field_of(index):
        if index == 0:
            return direction
        if index == S + 1:
            return residual
        return basis_out.at[index - 1 if index <= S else index - 2]

    members = [field_of(index) for index in range(BASIS)]
    families = products()
    sums = {}
    for x in range(planes):
        for start in range(0, rows, TILE):
            values = [member[x, start : start + TILE] for member in members]
            for family in families:
                for i, j in family:
                    product = values[i] * values[j]
                    sums[i, j] = sums[i, j] + product if (i, j) in sums else product

    half = 16
    total = jnp.zeros((BASIS * half, RECYCLED * half), jnp.float32)
    for x in range(planes):
        rounded = []
        against = []
        for start in range(0, rows, half):
            rounded.append(
                jnp.concatenate([member[x, start : start + half].astype(jnp.bfloat16) for member in members], axis=0)
            )
            against.append(images[:, x, start : start + half, :].reshape(RECYCLED * half, LANES))
        total = total + lax.dot_general(
            jnp.concatenate(rounded, axis=1),
            jnp.concatenate(against, axis=1),
            (((1,), (1,)), ((), ())),
            preferred_element_type=jnp.float32,
        )
    wide = (BASIS * half, RECYCLED * half)
    same = (
        lax.broadcasted_iota(jnp.int32, wide, 0) % half == lax.broadcasted_iota(jnp.int32, wide, 1) % half
    )
    total = jnp.where(same, total, 0.0)
    spot = lanes_of(TILE)
    table = jnp.zeros((TILE, LANES), jnp.float32)
    for index in range(BASIS):
        line = jnp.sum(total[half * index : half * (index + 1)], axis=0, keepdims=True)
        if index < TILE:
            table = jnp.where(row == index, line[:, :LANES], table)
            other = line[:, LANES:] if index == 0 else jnp.where(row == index, line[:, LANES:], other)
    third = jnp.where(row == 0, line[:, :LANES], jnp.where(row == 1, line[:, LANES:], 0.0))
    blocks = jnp.concatenate([table, jnp.broadcast_to(other, (TILE, LANES)), third], axis=0)
    for shift in (1, 2, 4, 8):
        blocks = blocks + turn(blocks, -shift, 1)
    table = jnp.where(spot % 16 == 0, blocks[:TILE], 0.0)
    table = jnp.where(spot % 16 == 8, turn(blocks[TILE : 2 * TILE], 8, 1), table)
    ninth = turn(blocks[2 * TILE :], 4, 1)
    table = jnp.where((row == 0) & (spot % 16 == 4), ninth, table)
    table = jnp.where((row == 1) & (spot % 16 == 12), turn(ninth, 8, 1), table)
    columns = [list(families[0][:TILE]), list(families[1]) + [families[0][TILE]], list(families[2])]
    for place, column in enumerate(columns):
        values = jnp.zeros((TILE, LANES), jnp.float32)
        for index, pair in enumerate(column):
            values = jnp.where(row == index, jnp.sum(sums[pair], axis=0, keepdims=True), values)
        values = jnp.sum(values, axis=1, keepdims=True)
        table = jnp.where(spot == RIM * place + 1, values, table)
    for device in range(parts_out.shape[0]):
        parts_out[device] = table


def moments_of(values):
    first = values[:2]
    return first + [2.0 * value - first[index % 2] for index, value in enumerate(values[2:])]


def finish_kernel(parts, coupling, direction, residual, basis, recycled, delta_out, residual_out, direction_out):
    table = jnp.sum(parts[...], axis=0)
    spot = lanes_of(TILE)
    row = rows_of(TILE)
    columns = [
        jnp.broadcast_to(table[:, RIM * place + 1 : RIM * place + 2], (TILE, LANES)) for place in range(3)
    ]

    def spread(column, index):
        return jnp.broadcast_to(columns[column][index : index + 1], (TILE, LANES))

    walk = moments_of([spread(0, index) for index in range(TILE)] + [spread(1, TILE - 1)])
    trail = moments_of([spread(1, index) for index in range(2 * S - 1)])
    cross = moments_of([spread(2, index) for index in range(2 * S)])
    gram = {}
    for i in range(BASIS):
        for j in range(i, BASIS):
            source = walk if j <= S else (cross if i <= S else trail)
            one = i if i <= S else i - S - 1
            two = j if j <= S else j - S - 1
            gram[i, j] = gram[j, i] = 0.5 * (source[one + two] + source[abs(one - two)])

    def dot(one, other):
        terms = [one[i] * other[i] for i in one if i in other]
        while len(terms) > 1:
            terms = [a + b for a, b in zip(terms[::2], terms[1::2])] + terms[len(terms) // 2 * 2 :]
        return terms[0]

    def applied(values):
        return {i: dot({j: gram[i, j] for j in values}, values) for i in range(BASIS)}

    def mapped_by(values):
        found = {}
        for j, value in values.items():
            first, length = (0, S + 1) if j <= S else (S + 1, S)
            k = j - first
            if k == 0:
                entries = ((j, center), (j + 1, half_width))
            elif k < length - 1:
                entries = ((j - 1, half_width / 2), (j, center), (j + 1, half_width / 2))
            else:
                entries = ()
            for i, factor in entries:
                found[i] = found[i] + factor * value if i in found else factor * value
        return found

    def plus(one, factor, other):
        found = dict(one)
        for i, value in other.items():
            found[i] = found[i] + factor * value if i in found else factor * value
        return found

    unit = jnp.ones((TILE, LANES), jnp.float32)
    residue = {S + 1: unit}
    search = {0: unit}
    update = {}
    norm_now = dot(residue, applied(residue))
    for iteration in range(S):
        mapped = mapped_by(search)
        step_size = norm_now / dot(search, applied(mapped))
        update = plus(update, step_size, search)
        residue = plus(residue, -step_size, mapped)
        norm_next = dot(residue, applied(residue))
        search = plus(residue, norm_next / norm_now, search)
        norm_now = norm_next
    down = residue[0]
    for index in range(1, TILE):
        down = jnp.where(row == index, residue[index], down)
    last = jnp.sum(jnp.where((spot % RIM == 4) & (row < 2), table, 0.0), axis=0, keepdims=True)
    last = turn(jnp.broadcast_to(last, (TILE, LANES)), -4, 1)
    projected = jnp.sum(jnp.where(spot % RIM == 0, table, 0.0) * down, axis=0, keepdims=True)
    projected = projected + (last * residue[BASIS - 1])[:1]
    weights = jnp.sum(coupling[...] * projected, axis=1, keepdims=True)
    weights = jnp.broadcast_to(weights.astype(jnp.bfloat16).astype(jnp.float32), (RECYCLED, LANES))
    rows = delta_out.shape[1]
    for plane in range(delta_out.shape[0]):
        for start in range(0, rows, 2 * TILE):
            part = slice(start, start + 2 * TILE)
            found = [0.0, 0.0, 0.0]
            for field in range(BASIS):
                if field == 0:
                    values = direction[plane, part]
                elif field == S + 1:
                    values = residual[plane, part]
                else:
                    values = basis[field - 1 if field <= S else field - 2, plane, part]
                for index, coefficients in enumerate((update, residue, search)):
                    if field in coefficients:
                        factor = jnp.concatenate([coefficients[field]] * 2, axis=0)
                        found[index] = found[index] + factor * values
            correction = 0.0
            for vector in range(RECYCLED):
                correction = correction + weights[vector : vector + 1] * recycled[vector, plane, part].astype(
                    jnp.float32
                )
            delta_out[plane, part] = found[0]
            residual_out[plane, part] = found[1]
            direction_out[plane, part] = found[2] - correction


def shifted(values, shifts):
    axes = tuple(shifts)
    counts = [lax.axis_size(axis) for axis in axes]
    pairs = [(0, 0)]
    for axis, count in zip(axes, counts):
        pairs = [
            (source * count + i, target * count + (i + shifts[axis]) % count)
            for source, target in pairs
            for i in range(count)
        ]
    return lax.ppermute(values, axes, pairs)


def call(kernel, out_shape, operands, name, scratch=(), limit=16):
    in_vmem = pl.BlockSpec(memory_space=pltpu.VMEM)
    in_smem = pl.BlockSpec(memory_space=pltpu.SMEM)
    return pl.pallas_call(
        kernel,
        out_shape=tuple(jax.ShapeDtypeStruct(shape, jnp.float32) for shape in out_shape),
        in_specs=[in_smem if operand.dtype == jnp.int32 else in_vmem for operand in operands],
        out_specs=(in_vmem,) * len(out_shape),
        scratch_shapes=list(scratch),
        compiler_params=pltpu.CompilerParams(vmem_limit_bytes=limit * 1024 * 1024),
        name=name,
    )(*operands)


def body(residual, direction, diagonal, recycled, recycled_images, coupling_inverse):
    planes, rows, columns = residual.shape
    if columns != LANES or rows % 16 or RIM * (planes + 2 * S) != LANES or lax.axis_size("gy") % 2:
        raise ValueError("unsupported block")
    fields = (direction, residual, diagonal)
    reach = (S, S - 1, S - 1)
    upper = jnp.concatenate([field[planes - width :] for field, width in zip(fields, reach)])
    lower = jnp.concatenate([field[:width] for field, width in zip(fields, reach)])
    low = shifted(upper, {"gx": 1})
    high = shifted(lower, {"gx": -1})
    rim, rim_after, rim_before, coupling = call(
        rim_kernel,
        [(3, rows, LANES), (rows, LANES), (rows, LANES), (RECYCLED, LANES)],
        (*fields, coupling_inverse),
        "rim",
    )
    sides = (-1,) if lax.axis_size("gz") == 2 else (-1, 1)
    rims = [shifted(rim, {"gz": side}) for side in sides]
    low_rims = [shifted(rim_after, {"gx": 1, "gz": side}) for side in sides]
    high_rims = [shifted(rim_before, {"gx": -1, "gz": side}) for side in sides]
    parity = (lax.axis_index("gy") % 2).astype(jnp.int32).reshape(1)
    tiles = len(packing(planes))
    first, second, whole_rims = call(
        edge_kernel,
        [(tiles, TILE, LANES), (tiles, TILE, LANES), (3, rows, LANES)],
        (parity, *fields, low, high, rims[0], rims[-1], low_rims[0], low_rims[-1], high_rims[0], high_rims[-1]),
        "edge",
    )
    count = lax.axis_size("gy")
    first = lax.ppermute(first, "gy", [(i, i ^ 1) for i in range(count)])
    second = lax.ppermute(second, "gy", [(i, (i - 1 + 2 * (i % 2)) % count) for i in range(count)])
    devices = lax.axis_size(AXES)
    ring = rows + 2 * S
    pairs = 2 * planes + 2 * (S - 1) + 2 * (S - 2)
    basis, parts = call(
        basis_kernel,
        [(BASIS - 2, planes, rows, LANES), (devices, TILE, LANES)],
        (parity, *fields, low, high, whole_rims, first, second, recycled_images, *shift_matrices()),
        "basis",
        [
            pltpu.VMEM((S, planes + 2 * S, ring, LANES), jnp.float32),
            pltpu.VMEM((S - 1, planes + 2 * S, ring, LANES), jnp.float32),
            pltpu.VMEM((planes + 2 * S, ring, LANES), jnp.float32),
            pltpu.VMEM((pairs * ring, 4 * LANES), jnp.bfloat16),
        ],
    )
    parts = lax.all_to_all(parts, AXES, 0, 0)
    return call(
        finish_kernel,
        [residual.shape] * 3,
        (parts, coupling, direction, residual, basis, recycled),
        "finish",
    )


def solution(mesh):
    in_specs = (
        P("gx", "gy", "gz"),
        P("gx", "gy", "gz"),
        P("gx", "gy", "gz"),
        P(None, "gx", "gy", "gz"),
        P(None, "gx", "gy", "gz"),
        P(),
    )
    out_specs = (P("gx", "gy", "gz"), P("gx", "gy", "gz"), P("gx", "gy", "gz"))
    return jax.shard_map(body, mesh=mesh, in_specs=in_specs, out_specs=out_specs, check_vma=False)
```

```python
import jax
import jax.numpy as jnp
import numpy as np
from jax import lax
from jax.experimental import pallas as pl
from jax.experimental.pallas import tpu as pltpu
from jax.sharding import PartitionSpec as P

S = 4
BASIS = 9
RECYCLED = 16
LANES = 128
TILE = 8
AXES = ("gx", "gy", "gz")

RIM = 2 * S
SIDE = RIM * S


center = 7.25
half_width = 6.75


def lanes_of(rows):
    return lax.broadcasted_iota(jnp.int32, (rows, LANES), 1)


def rows_of(rows):
    return lax.broadcasted_iota(jnp.int32, (rows, LANES), 0)


def turn(values, shift, axis):
    shift = shift % values.shape[axis]
    return pltpu.roll(values, shift, axis) if shift else values


def rim_kernel(direction, residual, diagonal, coupling, ends, rim_out, after_out, before_out, coupling_out):
    planes, rows, _ = direction.shape
    slot = lanes_of(rows) // RIM
    after = jnp.zeros((rows, LANES), jnp.float32)
    before = jnp.zeros((rows, LANES), jnp.float32)
    for field, source in enumerate((direction, residual, diagonal)):
        values = source[...].reshape(planes * rows, LANES)
        copies = jnp.dot(jnp.concatenate(split(values), axis=1), ends[...], preferred_element_type=jnp.float32)
        rim = jnp.zeros((rows, LANES), jnp.float32)
        for plane in range(planes):
            here = copies[rows * plane : rows * (plane + 1)]
            rim = jnp.where(slot == plane + S, here, rim)
            if plane < S:
                before = jnp.where(slot == S * field + plane, here, before)
            if plane >= planes - S:
                after = jnp.where(slot == S * field + plane - planes + S, here, after)
        rim_out[field] = rim
    after_out[...] = after
    before_out[...] = before
    vector = lax.broadcasted_iota(jnp.int32, (RECYCLED, LANES), 0)
    spread = (lanes_of(RECYCLED) == 16 * (vector % 8) + 8 * (vector // 8)).astype(jnp.float32)
    coupling_out[...] = jnp.dot(
        coupling[...], spread, precision=lax.Precision.HIGHEST, preferred_element_type=jnp.float32
    )


def plane_of(own, low, high, field, x):
    planes = own.shape[0]
    first = (0, S, 2 * S - 1)[field]
    width = (S, S - 1, S - 1)[field]
    if x < 0:
        return low[first + width + x]
    if x >= planes:
        return high[first + x - planes]
    return own[x]


def packing(planes):
    pieces = []
    for field in range(3):
        reach = (S, S - 1, S - 1)[field]
        for x in range(1 - reach, planes + reach - 1):
            pieces.append((reach - max(0, -x, x - planes + 1), field, x))
        pieces.append((reach - 1, field, None))
    pieces.sort(key=lambda piece: -piece[0])
    tiles = []
    for count, field, x in pieces:
        for tile in tiles:
            used = sum(piece[0] for piece in tile)
            if used + count <= TILE:
                tile.append((count, field, x, used))
                break
        else:
            tiles.append([(count, field, x, 0)])
    return tiles


def edge_kernel(
    parity, direction, residual, diagonal, low, high, rim_next, rim_before, rim_low_next, rim_low_before, rim_high_next, rim_high_before, first_out, second_out, rim_out
):
    planes, rows, _ = direction.shape
    lane = lanes_of(rows)
    nearer = lane % RIM < S
    low_rim = jnp.where(nearer, rim_low_next[...], rim_low_before[...])
    high_rim = jnp.where(nearer, rim_high_next[...], rim_high_before[...])
    for field in range(3):
        rim = jnp.where(nearer, rim_next[field], rim_before[field])
        rim = jnp.where(lane < SIDE, turn(low_rim, -SIDE * field, 1), rim)
        rim = jnp.where(lane >= SIDE + RIM * planes, turn(high_rim, SIDE + RIM * planes - SIDE * field, 1), rim)
        rim_out[field] = rim
    fields = (direction, residual, diagonal)
    row = rows_of(TILE)

    even = parity[0] == 0
    for index, tile in enumerate(packing(planes)):
        lower = jnp.zeros((TILE, LANES), jnp.float32)
        upper = jnp.zeros((TILE, LANES), jnp.float32)
        for count, field, x, offset in tile:
            values = rim_out[field] if x is None else plane_of(fields[field], low, high, field, x)
            mine = (row >= offset) & (row < offset + count)
            lower = jnp.where(mine, turn(values[:TILE], offset, 0), lower)
            upper = jnp.where(mine, turn(values[rows - TILE :], offset + count, 0), upper)
        first_out[index] = jnp.where(even, upper, lower)
        second_out[index] = jnp.where(even, lower, upper)


def shift_matrices():
    source = np.arange(LANES)[:, None]
    target = np.arange(LANES)[None, :]
    along = np.abs(source - target) == 1
    last = (target % RIM == 0) & (source == LANES - 1)
    ends = last | ((target % RIM == RIM - 1) & (source == 0))
    facing = ((target == 0) & (source % RIM == RIM - 1)) | ((target == LANES - 1) & (source % RIM == 0))
    around = (np.abs(source - target) == RIM) | (along & (source // RIM == target // RIM))
    copies = source == np.where(target % RIM < S, target % RIM, LANES - RIM + target % RIM)
    inner = np.concatenate([along, ends], 1)
    outer = np.concatenate([facing, np.zeros_like(facing)], 1)
    matrices = ([inner, inner, outer, outer], [around, around], [copies, copies])
    return [jnp.asarray(np.concatenate(parts), jnp.bfloat16) for parts in matrices]


def split(values):
    leading = values.astype(jnp.bfloat16)
    return leading, (values - leading.astype(jnp.float32)).astype(jnp.bfloat16)


def products():
    found = []
    for one, other, count in ((0, 0, 2 * S + 1), (S + 1, S + 1, 2 * S - 1), (0, S + 1, 2 * S)):
        found.append([(one + (m + 1) // 2, other + m // 2) for m in range(count)])
    return found


def march(load, planes, ring, walk, trail, weight, left, shifts, rim_shifts, emit):
    lane = lanes_of(ring)

    def scaled(values):
        return (values - (center - 6.0)) * (2.0 / half_width)

    for x in range(1 - S, planes + S - 1):
        weight[x + S] = scaled(load(2, x))
    weight_rim = scaled(load(2, None))
    chains = ((0, walk, 0, S), (1, trail, S, S - 1))
    rim_levels = {}
    for field, history, offset, length in chains:
        for x in range(-length, planes + length):
            history[0, x + S] = load(field, x)
        rim_levels[field] = [load(field, None)]

    def advance(values, before, factor, beside):
        following = factor * values - (2.0 / half_width) * beside
        return 0.5 * following if before is None else following - before

    for level in range(S):
        work = []
        for field, history, offset, length in chains:
            reach = length - 1 - level
            if reach < 0:
                continue
            lead, rest = split(rim_levels[field][level])
            lead = lead.astype(jnp.float32)
            rest = rest.astype(jnp.float32)
            for x in range(-reach, planes + reach, 2):
                pair = jnp.concatenate([history[level, x + S], history[level, x + S + 1]], axis=0)
                parts = list(split(pair))
                for facing in (lead, rest):
                    slots = [jnp.where(lane // RIM == x + S + k, facing, 0.0) for k in range(2)]
                    parts.append(jnp.concatenate(slots, axis=0).astype(jnp.bfloat16))
                for index, part in enumerate(parts):
                    left[ring * len(work) : ring * (len(work) + 2), LANES * index : LANES * (index + 1)] = part
                work.append((field, history, offset, reach, x))
                work.append((field, history, offset, reach, x + 1))
        moved = jnp.dot(left[: ring * len(work)], shifts[...], preferred_element_type=jnp.float32)
        gathered = {}
        for index, (field, history, offset, reach, x) in enumerate(work):
            at = x + S
            here = moved[ring * index : ring * (index + 1)]
            values = history[level, at]
            beside = here[:, :LANES] + (history[level, at - 1] + history[level, at + 1])
            beside = beside + (turn(values, 1, 0) + turn(values, -1, 0))
            before = None if level == 0 else history[level - 1, at]
            following = advance(values, before, weight[at], beside)
            if 0 <= x < planes:
                emit(offset + level, x, following)
            if reach:
                history[level + 1, at] = following
                gathered[field] = jnp.where(lane // RIM == at, here[:, LANES:], gathered.get(field, 0.0))
        for field in gathered:
            levels = rim_levels[field]
            rim = levels[level]
            beside = jnp.dot(
                jnp.concatenate(split(rim), axis=1), rim_shifts[...], preferred_element_type=jnp.float32
            )
            beside = beside + (turn(rim, 1, 0) + turn(rim, -1, 0)) + gathered[field]
            levels.append(advance(rim, None if level == 0 else levels[level - 1], weight_rim, beside))


def inner_products(planes, tiles_of, images_of):
    families = products()
    sums = {}
    for x in range(planes):
        for tile in range(2):
            values = [tiles_of(index, x)[tile] for index in range(BASIS)]
            for family in families:
                for i, j in family:
                    product = values[i] * values[j]
                    sums[i, j] = sums[i, j] + product if (i, j) in sums else product
    half = 2 * TILE
    total = jnp.zeros((BASIS * half, RECYCLED * half), jnp.float32)
    for x in range(0, planes, 2):
        rounded = []
        for k in range(2):
            blocks = [jnp.concatenate(tiles_of(index, x + k), axis=0).astype(jnp.bfloat16) for index in range(BASIS)]
            rounded.append(jnp.concatenate(blocks, axis=0))
        against = [images_of(x + k).reshape(RECYCLED * half, LANES) for k in range(2)]
        total = total + lax.dot_general(
            jnp.concatenate(rounded, axis=1),
            jnp.concatenate(against, axis=1),
            (((1,), (1,)), ((), ())),
            preferred_element_type=jnp.float32,
        )
    wide = (BASIS * half, RECYCLED * half)
    same = lax.broadcasted_iota(jnp.int32, wide, 0) % half == lax.broadcasted_iota(jnp.int32, wide, 1) % half
    total = jnp.where(same, total, 0.0).reshape(BASIS, 2, TILE, RECYCLED * half)
    return sums, total[:, 0] + total[:, 1]


def inner_kernel(
    direction, residual, diagonal, low, high, rims, images, shifts, rim_shifts, basis_out, sums_out, total_out, walk, trail, weight, left
):
    planes, rows, _ = direction.shape
    fields = (direction, residual, diagonal)

    def load(field, x):
        return rims[field] if x is None else plane_of(fields[field], low, high, field, x)

    def emit(index, x, values):
        basis_out[index, x] = values

    march(load, planes, rows, walk, trail, weight, left, shifts, rim_shifts, emit)
    upper = lax.broadcasted_iota(jnp.int32, (RECYCLED, 2 * TILE, LANES), 1) < TILE

    def tiles_of(index, x):
        if index in (0, S + 1):
            values = fields[index > 0][x]
        else:
            values = basis_out[index - 1 if index <= S else index - 2, x]
        return values[rows - 2 * TILE : rows - TILE], values[TILE : 2 * TILE]

    def images_of(x):
        return jnp.where(upper, images[:, x, 2 * TILE :], images[:, x, : 2 * TILE])

    sums, total = inner_products(planes, tiles_of, images_of)
    for index, pair in enumerate(sorted(sums)):
        sums_out[index] = sums[pair]
    total_out[...] = total


def caps_kernel(
    parity, direction, residual, diagonal, low, high, rims, first, second, images, shifts, rim_shifts, basis, sums_in, total_in, caps_out, parts_out, walk, trail, weight, left
):
    planes, rows, _ = direction.shape
    ring = 3 * TILE
    fields = (direction, residual, diagonal)
    row = rows_of(TILE)
    even = parity[0] == 0
    halo = {}
    for index, tile in enumerate(packing(planes)):
        above = jnp.where(even, first[index], second[index])
        below = jnp.where(even, second[index], first[index])
        for count, field, x, offset in tile:
            halo[field, x] = jnp.where(row < S, turn(above, -offset, 0), turn(below, -offset - count, 0))
    nothing = jnp.zeros((TILE, LANES), jnp.float32)

    def load(field, x):
        values = rims[field] if x is None else plane_of(fields[field], low, high, field, x)
        return jnp.concatenate([values[rows - TILE :], halo.get((field, x), nothing), values[:TILE]], axis=0)

    def emit(index, x, values):
        caps_out[index, x, :TILE] = jnp.where(row < S, values[2 * TILE :], basis[index, x, :TILE])
        caps_out[index, x, TILE:] = jnp.where(row < S, basis[index, x, rows - TILE :], values[:TILE])

    march(load, planes, ring, walk, trail, weight, left, shifts, rim_shifts, emit)
    upper = lax.broadcasted_iota(jnp.int32, (RECYCLED, 2 * TILE, LANES), 1) < TILE

    def tiles_of(index, x):
        if index in (0, S + 1):
            values = fields[index > 0][x]
            return values[:TILE], values[rows - TILE :]
        values = caps_out[index - 1 if index <= S else index - 2, x]
        return values[:TILE], values[TILE:]

    def images_of(x):
        return jnp.where(upper, images[:, x, : 2 * TILE], images[:, x, 2 * TILE :])

    sums, total = inner_products(planes, tiles_of, images_of)
    for index, pair in enumerate(sorted(sums)):
        sums[pair] = sums[pair] + sums_in[index]
    total = total + total_in[...]
    spot = lanes_of(TILE)
    table = jnp.zeros((TILE, LANES), jnp.float32)
    other = jnp.zeros((TILE, LANES), jnp.float32)
    for index in range(BASIS):
        line = jnp.sum(total[index], axis=0, keepdims=True)
        if index < TILE:
            table = jnp.where(row == index, line[:, :LANES], table)
            other = jnp.where(row == index, line[:, LANES:], other)
    third = jnp.where(row == 0, line[:, :LANES], jnp.where(row == 1, line[:, LANES:], 0.0))
    blocks = jnp.concatenate([table, other, third], axis=0)
    for shift in (1, 2, 4, 8):
        blocks = blocks + turn(blocks, -shift, 1)
    table = jnp.where(spot % 16 == 0, blocks[:TILE], 0.0)
    table = jnp.where(spot % 16 == 8, turn(blocks[TILE : 2 * TILE], 8, 1), table)
    ninth = turn(blocks[2 * TILE :], 4, 1)
    table = jnp.where((row == 0) & (spot % 16 == 4), ninth, table)
    table = jnp.where((row == 1) & (spot % 16 == 12), turn(ninth, 8, 1), table)
    families = products()
    columns = [list(families[0][:TILE]), list(families[1]) + [families[0][TILE]], list(families[2])]
    for place, column in enumerate(columns):
        values = jnp.zeros((TILE, LANES), jnp.float32)
        for index, pair in enumerate(column):
            values = jnp.where(row == index, jnp.sum(sums[pair], axis=0, keepdims=True), values)
        values = jnp.sum(values, axis=1, keepdims=True)
        table = jnp.where(spot == RIM * place + 1, values, table)
    for device in range(parts_out.shape[0]):
        parts_out[device] = table


def moments_of(values):
    first = values[:2]
    return first + [2.0 * value - first[index % 2] for index, value in enumerate(values[2:])]


def finish_kernel(
    parts, coupling, direction, residual, basis, caps, recycled, delta_out, residual_out, direction_out, delta, left, ahead, done
):
    table = jnp.sum(parts[...], axis=0)
    spot = lanes_of(TILE)
    row = rows_of(TILE)
    columns = [
        jnp.broadcast_to(table[:, RIM * place + 1 : RIM * place + 2], (TILE, LANES)) for place in range(3)
    ]

    def spread(column, index):
        return jnp.broadcast_to(columns[column][index : index + 1], (TILE, LANES))

    walk = moments_of([spread(0, index) for index in range(TILE)] + [spread(1, TILE - 1)])
    trail = moments_of([spread(1, index) for index in range(2 * S - 1)])
    cross = moments_of([spread(2, index) for index in range(2 * S)])
    gram = {}
    for i in range(BASIS):
        for j in range(i, BASIS):
            source = walk if j <= S else (cross if i <= S else trail)
            one = i if i <= S else i - S - 1
            two = j if j <= S else j - S - 1
            gram[i, j] = gram[j, i] = 0.5 * (source[one + two] + source[abs(one - two)])

    def dot(one, other):
        terms = [one[i] * other[i] for i in one if i in other]
        while len(terms) > 1:
            terms = [a + b for a, b in zip(terms[::2], terms[1::2])] + terms[len(terms) // 2 * 2 :]
        return terms[0]

    def applied(values):
        return {i: dot({j: gram[i, j] for j in values}, values) for i in range(BASIS)}

    def mapped_by(values):
        found = {}
        for j, value in values.items():
            first, length = (0, S + 1) if j <= S else (S + 1, S)
            k = j - first
            if k == 0:
                entries = ((j, center), (j + 1, half_width))
            elif k < length - 1:
                entries = ((j - 1, half_width / 2), (j, center), (j + 1, half_width / 2))
            else:
                entries = ()
            for i, factor in entries:
                found[i] = found[i] + factor * value if i in found else factor * value
        return found

    def plus(one, factor, other):
        found = dict(one)
        for i, value in other.items():
            found[i] = found[i] + factor * value if i in found else factor * value
        return found

    unit = jnp.ones((TILE, LANES), jnp.float32)
    residue = {S + 1: unit}
    search = {0: unit}
    update = {}
    norm_now = dot(residue, applied(residue))
    for iteration in range(S):
        mapped = mapped_by(search)
        step_size = norm_now / dot(search, applied(mapped))
        update = plus(update, step_size, search)
        residue = plus(residue, -step_size, mapped)
        norm_next = dot(residue, applied(residue))
        search = plus(residue, norm_next / norm_now, search)
        norm_now = norm_next
    down = residue[0]
    for index in range(1, TILE):
        down = jnp.where(row == index, residue[index], down)
    last = jnp.sum(jnp.where((spot % RIM == 4) & (row < 2), table, 0.0), axis=0, keepdims=True)
    last = turn(jnp.broadcast_to(last, (TILE, LANES)), -4, 1)
    projected = jnp.sum(jnp.where(spot % RIM == 0, table, 0.0) * down, axis=0, keepdims=True)
    projected = projected + (last * residue[BASIS - 1])[:1]
    weights = jnp.sum(coupling[...] * projected, axis=1, keepdims=True)
    weights = jnp.broadcast_to(weights.astype(jnp.bfloat16).astype(jnp.float32), (RECYCLED, LANES))
    planes, rows, _ = direction.shape
    copies = []
    for plane in range(planes):
        for start in range(0, rows, 2 * TILE):
            part = slice(start, start + 2 * TILE)
            found = [0.0, 0.0, 0.0]
            for field in range(BASIS):
                if field in (0, S + 1):
                    values = (residual if field else direction)[plane, part]
                else:
                    at = field - 1 if field <= S else field - 2
                    if start == 0:
                        pieces = [caps[at, plane, :TILE], basis[at, plane, TILE : 2 * TILE]]
                    elif start + 2 * TILE == rows:
                        pieces = [basis[at, plane, start : start + TILE], caps[at, plane, TILE:]]
                    else:
                        pieces = [basis[at, plane, part]]
                    values = jnp.concatenate(pieces, axis=0)
                for index, coefficients in enumerate((update, residue, search)):
                    if field in coefficients:
                        factor = jnp.concatenate([coefficients[field]] * 2, axis=0)
                        found[index] = found[index] + factor * values
            correction = 0.0
            for vector in range(RECYCLED):
                correction = correction + weights[vector : vector + 1] * recycled[vector, plane, part].astype(
                    jnp.float32
                )
            delta[plane, part] = found[0]
            left[plane, part] = found[1]
            ahead[plane, part] = found[2] - correction
        if plane % 2:
            for index, (kept, out) in enumerate(((delta, delta_out), (left, residual_out), (ahead, direction_out))):
                chunk = pl.ds(plane - 1, 2)
                copy = pltpu.make_async_copy(kept.at[chunk], out.at[chunk], done.at[index, plane // 2])
                copy.start()
                copies.append(copy)
    for copy in copies:
        copy.wait()


def shifted(values, shifts):
    axes = tuple(shifts)
    counts = [lax.axis_size(axis) for axis in axes]
    pairs = [(0, 0)]
    for axis, count in zip(axes, counts):
        pairs = [
            (source * count + i, target * count + (i + shifts[axis]) % count)
            for source, target in pairs
            for i in range(count)
        ]
    return lax.ppermute(values, axes, pairs)


def call(kernel, out_shape, operands, name, scratch=(), limit=16, out_space=pltpu.VMEM):
    in_vmem = pl.BlockSpec(memory_space=pltpu.VMEM)
    in_smem = pl.BlockSpec(memory_space=pltpu.SMEM)
    return pl.pallas_call(
        kernel,
        out_shape=tuple(jax.ShapeDtypeStruct(shape, jnp.float32) for shape in out_shape),
        in_specs=[in_smem if operand.dtype == jnp.int32 else in_vmem for operand in operands],
        out_specs=(pl.BlockSpec(memory_space=out_space),) * len(out_shape),
        scratch_shapes=list(scratch),
        compiler_params=pltpu.CompilerParams(vmem_limit_bytes=limit * 1024 * 1024),
        name=name,
    )(*operands)


def body(residual, direction, diagonal, recycled, recycled_images, coupling_inverse):
    planes, rows, columns = residual.shape
    if columns != LANES or rows != 4 * TILE or RIM * (planes + 2 * S) != LANES or lax.axis_size("gy") % 2:
        raise ValueError("unsupported block")
    fields = (direction, residual, diagonal)
    reach = (S, S - 1, S - 1)
    shifts, rim_shifts, ends = shift_matrices()
    upper = jnp.concatenate([field[planes - width :] for field, width in zip(fields, reach)])
    lower = jnp.concatenate([field[:width] for field, width in zip(fields, reach)])
    low = shifted(upper, {"gx": 1})
    high = shifted(lower, {"gx": -1})
    rim, rim_after, rim_before, coupling = call(
        rim_kernel,
        [(3, rows, LANES), (rows, LANES), (rows, LANES), (RECYCLED, LANES)],
        (*fields, coupling_inverse, ends),
        "rim",
    )
    sides = (-1,) if lax.axis_size("gz") == 2 else (-1, 1)
    rims = [shifted(rim, {"gz": side}) for side in sides]
    low_rims = [shifted(rim_after, {"gx": 1, "gz": side}) for side in sides]
    high_rims = [shifted(rim_before, {"gx": -1, "gz": side}) for side in sides]
    parity = (lax.axis_index("gy") & 1).astype(jnp.int32).reshape(1)
    tiles = len(packing(planes))
    first, second, whole_rims = call(
        edge_kernel,
        [(tiles, TILE, LANES), (tiles, TILE, LANES), (3, rows, LANES)],
        (parity, *fields, low, high, rims[0], rims[-1], low_rims[0], low_rims[-1], high_rims[0], high_rims[-1]),
        "edge",
    )
    count = lax.axis_size("gy")
    first = lax.ppermute(first, "gy", [(i, i ^ 1) for i in range(count)])
    second = lax.ppermute(second, "gy", [(i, (i - 1 + 2 * (i % 2)) % count) for i in range(count)])
    devices = lax.axis_size(AXES)
    pairs = 2 * planes + 2 * (S - 1) + 2 * (S - 2)

    def scratch(ring):
        return [
            pltpu.VMEM((S, planes + 2 * S, ring, LANES), jnp.float32),
            pltpu.VMEM((S - 1, planes + 2 * S, ring, LANES), jnp.float32),
            pltpu.VMEM((planes + 2 * S, ring, LANES), jnp.float32),
            pltpu.VMEM((pairs * ring, 4 * LANES), jnp.bfloat16),
        ]

    count = sum(len(family) for family in products())
    basis, sums, total = call(
        inner_kernel,
        [(BASIS - 2, planes, rows, LANES), (count, TILE, LANES), (BASIS, TILE, 2 * LANES)],
        (*fields, low, high, whole_rims, recycled_images, shifts, rim_shifts),
        "inner",
        scratch(rows),
    )
    caps, parts = call(
        caps_kernel,
        [(BASIS - 2, planes, 2 * TILE, LANES), (devices, TILE, LANES)],
        (parity, *fields, low, high, whole_rims, first, second, recycled_images, shifts, rim_shifts, basis, sums, total),
        "caps",
        scratch(3 * TILE),
    )
    parts = lax.all_to_all(parts, AXES, 0, 0)
    return call(
        finish_kernel,
        [residual.shape] * 3,
        (parts, coupling, direction, residual, basis, caps, recycled),
        "finish",
        [pltpu.VMEM(residual.shape, jnp.float32)] * 3 + [pltpu.SemaphoreType.DMA((3, planes // 2))],
        out_space=pl.ANY,
    )


def solution(mesh):
    in_specs = (
        P("gx", "gy", "gz"),
        P("gx", "gy", "gz"),
        P("gx", "gy", "gz"),
        P(None, "gx", "gy", "gz"),
        P(None, "gx", "gy", "gz"),
        P(),
    )
    out_specs = (P("gx", "gy", "gz"), P("gx", "gy", "gz"), P("gx", "gy", "gz"))
    return jax.shard_map(body, mesh=mesh, in_specs=in_specs, out_specs=out_specs, check_vma=False)
```

```python
import jax
import jax.numpy as jnp
import numpy as np
from jax import lax
from jax.experimental import pallas as pl
from jax.experimental.pallas import tpu as pltpu
from jax.sharding import PartitionSpec as P

S = 4
BASIS = 9
RECYCLED = 16
LANES = 128
TILE = 8
AXES = ("gx", "gy", "gz")

RIM = 2 * S
SIDE = RIM * S


center = 7.25
half_width = 6.75


def lanes_of(rows):
    return lax.broadcasted_iota(jnp.int32, (rows, LANES), 1)


def rows_of(rows):
    return lax.broadcasted_iota(jnp.int32, (rows, LANES), 0)


def turn(values, shift, axis):
    shift = shift % values.shape[axis]
    return pltpu.roll(values, shift, axis) if shift else values


def load_kernel(
    direction_in, residual_in, diagonal_in, coupling_in, direction, residual, diagonal, upper, lower, coupling, done
):
    pairs = (
        (direction_in, direction, S),
        (residual_in, residual, S - 1),
        (diagonal_in, diagonal, S - 1),
        (coupling_in, coupling, 0),
    )
    copies = [pltpu.make_async_copy(source, kept, done.at[index]) for index, (source, kept, _) in enumerate(pairs)]
    for copy in copies:
        copy.start()
    planes = direction.shape[0]
    at = 0
    for copy, (_, kept, width) in zip(copies, pairs):
        copy.wait()
        if not width:
            continue
        upper[at : at + width] = kept[planes - width :]
        lower[at : at + width] = kept[:width]
        at += width


def rim_kernel(direction, residual, diagonal, coupling, rim_out, after_out, before_out, coupling_out):
    planes, rows, _ = direction.shape
    slot = lanes_of(rows) // RIM
    after = jnp.zeros((rows, LANES), jnp.float32)
    before = jnp.zeros((rows, LANES), jnp.float32)
    source = lax.broadcasted_iota(jnp.int32, (LANES, LANES), 0)
    target = lax.broadcasted_iota(jnp.int32, (LANES, LANES), 1) % RIM
    ends = (source == jnp.where(target < S, target, LANES - RIM + target)).astype(jnp.float32).astype(jnp.bfloat16)
    ends = jnp.concatenate([ends, ends], axis=0)
    for field, values in enumerate((direction, residual, diagonal)):
        values = values[...].reshape(planes * rows, LANES)
        copies = jnp.dot(jnp.concatenate(split(values), axis=1), ends, preferred_element_type=jnp.float32)
        rim = jnp.zeros((rows, LANES), jnp.float32)
        for plane in range(planes):
            here = copies[rows * plane : rows * (plane + 1)]
            rim = jnp.where(slot == plane + S, here, rim)
            if plane < S:
                before = jnp.where(slot == S * field + plane, here, before)
            if plane >= planes - S:
                after = jnp.where(slot == S * field + plane - planes + S, here, after)
        rim_out[field] = rim
    after_out[...] = after
    before_out[...] = before
    vector = lax.broadcasted_iota(jnp.int32, (RECYCLED, LANES), 0)
    spread = (lanes_of(RECYCLED) // TILE == vector).astype(jnp.float32)
    coupling_out[...] = jnp.dot(
        coupling[...], spread, precision=lax.Precision.HIGHEST, preferred_element_type=jnp.float32
    )


def plane_of(own, low, high, field, x):
    planes = own.shape[0]
    first = (0, S, 2 * S - 1)[field]
    width = (S, S - 1, S - 1)[field]
    if x < 0:
        return low[first + width + x]
    if x >= planes:
        return high[first + x - planes]
    return own[x]


def packing(planes):
    pieces = []
    for field in range(3):
        reach = (S, S - 1, S - 1)[field]
        for x in range(1 - reach, planes + reach - 1):
            pieces.append((reach - max(0, -x, x - planes + 1), field, x))
        pieces.append((reach - 1, field, None))
    pieces.sort(key=lambda piece: -piece[0])
    tiles = []
    for count, field, x in pieces:
        for tile in tiles:
            used = sum(piece[0] for piece in tile)
            if used + count <= TILE:
                tile.append((count, field, x, used))
                break
        else:
            tiles.append([(count, field, x, 0)])
    return tiles


def edge_kernel(
    parity, direction, residual, diagonal, low, high, rim_next, rim_before, rim_low_next, rim_low_before, rim_high_next, rim_high_before, first_out, second_out, rim_out
):
    planes, rows, _ = direction.shape
    lane = lanes_of(rows)
    nearer = lane % RIM < S
    low_rim = jnp.where(nearer, rim_low_next[...], rim_low_before[...])
    high_rim = jnp.where(nearer, rim_high_next[...], rim_high_before[...])
    for field in range(3):
        rim = jnp.where(nearer, rim_next[field], rim_before[field])
        rim = jnp.where(lane < SIDE, turn(low_rim, -SIDE * field, 1), rim)
        rim = jnp.where(lane >= SIDE + RIM * planes, turn(high_rim, SIDE + RIM * planes - SIDE * field, 1), rim)
        rim_out[field] = rim
    fields = (direction, residual, diagonal)
    row = rows_of(TILE)

    even = parity[0] == 0
    for index, tile in enumerate(packing(planes)):
        lower = jnp.zeros((TILE, LANES), jnp.float32)
        upper = jnp.zeros((TILE, LANES), jnp.float32)
        for count, field, x, offset in tile:
            values = rim_out[field] if x is None else plane_of(fields[field], low, high, field, x)
            mine = (row >= offset) & (row < offset + count)
            lower = jnp.where(mine, turn(values[:TILE], offset, 0), lower)
            upper = jnp.where(mine, turn(values[rows - TILE :], offset + count, 0), upper)
        first_out[index] = jnp.where(even, upper, lower)
        second_out[index] = jnp.where(even, lower, upper)


def shift_matrices():
    source = np.arange(LANES)[:, None]
    target = np.arange(LANES)[None, :]
    along = np.abs(source - target) == 1
    last = (target % RIM == 0) & (source == LANES - 1)
    ends = last | ((target % RIM == RIM - 1) & (source == 0))
    facing = ((target == 0) & (source % RIM == RIM - 1)) | ((target == LANES - 1) & (source % RIM == 0))
    around = (np.abs(source - target) == RIM) | (along & (source // RIM == target // RIM))
    groups = np.arange(2 * TILE * RECYCLED)[:, None] // (2 * TILE) == target // TILE
    inner = np.concatenate([along, ends], 1)
    outer = np.concatenate([facing, np.zeros_like(facing)], 1)
    matrices = ([inner, inner, outer, outer], [around, around], [groups, groups])
    return [jnp.asarray(np.concatenate(parts), jnp.bfloat16) for parts in matrices]


def split(values):
    leading = values.astype(jnp.bfloat16)
    return leading, (values - leading.astype(jnp.float32)).astype(jnp.bfloat16)


def products():
    found = []
    for one, other, count in ((0, 0, 2 * S + 1), (S + 1, S + 1, 2 * S - 1), (0, S + 1, 2 * S)):
        found.append([(one + (m + 1) // 2, other + m // 2) for m in range(count)])
    return found


def march(load, vertical, planes, ring, walk, trail, weight, left, shifts, rim_shifts, emit, keep):
    slot = lanes_of(ring) // RIM

    def scaled(values):
        return (values - (center - 6.0)) * (2.0 / half_width)

    for x in range(1 - S, planes + S - 1):
        weight[x + S] = scaled(load(2, x))
    weight_rim = scaled(load(2, None))
    chains = ((0, walk, 0, S), (1, trail, S, S - 1))
    rim_levels = {}
    for field, history, offset, length in chains:
        for x in range(-length, planes + length):
            history[0, x + S] = load(field, x)
        rim_levels[field] = [load(field, None)]
        keep(field, 0, rim_levels[field][0])

    def advance(values, before, factor, beside):
        following = factor * values - (2.0 / half_width) * beside
        return 0.5 * following if before is None else following - before

    for level in range(S):
        work = []
        for field, history, offset, length in chains:
            reach = length - 1 - level
            if reach < 0:
                continue
            facing = [part.astype(jnp.float32) for part in split(rim_levels[field][level])]
            for x in range(-reach, planes + reach):
                parts = list(split(history[level, x + S]))
                parts += [jnp.where(slot == x + S, part, 0.0).astype(jnp.bfloat16) for part in facing]
                for index, part in enumerate(parts):
                    left[ring * len(work) : ring * (len(work) + 1), LANES * index : LANES * (index + 1)] = part
                work.append((field, history, offset, reach, x))
        moved = jnp.dot(left[: ring * len(work)], shifts[...], preferred_element_type=jnp.float32)
        gathered = {}
        for index, (field, history, offset, reach, x) in enumerate(work):
            at = x + S
            here = moved[ring * index : ring * (index + 1)]
            values = history[level, at]
            beside = here[:, :LANES] + (history[level, at - 1] + history[level, at + 1])
            beside = beside + vertical(values, field, level, x)
            before = None if level == 0 else history[level - 1, at]
            following = advance(values, before, weight[at], beside)
            if 0 <= x < planes:
                emit(offset + level, x, following)
            if reach:
                history[level + 1, at] = following
                gathered[field] = jnp.where(slot == at, here[:, LANES:], gathered.get(field, 0.0))
        for field in gathered:
            levels = rim_levels[field]
            rim = levels[level]
            beside = jnp.dot(
                jnp.concatenate(split(rim), axis=1), rim_shifts[...], preferred_element_type=jnp.float32
            )
            beside = beside + vertical(rim, field, level, None) + gathered[field]
            levels.append(advance(rim, None if level == 0 else levels[level - 1], weight_rim, beside))
            keep(field, level + 1, levels[-1])


def inner_products(planes, tiles_of, images_of):
    families = products()
    sums = {}
    half = 2 * TILE
    total = jnp.zeros((BASIS * half, RECYCLED * half), jnp.float32)
    rounded = []
    against = []
    for x in range(planes):
        values = [tiles_of(index, x) for index in range(BASIS)]
        for tile in range(len(values[0])):
            if values[0][tile] is None:
                continue
            for family in families:
                for i, j in family:
                    product = values[i][tile] * values[j][tile]
                    sums[i, j] = sums[i, j] + product if (i, j) in sums else product
        nothing = jnp.zeros((TILE, LANES), jnp.float32)
        for block, images in enumerate(images_of(x)):
            pieces = [value[2 * block : 2 * block + 2] for value in values]
            pieces = [nothing if piece is None else piece for pair in pieces for piece in pair]
            rounded.append(jnp.concatenate(pieces, axis=0).astype(jnp.bfloat16))
            against.append(images.reshape(RECYCLED * half, LANES))
        if len(rounded) == 2:
            total = total + lax.dot_general(
                jnp.concatenate(rounded, axis=1),
                jnp.concatenate(against, axis=1),
                (((1,), (1,)), ((), ())),
                preferred_element_type=jnp.float32,
            )
            rounded = []
            against = []
    return sums, total


def inner_kernel(
    direction, residual, diagonal, low, high, rims, images, shifts, rim_shifts, basis_out, sums_out, total_out, walk, trail, rim_walk, rim_trail, weight, left
):
    planes, rows, _ = direction.shape
    fields = (direction, residual, diagonal)
    row = rows_of(TILE)

    def load(field, x):
        return rims[field] if x is None else plane_of(fields[field], low, high, field, x)

    def vertical(values, field, level, x):
        return turn(values, 1, 0) + turn(values, -1, 0)

    def emit(index, x, values):
        basis_out[index, x] = values

    def keep(field, level, values):
        (rim_trail if field else rim_walk)[level] = values

    march(load, vertical, planes, rows, walk, trail, weight, left, shifts, rim_shifts, emit, keep)

    def tiles_of(index, x):
        if index in (0, S + 1):
            values = fields[index > 0][x]
        else:
            values = basis_out[index - 1 if index <= S else index - 2, x]
        tiles = [values[start : start + TILE] for start in range(0, rows, TILE)]
        tiles[0] = jnp.where(row < S, 0.0, tiles[0])
        tiles[-1] = jnp.where(row < S, tiles[-1], 0.0)
        return tiles

    def images_of(x):
        return [images[:, x, start : start + 2 * TILE] for start in range(0, rows, 2 * TILE)]

    sums, total = inner_products(planes, tiles_of, images_of)
    for index, pair in enumerate(sorted(sums)):
        sums_out[index] = sums[pair]
    total_out[...] = total


def caps_kernel(
    parity, direction, residual, diagonal, low, high, rims, first, second, images, shifts, rim_shifts, groups, sums_in, total_in, inner_walk, inner_trail, inner_rim_walk, inner_rim_trail, caps_out, parts_out, walk, trail, weight, left
):
    planes, rows, _ = direction.shape
    ring = 2 * TILE
    fields = (direction, residual, diagonal)
    row = rows_of(TILE)
    near = row < S
    even = parity[0] == 0
    halo = {}
    for index, tile in enumerate(packing(planes)):
        above = jnp.where(even, first[index], second[index])
        below = jnp.where(even, second[index], first[index])
        for count, field, x, offset in tile:
            halo[field, x] = jnp.where(near, turn(above, -offset, 0), turn(below, -offset - count, 0))
    nothing = jnp.zeros((TILE, LANES), jnp.float32)

    def load(field, x):
        values = rims[field] if x is None else plane_of(fields[field], low, high, field, x)
        beyond = halo.get((field, x), nothing)
        return jnp.concatenate(
            [jnp.where(near, beyond, values[rows - TILE :]), jnp.where(near, values[:TILE], beyond)], axis=0
        )

    def vertical(values, field, level, x):
        if x is None:
            known = (inner_rim_trail if field else inner_rim_walk)[level]
        else:
            known = (inner_trail if field else inner_walk)[level, x + S]
        top = values[:TILE]
        bottom = values[TILE:]
        top_sum = turn(top, -1, 0) + turn(jnp.where(row == S - 1, known[rows - TILE :], top), 1, 0)
        bottom_sum = turn(jnp.where(row == S, known[:TILE], bottom), -1, 0) + turn(bottom, 1, 0)
        return jnp.concatenate([top_sum, bottom_sum], axis=0)

    def emit(index, x, values):
        caps_out[index, x] = jnp.where(near, values[TILE:], values[:TILE])

    march(load, vertical, planes, ring, walk, trail, weight, left, shifts, rim_shifts, emit, lambda *_: None)

    def tile_of(index, x):
        if index in (0, S + 1):
            values = fields[index > 0][x]
            return jnp.where(near, values[:TILE], values[rows - TILE :])
        return caps_out[index - 1 if index <= S else index - 2, x]

    upper = lax.broadcasted_iota(jnp.int32, (RECYCLED, 2 * TILE, LANES), 1) < TILE
    families = products()
    sums = {}
    half = 2 * TILE
    total = total_in[...]
    for x in range(0, planes, 2):
        rounded = []
        against = []
        for k in range(2):
            values = [tile_of(index, x + k) for index in range(BASIS)]
            for family in families:
                for i, j in family:
                    product = values[i] * values[j]
                    sums[i, j] = sums[i, j] + product if (i, j) in sums else product
            pieces = [
                piece for value in values for piece in (jnp.where(near, value, 0.0), jnp.where(near, 0.0, value))
            ]
            rounded.append(jnp.concatenate(pieces, axis=0).astype(jnp.bfloat16))
            images_here = jnp.where(upper, images[:, x + k, :half], images[:, x + k, rows - half :])
            against.append(images_here.reshape(RECYCLED * half, LANES))
        total = total + lax.dot_general(
            jnp.concatenate(rounded, axis=1),
            jnp.concatenate(against, axis=1),
            (((1,), (1,)), ((), ())),
            preferred_element_type=jnp.float32,
        )
    spot = lanes_of(TILE)
    columns = [list(families[0][:TILE]), list(families[1]) + [families[0][TILE]], list(families[2])]
    order = {pair: index for index, pair in enumerate(sorted(sums))}
    scalars = jnp.zeros((TILE, LANES), jnp.float32)
    for place, column in enumerate(columns):
        values = jnp.zeros((TILE, LANES), jnp.float32)
        for index, pair in enumerate(column):
            whole = sums[pair] + sums_in[order[pair]]
            values = jnp.where(row == index, jnp.sum(whole, axis=0, keepdims=True), values)
        values = jnp.sum(values, axis=1, keepdims=True)
        scalars = jnp.where((spot // TILE == row) & (spot % TILE == place + 1), values, scalars)
    wide = (BASIS * half, RECYCLED * half)
    same = lax.broadcasted_iota(jnp.int32, wide, 0) % half == lax.broadcasted_iota(jnp.int32, wide, 1) % half
    total = jnp.where(same, total, 0.0).reshape(BASIS, 2, TILE, RECYCLED * half)
    total = (total[:, 0] + total[:, 1]).reshape(BASIS * TILE, RECYCLED * half)
    lines = jnp.dot(jnp.concatenate(split(total), axis=1), groups[...], preferred_element_type=jnp.float32)
    mixed = jnp.zeros((TILE, LANES), jnp.float32)
    for index in range(TILE):
        mixed = jnp.where(spot % TILE == index, lines[TILE * index : TILE * (index + 1)], mixed)
    extra = jnp.where(spot % TILE == 0, lines[TILE * TILE :], scalars)
    table = jnp.concatenate(
        [jnp.sum(mixed, axis=0, keepdims=True), jnp.sum(extra, axis=0, keepdims=True)], axis=0
    )
    for device in range(parts_out.shape[0]):
        parts_out[device] = table


def moments_of(values):
    first = values[:2]
    return first + [2.0 * value - first[index % 2] for index, value in enumerate(values[2:])]


def finish_kernel(
    parts, coupling, direction, residual, basis, caps, recycled, delta_out, residual_out, direction_out
):
    table = jnp.sum(parts[...], axis=0)
    spot = lanes_of(TILE)
    row = rows_of(TILE)
    mixed = jnp.broadcast_to(table[:1], (TILE, LANES))
    extra = jnp.broadcast_to(table[1:], (TILE, LANES))
    columns = []
    for place in range(3):
        mine = (spot // TILE == row) & (spot % TILE == place + 1)
        column = jnp.sum(jnp.where(mine, extra, 0.0), axis=1, keepdims=True)
        columns.append(jnp.broadcast_to(column, (TILE, LANES)))

    def spread(column, index):
        return jnp.broadcast_to(columns[column][index : index + 1], (TILE, LANES))

    walk = moments_of([spread(0, index) for index in range(TILE)] + [spread(1, TILE - 1)])
    trail = moments_of([spread(1, index) for index in range(2 * S - 1)])
    cross = moments_of([spread(2, index) for index in range(2 * S)])
    gram = {}
    for i in range(BASIS):
        for j in range(i, BASIS):
            source = walk if j <= S else (cross if i <= S else trail)
            one = i if i <= S else i - S - 1
            two = j if j <= S else j - S - 1
            gram[i, j] = gram[j, i] = 0.5 * (source[one + two] + source[abs(one - two)])

    def dot(one, other):
        terms = [one[i] * other[i] for i in one if i in other]
        while len(terms) > 1:
            terms = [a + b for a, b in zip(terms[::2], terms[1::2])] + terms[len(terms) // 2 * 2 :]
        return terms[0]

    def applied(values):
        return {i: dot({j: gram[i, j] for j in values}, values) for i in range(BASIS)}

    def mapped_by(values):
        found = {}
        for j, value in values.items():
            first, length = (0, S + 1) if j <= S else (S + 1, S)
            k = j - first
            if k == 0:
                entries = ((j, center), (j + 1, half_width))
            elif k < length - 1:
                entries = ((j - 1, half_width / 2), (j, center), (j + 1, half_width / 2))
            else:
                entries = ()
            for i, factor in entries:
                found[i] = found[i] + factor * value if i in found else factor * value
        return found

    def plus(one, factor, other):
        found = dict(one)
        for i, value in other.items():
            found[i] = found[i] + factor * value if i in found else factor * value
        return found

    unit = jnp.ones((TILE, LANES), jnp.float32)
    residue = {S + 1: unit}
    search = {0: unit}
    update = {}
    norm_now = dot(residue, applied(residue))
    for iteration in range(S):
        mapped = mapped_by(search)
        step_size = norm_now / dot(search, applied(mapped))
        update = plus(update, step_size, search)
        residue = plus(residue, -step_size, mapped)
        norm_next = dot(residue, applied(residue))
        search = plus(residue, norm_next / norm_now, search)
        norm_now = norm_next
    across = residue[0]
    for index in range(1, TILE):
        across = jnp.where(spot % TILE == index, residue[index], across)
    projected = mixed * across + jnp.where(spot % TILE == 0, extra * residue[BASIS - 1], 0.0)
    projected = projected[:1]
    weights = jnp.sum(coupling[...] * projected, axis=1, keepdims=True)
    weights = jnp.broadcast_to(weights.astype(jnp.bfloat16).astype(jnp.float32), (RECYCLED, LANES))
    planes, rows, _ = direction.shape
    near = row < S
    for plane in range(planes):
        for start in range(0, rows, 2 * TILE):
            part = slice(start, start + 2 * TILE)
            found = [0.0, 0.0, 0.0]
            for field in range(BASIS):
                if field in (0, S + 1):
                    values = (residual if field else direction)[plane, part]
                else:
                    at = field - 1 if field <= S else field - 2
                    pieces = [basis[at, plane, start : start + TILE], basis[at, plane, start + TILE : start + 2 * TILE]]
                    if start == 0:
                        pieces[0] = jnp.where(near, caps[at, plane], pieces[0])
                    if start + 2 * TILE == rows:
                        pieces[1] = jnp.where(near, pieces[1], caps[at, plane])
                    values = jnp.concatenate(pieces, axis=0)
                for index, coefficients in enumerate((update, residue, search)):
                    if field in coefficients:
                        factor = jnp.concatenate([coefficients[field]] * 2, axis=0)
                        found[index] = found[index] + factor * values
            correction = 0.0
            for vector in range(RECYCLED):
                correction = correction + weights[vector : vector + 1] * recycled[vector, plane, part].astype(
                    jnp.float32
                )
            delta_out[plane, part] = found[0]
            residual_out[plane, part] = found[1]
            direction_out[plane, part] = found[2] - correction


def shifted(values, shifts):
    axes = tuple(shifts)
    counts = [lax.axis_size(axis) for axis in axes]
    pairs = [(0, 0)]
    for axis, count in zip(axes, counts):
        pairs = [
            (source * count + i, target * count + (i + shifts[axis]) % count)
            for source, target in pairs
            for i in range(count)
        ]
    return lax.ppermute(values, axes, pairs)


def call(kernel, out_shape, operands, name, scratch=(), limit=16, space=pltpu.VMEM):
    in_vmem = pl.BlockSpec(memory_space=pltpu.VMEM)
    in_smem = pl.BlockSpec(memory_space=pltpu.SMEM)
    given = pl.BlockSpec(memory_space=space)
    return pl.pallas_call(
        kernel,
        out_shape=tuple(jax.ShapeDtypeStruct(shape, jnp.float32) for shape in out_shape),
        in_specs=[in_smem if operand.dtype == jnp.int32 else given for operand in operands],
        out_specs=(in_vmem,) * len(out_shape),
        scratch_shapes=list(scratch),
        compiler_params=pltpu.CompilerParams(vmem_limit_bytes=limit * 1024 * 1024),
        name=name,
    )(*operands)


def body(residual, direction, diagonal, recycled, recycled_images, coupling_inverse):
    planes, rows, columns = residual.shape
    if columns != LANES or rows != 4 * TILE or RIM * (planes + 2 * S) != LANES or lax.axis_size("gy") % 2:
        raise ValueError("unsupported block")
    shape = residual.shape
    shifts, rim_shifts, groups = shift_matrices()
    slab = (3 * S - 2, rows, LANES)
    *fields, upper, lower, coupling = call(
        load_kernel,
        [shape] * 3 + [slab] * 2 + [coupling_inverse.shape],
        [pltpu.with_memory_space_constraint(value, pltpu.HBM) for value in (direction, residual, diagonal, coupling_inverse)],
        "load",
        [pltpu.SemaphoreType.DMA((4,))],
        space=pltpu.HBM,
    )
    low = shifted(upper, {"gx": 1})
    high = shifted(lower, {"gx": -1})
    rim, rim_after, rim_before, coupling = call(
        rim_kernel,
        [(3, rows, LANES), (rows, LANES), (rows, LANES), (RECYCLED, LANES)],
        (*fields, coupling),
        "rim",
    )
    sides = (-1,) if lax.axis_size("gz") == 2 else (-1, 1)
    rims = [shifted(rim, {"gz": side}) for side in sides]
    low_rims = [shifted(rim_after, {"gx": 1, "gz": side}) for side in sides]
    high_rims = [shifted(rim_before, {"gx": -1, "gz": side}) for side in sides]
    parity = (lax.axis_index("gy") & 1).astype(jnp.int32).reshape(1)
    tiles = len(packing(planes))
    first, second, whole_rims = call(
        edge_kernel,
        [(tiles, TILE, LANES), (tiles, TILE, LANES), (3, rows, LANES)],
        (parity, *fields, low, high, rims[0], rims[-1], low_rims[0], low_rims[-1], high_rims[0], high_rims[-1]),
        "edge",
    )
    count = lax.axis_size("gy")
    second = lax.ppermute(second, "gy", [(i, (i - 1 + 2 * (i % 2)) % count) for i in range(count)])
    first = lax.ppermute(first, "gy", [(i, i ^ 1) for i in range(count)])
    devices = lax.axis_size(AXES)
    wide = planes + 2 * S
    worked = 2 * planes + 2 * (S - 1) + 2 * (S - 2)

    def weights_and_left(ring):
        return [pltpu.VMEM((wide, ring, LANES), jnp.float32), pltpu.VMEM((worked * ring, 4 * LANES), jnp.bfloat16)]

    count = sum(len(family) for family in products())
    block = 2 * TILE
    basis, sums, total, *levels = call(
        inner_kernel,
        [
            (BASIS - 2, *shape),
            (count, TILE, LANES),
            (BASIS * block, RECYCLED * block),
            (S, wide, rows, LANES),
            (S - 1, wide, rows, LANES),
            (S, rows, LANES),
            (S - 1, rows, LANES),
        ],
        (*fields, low, high, whole_rims, recycled_images, shifts, rim_shifts),
        "inner",
        weights_and_left(rows),
    )
    caps, parts = call(
        caps_kernel,
        [(BASIS - 2, planes, TILE, LANES), (devices, 2, LANES)],
        (parity, *fields, low, high, whole_rims, first, second, recycled_images)
        + (shifts, rim_shifts, groups, sums, total, *levels),
        "caps",
        [pltpu.VMEM((S, wide, block, LANES), jnp.float32), pltpu.VMEM((S - 1, wide, block, LANES), jnp.float32)]
        + weights_and_left(block),
    )
    parts = lax.all_to_all(parts, AXES, 0, 0)
    return call(
        finish_kernel,
        [shape] * 3,
        (parts, coupling, fields[0], fields[1], basis, caps, recycled),
        "finish",
    )


def solution(mesh):
    in_specs = (
        P("gx", "gy", "gz"),
        P("gx", "gy", "gz"),
        P("gx", "gy", "gz"),
        P(None, "gx", "gy", "gz"),
        P(None, "gx", "gy", "gz"),
        P(),
    )
    out_specs = (P("gx", "gy", "gz"), P("gx", "gy", "gz"), P("gx", "gy", "gz"))
    return jax.shard_map(body, mesh=mesh, in_specs=in_specs, out_specs=out_specs, check_vma=False)
```

```python
import jax
import jax.numpy as jnp
import numpy as np
from jax import lax
from jax.experimental import pallas as pl
from jax.experimental.pallas import tpu as pltpu
from jax.sharding import PartitionSpec as P

S = 4
BASIS = 9
RECYCLED = 16
LANES = 128
TILE = 8
AXES = ("gx", "gy", "gz")

RIM = 2 * S
SIDE = RIM * S


center = 7.25
half_width = 6.75


def lanes_of(rows):
    return lax.broadcasted_iota(jnp.int32, (rows, LANES), 1)


def rows_of(rows):
    return lax.broadcasted_iota(jnp.int32, (rows, LANES), 0)


def turn(values, shift, axis):
    shift = shift % values.shape[axis]
    return pltpu.roll(values, shift, axis) if shift else values


def load_kernel(
    direction_in, residual_in, diagonal_in, coupling_in, direction, residual, diagonal, upper, lower, coupling, done
):
    pairs = (
        (direction_in, direction, S),
        (residual_in, residual, S - 1),
        (diagonal_in, diagonal, S - 1),
        (coupling_in, coupling, 0),
    )
    copies = [pltpu.make_async_copy(source, kept, done.at[index]) for index, (source, kept, _) in enumerate(pairs)]
    for copy in copies:
        copy.start()
    planes = direction.shape[0]
    at = 0
    for copy, (_, kept, width) in zip(copies, pairs):
        copy.wait()
        if not width:
            continue
        upper[at : at + width] = kept[planes - width :]
        lower[at : at + width] = kept[:width]
        at += width


def rim_kernel(direction, residual, diagonal, coupling, rim_out, after_out, before_out, coupling_out):
    planes, rows, _ = direction.shape
    slot = lanes_of(rows) // RIM
    after = jnp.zeros((rows, LANES), jnp.float32)
    before = jnp.zeros((rows, LANES), jnp.float32)
    source = lax.broadcasted_iota(jnp.int32, (LANES, LANES), 0)
    target = lax.broadcasted_iota(jnp.int32, (LANES, LANES), 1) % RIM
    ends = (source == jnp.where(target < S, target, LANES - RIM + target)).astype(jnp.float32).astype(jnp.bfloat16)
    ends = jnp.concatenate([ends, ends], axis=0)
    for field, values in enumerate((direction, residual, diagonal)):
        values = values[...].reshape(planes * rows, LANES)
        copies = jnp.dot(jnp.concatenate(split(values), axis=1), ends, preferred_element_type=jnp.float32)
        rim = jnp.zeros((rows, LANES), jnp.float32)
        for plane in range(planes):
            here = copies[rows * plane : rows * (plane + 1)]
            rim = jnp.where(slot == plane + S, here, rim)
            if plane < S:
                before = jnp.where(slot == S * field + plane, here, before)
            if plane >= planes - S:
                after = jnp.where(slot == S * field + plane - planes + S, here, after)
        rim_out[field] = rim
    after_out[...] = after
    before_out[...] = before
    vector = lax.broadcasted_iota(jnp.int32, (RECYCLED, LANES), 0)
    spread = (lanes_of(RECYCLED) // TILE == vector).astype(jnp.float32)
    coupling_out[...] = jnp.dot(
        coupling[...], spread, precision=lax.Precision.HIGHEST, preferred_element_type=jnp.float32
    )


def plane_of(own, low, high, field, x):
    planes = own.shape[0]
    first = (0, S, 2 * S - 1)[field]
    width = (S, S - 1, S - 1)[field]
    if x < 0:
        return low[first + width + x]
    if x >= planes:
        return high[first + x - planes]
    return own[x]


def packing(planes):
    pieces = []
    for field in range(3):
        reach = (S, S - 1, S - 1)[field]
        for x in range(1 - reach, planes + reach - 1):
            pieces.append((reach - max(0, -x, x - planes + 1), field, x))
        pieces.append((reach - 1, field, None))
    pieces.sort(key=lambda piece: -piece[0])
    tiles = []
    for count, field, x in pieces:
        for tile in tiles:
            used = sum(piece[0] for piece in tile)
            if used + count <= TILE:
                tile.append((count, field, x, used))
                break
        else:
            tiles.append([(count, field, x, 0)])
    return tiles


def edge_kernel(
    parity, direction, residual, diagonal, low, high, rim_next, rim_before, rim_low_next, rim_low_before, rim_high_next, rim_high_before, first_out, second_out, rim_out
):
    planes, rows, _ = direction.shape
    lane = lanes_of(rows)
    nearer = lane % RIM < S
    low_rim = jnp.where(nearer, rim_low_next[...], rim_low_before[...])
    high_rim = jnp.where(nearer, rim_high_next[...], rim_high_before[...])
    for field in range(3):
        rim = jnp.where(nearer, rim_next[field], rim_before[field])
        rim = jnp.where(lane < SIDE, turn(low_rim, -SIDE * field, 1), rim)
        rim = jnp.where(lane >= SIDE + RIM * planes, turn(high_rim, SIDE + RIM * planes - SIDE * field, 1), rim)
        rim_out[field] = rim
    fields = (direction, residual, diagonal)
    row = rows_of(TILE)

    even = parity[0] == 0
    for index, tile in enumerate(packing(planes)):
        lower = jnp.zeros((TILE, LANES), jnp.float32)
        upper = jnp.zeros((TILE, LANES), jnp.float32)
        for count, field, x, offset in tile:
            values = rim_out[field] if x is None else plane_of(fields[field], low, high, field, x)
            mine = (row >= offset) & (row < offset + count)
            lower = jnp.where(mine, turn(values[:TILE], offset, 0), lower)
            upper = jnp.where(mine, turn(values[rows - TILE :], offset + count, 0), upper)
        first_out[index] = jnp.where(even, upper, lower)
        second_out[index] = jnp.where(even, lower, upper)


def shift_matrices():
    source = np.arange(LANES)[:, None]
    target = np.arange(LANES)[None, :]
    along = np.abs(source - target) == 1
    last = (target % RIM == 0) & (source == LANES - 1)
    ends = last | ((target % RIM == RIM - 1) & (source == 0))
    facing = ((target == 0) & (source % RIM == RIM - 1)) | ((target == LANES - 1) & (source % RIM == 0))
    around = (np.abs(source - target) == RIM) | (along & (source // RIM == target // RIM))
    groups = np.arange(2 * TILE * RECYCLED)[:, None] // (2 * TILE) == target // TILE
    inner = np.concatenate([along, ends], 1)
    outer = np.concatenate([facing, np.zeros_like(facing)], 1)
    matrices = ([inner, inner, outer, outer], [around, around], [groups, groups, groups])
    return [jnp.asarray(np.concatenate(parts), jnp.bfloat16) for parts in matrices]


def split(values, count=2):
    terms = []
    for index in range(count):
        terms.append(values.astype(jnp.bfloat16))
        if index + 1 < count:
            values = values - terms[-1].astype(jnp.float32)
    return terms


def products():
    found = []
    for one, other, count in ((0, 0, 2 * S + 1), (S + 1, S + 1, 2 * S - 1), (0, S + 1, 2 * S)):
        found.append([(one + (m + 1) // 2, other + m // 2) for m in range(count)])
    return found


def march(load, vertical, planes, ring, walk, trail, weight, left, shifts, rim_shifts, emit, keep):
    slot = lanes_of(ring) // RIM

    def scaled(values):
        return (values - (center - 6.0)) * (2.0 / half_width)

    for x in range(1 - S, planes + S - 1):
        weight[x + S] = scaled(load(2, x))
    weight_rim = scaled(load(2, None))
    chains = ((0, walk, 0, S), (1, trail, S, S - 1))
    rim_levels = {}
    for field, history, offset, length in chains:
        for x in range(-length, planes + length):
            history[0, x + S] = load(field, x)
        rim_levels[field] = [load(field, None)]
        keep(field, 0, rim_levels[field][0])

    def advance(values, before, factor, beside):
        following = factor * values - (2.0 / half_width) * beside
        return 0.5 * following if before is None else following - before

    for level in range(S):
        work = []
        for field, history, offset, length in chains:
            reach = length - 1 - level
            if reach < 0:
                continue
            facing = [part.astype(jnp.float32) for part in split(rim_levels[field][level])]
            for x in range(-reach, planes + reach):
                parts = list(split(history[level, x + S]))
                parts += [jnp.where(slot == x + S, part, 0.0).astype(jnp.bfloat16) for part in facing]
                for index, part in enumerate(parts):
                    left[ring * len(work) : ring * (len(work) + 1), LANES * index : LANES * (index + 1)] = part
                work.append((field, history, offset, reach, x))
        moved = jnp.dot(left[: ring * len(work)], shifts[...], preferred_element_type=jnp.float32)
        gathered = {}
        for index, (field, history, offset, reach, x) in enumerate(work):
            at = x + S
            here = moved[ring * index : ring * (index + 1)]
            values = history[level, at]
            beside = here[:, :LANES] + (history[level, at - 1] + history[level, at + 1])
            beside = beside + vertical(values, field, level, x)
            before = None if level == 0 else history[level - 1, at]
            following = advance(values, before, weight[at], beside)
            if 0 <= x < planes:
                emit(offset + level, x, following)
            if reach:
                history[level + 1, at] = following
                gathered[field] = jnp.where(slot == at, here[:, LANES:], gathered.get(field, 0.0))
        for field in gathered:
            levels = rim_levels[field]
            rim = levels[level]
            beside = jnp.dot(
                jnp.concatenate(split(rim), axis=1), rim_shifts[...], preferred_element_type=jnp.float32
            )
            beside = beside + vertical(rim, field, level, None) + gathered[field]
            levels.append(advance(rim, None if level == 0 else levels[level - 1], weight_rim, beside))
            keep(field, level + 1, levels[-1])


def inner_products(planes, tiles_of, images_of):
    families = products()
    sums = {}
    half = 2 * TILE
    total = jnp.zeros((BASIS * half, RECYCLED * half), jnp.float32)
    rounded = []
    against = []
    for x in range(planes):
        values = [tiles_of(index, x) for index in range(BASIS)]
        for tile in range(len(values[0])):
            if values[0][tile] is None:
                continue
            for family in families:
                for i, j in family:
                    product = values[i][tile] * values[j][tile]
                    sums[i, j] = sums[i, j] + product if (i, j) in sums else product
        nothing = jnp.zeros((TILE, LANES), jnp.float32)
        for block, images in enumerate(images_of(x)):
            pieces = [value[2 * block : 2 * block + 2] for value in values]
            pieces = [nothing if piece is None else piece for pair in pieces for piece in pair]
            rounded.append(jnp.concatenate(pieces, axis=0).astype(jnp.bfloat16))
            against.append(images.reshape(RECYCLED * half, LANES))
        if len(rounded) == 2:
            total = total + lax.dot_general(
                jnp.concatenate(rounded, axis=1),
                jnp.concatenate(against, axis=1),
                (((1,), (1,)), ((), ())),
                preferred_element_type=jnp.float32,
            )
            rounded = []
            against = []
    return sums, total


def inner_kernel(
    direction, residual, diagonal, low, high, rims, shifts, rim_shifts, images_in, basis_out, sums_out, total_out, walk, trail, rim_walk, rim_trail, images, weight, left, done
):
    planes, rows, _ = direction.shape
    fields = (direction, residual, diagonal)
    row = rows_of(TILE)
    copy = pltpu.make_async_copy(images_in, images, done)
    copy.start()

    def load(field, x):
        return rims[field] if x is None else plane_of(fields[field], low, high, field, x)

    def vertical(values, field, level, x):
        return turn(values, 1, 0) + turn(values, -1, 0)

    def emit(index, x, values):
        basis_out[index, x] = values

    def keep(field, level, values):
        (rim_trail if field else rim_walk)[level] = values

    march(load, vertical, planes, rows, walk, trail, weight, left, shifts, rim_shifts, emit, keep)

    def tiles_of(index, x):
        if index in (0, S + 1):
            values = fields[index > 0][x]
        else:
            values = basis_out[index - 1 if index <= S else index - 2, x]
        tiles = [values[start : start + TILE] for start in range(0, rows, TILE)]
        tiles[0] = jnp.where(row < S, 0.0, tiles[0])
        tiles[-1] = jnp.where(row < S, tiles[-1], 0.0)
        return tiles

    copy.wait()

    def images_of(x):
        return [images[:, x, start : start + 2 * TILE] for start in range(0, rows, 2 * TILE)]

    sums, total = inner_products(planes, tiles_of, images_of)
    for index, pair in enumerate(sorted(sums)):
        sums_out[index] = sums[pair]
    total_out[...] = total


def caps_kernel(
    parity, direction, residual, diagonal, low, high, rims, first, second, images, shifts, rim_shifts, groups, sums_in, total_in, inner_walk, inner_trail, inner_rim_walk, inner_rim_trail, caps_out, parts_out, walk, trail, weight, left
):
    planes, rows, _ = direction.shape
    ring = 2 * TILE
    fields = (direction, residual, diagonal)
    row = rows_of(TILE)
    near = row < S
    even = parity[0] == 0
    halo = {}
    for index, tile in enumerate(packing(planes)):
        above = jnp.where(even, first[index], second[index])
        below = jnp.where(even, second[index], first[index])
        for count, field, x, offset in tile:
            halo[field, x] = jnp.where(near, turn(above, -offset, 0), turn(below, -offset - count, 0))
    nothing = jnp.zeros((TILE, LANES), jnp.float32)

    def load(field, x):
        values = rims[field] if x is None else plane_of(fields[field], low, high, field, x)
        beyond = halo.get((field, x), nothing)
        return jnp.concatenate(
            [jnp.where(near, beyond, values[rows - TILE :]), jnp.where(near, values[:TILE], beyond)], axis=0
        )

    def vertical(values, field, level, x):
        if x is None:
            known = (inner_rim_trail if field else inner_rim_walk)[level]
        else:
            known = (inner_trail if field else inner_walk)[level, x + S]
        top = values[:TILE]
        bottom = values[TILE:]
        top_sum = turn(top, -1, 0) + turn(jnp.where(row == S - 1, known[rows - TILE :], top), 1, 0)
        bottom_sum = turn(jnp.where(row == S, known[:TILE], bottom), -1, 0) + turn(bottom, 1, 0)
        return jnp.concatenate([top_sum, bottom_sum], axis=0)

    def emit(index, x, values):
        caps_out[index, x] = jnp.where(near, values[TILE:], values[:TILE])

    march(load, vertical, planes, ring, walk, trail, weight, left, shifts, rim_shifts, emit, lambda *_: None)

    def tile_of(index, x):
        if index in (0, S + 1):
            values = fields[index > 0][x]
            return jnp.where(near, values[:TILE], values[rows - TILE :])
        return caps_out[index - 1 if index <= S else index - 2, x]

    upper = lax.broadcasted_iota(jnp.int32, (RECYCLED, 2 * TILE, LANES), 1) < TILE
    families = products()
    sums = {}
    half = 2 * TILE
    total = total_in[...]
    for x in range(0, planes, 2):
        rounded = []
        against = []
        for k in range(2):
            values = [tile_of(index, x + k) for index in range(BASIS)]
            for family in families:
                for i, j in family:
                    product = values[i] * values[j]
                    sums[i, j] = sums[i, j] + product if (i, j) in sums else product
            pieces = [
                piece for value in values for piece in (jnp.where(near, value, 0.0), jnp.where(near, 0.0, value))
            ]
            rounded.append(jnp.concatenate(pieces, axis=0).astype(jnp.bfloat16))
            images_here = jnp.where(upper, images[:, x + k, :half], images[:, x + k, rows - half :])
            against.append(images_here.reshape(RECYCLED * half, LANES))
        total = total + lax.dot_general(
            jnp.concatenate(rounded, axis=1),
            jnp.concatenate(against, axis=1),
            (((1,), (1,)), ((), ())),
            preferred_element_type=jnp.float32,
        )
    spot = lanes_of(TILE)
    columns = [list(families[0][:TILE]), list(families[1]) + [families[0][TILE]], list(families[2])]
    order = {pair: index for index, pair in enumerate(sorted(sums))}
    scalars = jnp.zeros((TILE, LANES), jnp.float32)
    for place, column in enumerate(columns):
        values = jnp.zeros((TILE, LANES), jnp.float32)
        for index, pair in enumerate(column):
            whole = sums[pair] + sums_in[order[pair]]
            values = jnp.where(row == index, jnp.sum(whole, axis=0, keepdims=True), values)
        values = jnp.sum(values, axis=1, keepdims=True)
        scalars = jnp.where((spot // TILE == row) & (spot % TILE == place + 1), values, scalars)
    wide = (BASIS * half, RECYCLED * half)
    same = lax.broadcasted_iota(jnp.int32, wide, 0) % half == lax.broadcasted_iota(jnp.int32, wide, 1) % half
    total = jnp.where(same, total, 0.0).reshape(BASIS, 2, TILE, RECYCLED * half)
    total = (total[:, 0] + total[:, 1]).reshape(BASIS * TILE, RECYCLED * half)
    lines = jnp.dot(jnp.concatenate(split(total, 3), axis=1), groups[...], preferred_element_type=jnp.float32)
    mixed = jnp.zeros((TILE, LANES), jnp.float32)
    for index in range(TILE):
        mixed = jnp.where(spot % TILE == index, lines[TILE * index : TILE * (index + 1)], mixed)
    extra = jnp.where(spot % TILE == 0, lines[TILE * TILE :], scalars)
    table = jnp.concatenate(
        [jnp.sum(mixed, axis=0, keepdims=True), jnp.sum(extra, axis=0, keepdims=True)], axis=0
    )
    for device in range(parts_out.shape[0]):
        parts_out[device] = table


def moments_of(values):
    first = values[:2]
    return first + [2.0 * value - first[index % 2] for index, value in enumerate(values[2:])]


def finish_kernel(
    parts, coupling, direction, residual, basis, caps, recycled, delta_out, residual_out, direction_out
):
    table = jnp.sum(parts[...], axis=0)
    spot = lanes_of(TILE)
    row = rows_of(TILE)
    mixed = jnp.broadcast_to(table[:1], (TILE, LANES))
    extra = jnp.broadcast_to(table[1:], (TILE, LANES))
    columns = []
    for place in range(3):
        mine = (spot // TILE == row) & (spot % TILE == place + 1)
        column = jnp.sum(jnp.where(mine, extra, 0.0), axis=1, keepdims=True)
        columns.append(jnp.broadcast_to(column, (TILE, LANES)))

    def spread(column, index):
        return jnp.broadcast_to(columns[column][index : index + 1], (TILE, LANES))

    walk = moments_of([spread(0, index) for index in range(TILE)] + [spread(1, TILE - 1)])
    trail = moments_of([spread(1, index) for index in range(2 * S - 1)])
    cross = moments_of([spread(2, index) for index in range(2 * S)])
    gram = {}
    for i in range(BASIS):
        for j in range(i, BASIS):
            source = walk if j <= S else (cross if i <= S else trail)
            one = i if i <= S else i - S - 1
            two = j if j <= S else j - S - 1
            gram[i, j] = gram[j, i] = 0.5 * (source[one + two] + source[abs(one - two)])

    def dot(one, other):
        terms = [one[i] * other[i] for i in one if i in other]
        while len(terms) > 1:
            terms = [a + b for a, b in zip(terms[::2], terms[1::2])] + terms[len(terms) // 2 * 2 :]
        return terms[0]

    def applied(values):
        return {i: dot({j: gram[i, j] for j in values}, values) for i in range(BASIS)}

    def mapped_by(values):
        found = {}
        for j, value in values.items():
            first, length = (0, S + 1) if j <= S else (S + 1, S)
            k = j - first
            if k == 0:
                entries = ((j, center), (j + 1, half_width))
            elif k < length - 1:
                entries = ((j - 1, half_width / 2), (j, center), (j + 1, half_width / 2))
            else:
                entries = ()
            for i, factor in entries:
                found[i] = found[i] + factor * value if i in found else factor * value
        return found

    def plus(one, factor, other):
        found = dict(one)
        for i, value in other.items():
            found[i] = found[i] + factor * value if i in found else factor * value
        return found

    unit = jnp.ones((TILE, LANES), jnp.float32)
    residue = {S + 1: unit}
    search = {0: unit}
    update = {}
    norm_now = dot(residue, applied(residue))
    for _ in range(S):
        mapped = mapped_by(search)
        step_size = norm_now / dot(search, applied(mapped))
        update = plus(update, step_size, search)
        residue = plus(residue, -step_size, mapped)
        norm_next = dot(residue, applied(residue))
        search = plus(residue, norm_next / norm_now, search)
        norm_now = norm_next
    across = residue[0]
    for index in range(1, TILE):
        across = jnp.where(spot % TILE == index, residue[index], across)
    projected = mixed * across + jnp.where(spot % TILE == 0, extra * residue[BASIS - 1], 0.0)
    projected = projected[:1]
    weights = jnp.sum(coupling[...] * projected, axis=1, keepdims=True)
    weights = jnp.broadcast_to(weights.astype(jnp.bfloat16).astype(jnp.float32), (RECYCLED, LANES))
    planes, rows, _ = direction.shape
    near = row < S
    for plane in range(planes):
        for start in range(0, rows, 2 * TILE):
            part = slice(start, start + 2 * TILE)
            found = [0.0, 0.0, 0.0]
            for field in range(BASIS):
                if field in (0, S + 1):
                    values = (residual if field else direction)[plane, part]
                else:
                    at = field - 1 if field <= S else field - 2
                    pieces = [basis[at, plane, start : start + TILE], basis[at, plane, start + TILE : start + 2 * TILE]]
                    if start == 0:
                        pieces[0] = jnp.where(near, caps[at, plane], pieces[0])
                    if start + 2 * TILE == rows:
                        pieces[1] = jnp.where(near, pieces[1], caps[at, plane])
                    values = jnp.concatenate(pieces, axis=0)
                for index, coefficients in enumerate((update, residue, search)):
                    if field in coefficients:
                        factor = jnp.concatenate([coefficients[field]] * 2, axis=0)
                        found[index] = found[index] + factor * values
            correction = 0.0
            for vector in range(RECYCLED):
                correction = correction + weights[vector : vector + 1] * recycled[vector, plane, part].astype(
                    jnp.float32
                )
            delta_out[plane, part] = found[0]
            residual_out[plane, part] = found[1]
            direction_out[plane, part] = found[2] - correction


def shifted(values, shifts):
    axes = tuple(shifts)
    counts = [lax.axis_size(axis) for axis in axes]
    pairs = [(0, 0)]
    for axis, count in zip(axes, counts):
        pairs = [
            (source * count + i, target * count + (i + shifts[axis]) % count)
            for source, target in pairs
            for i in range(count)
        ]
    return lax.ppermute(values, axes, pairs)


def call(kernel, out_shape, operands, scratch=(), limit=16, in_hbm=()):
    in_vmem = pl.BlockSpec(memory_space=pltpu.VMEM)
    in_smem = pl.BlockSpec(memory_space=pltpu.SMEM)
    in_place = pl.BlockSpec(memory_space=pltpu.HBM)
    in_hbm = [pltpu.with_memory_space_constraint(operand, pltpu.HBM) for operand in in_hbm]
    out_shape = [shape if isinstance(shape, jax.ShapeDtypeStruct) else jax.ShapeDtypeStruct(shape, jnp.float32) for shape in out_shape]
    return pl.pallas_call(
        kernel,
        out_shape=tuple(out_shape),
        in_specs=[in_smem if operand.dtype == jnp.int32 else in_vmem for operand in operands] + [in_place] * len(in_hbm),
        out_specs=(in_vmem,) * len(out_shape),
        scratch_shapes=list(scratch),
        compiler_params=pltpu.CompilerParams(vmem_limit_bytes=limit * 1024 * 1024),
    )(*operands, *in_hbm)


def body(residual, direction, diagonal, recycled, recycled_images, coupling_inverse):
    planes, rows, columns = residual.shape
    if columns != LANES or rows != 4 * TILE or RIM * (planes + 2 * S) != LANES or lax.axis_size("gy") % 2:
        raise ValueError("unsupported block")
    shape = residual.shape
    shifts, rim_shifts, groups = shift_matrices()
    slab = (3 * S - 2, rows, LANES)
    *fields, upper, lower, coupling = call(
        load_kernel,
        [shape] * 3 + [slab] * 2 + [coupling_inverse.shape],
        (),
        [pltpu.SemaphoreType.DMA((4,))],
        in_hbm=(direction, residual, diagonal, coupling_inverse),
    )
    low = shifted(upper, {"gx": 1})
    high = shifted(lower, {"gx": -1})
    rim, rim_after, rim_before, coupling = call(
        rim_kernel, [(3, rows, LANES), (rows, LANES), (rows, LANES), (RECYCLED, LANES)], (*fields, coupling)
    )
    sides = (-1,) if lax.axis_size("gz") == 2 else (-1, 1)
    rims = [shifted(rim, {"gz": side}) for side in sides]
    low_rims = [shifted(rim_after, {"gx": 1, "gz": side}) for side in sides]
    high_rims = [shifted(rim_before, {"gx": -1, "gz": side}) for side in sides]
    parity = (lax.axis_index("gy") & 1).astype(jnp.int32).reshape(1)
    tiles = len(packing(planes))
    first, second, whole_rims = call(
        edge_kernel,
        [(tiles, TILE, LANES), (tiles, TILE, LANES), (3, rows, LANES)],
        (parity, *fields, low, high, rims[0], rims[-1], low_rims[0], low_rims[-1], high_rims[0], high_rims[-1]),
    )
    count = lax.axis_size("gy")
    second = lax.ppermute(second, "gy", [(i, (i - 1 + 2 * (i % 2)) % count) for i in range(count)])
    first = lax.ppermute(first, "gy", [(i, i ^ 1) for i in range(count)])
    devices = lax.axis_size(AXES)
    wide = planes + 2 * S
    worked = 2 * planes + 2 * (S - 1) + 2 * (S - 2)

    def weights_and_left(ring):
        return [pltpu.VMEM((wide, ring, LANES), jnp.float32), pltpu.VMEM((worked * ring, 4 * LANES), jnp.bfloat16)]

    count = sum(len(family) for family in products())
    block = 2 * TILE
    basis, sums, total, *levels, images = call(
        inner_kernel,
        [
            (BASIS - 2, *shape),
            (count, TILE, LANES),
            (BASIS * block, RECYCLED * block),
            (S, wide, rows, LANES),
            (S - 1, wide, rows, LANES),
            (S, rows, LANES),
            (S - 1, rows, LANES),
            jax.ShapeDtypeStruct(recycled_images.shape, recycled_images.dtype),
        ],
        (*fields, low, high, whole_rims, shifts, rim_shifts),
        weights_and_left(rows) + [pltpu.SemaphoreType.DMA],
        in_hbm=(recycled_images,),
    )
    caps, parts = call(
        caps_kernel,
        [(BASIS - 2, planes, TILE, LANES), (devices, 2, LANES)],
        (parity, *fields, low, high, whole_rims, first, second, images)
        + (shifts, rim_shifts, groups, sums, total, *levels),
        [pltpu.VMEM((S, wide, block, LANES), jnp.float32), pltpu.VMEM((S - 1, wide, block, LANES), jnp.float32)]
        + weights_and_left(block),
    )
    parts = lax.all_to_all(parts, AXES, 0, 0)
    return call(finish_kernel, [shape] * 3, (parts, coupling, fields[0], fields[1], basis, caps, recycled))


def solution(mesh):
    in_specs = (
        P("gx", "gy", "gz"),
        P("gx", "gy", "gz"),
        P("gx", "gy", "gz"),
        P(None, "gx", "gy", "gz"),
        P(None, "gx", "gy", "gz"),
        P(),
    )
    out_specs = (P("gx", "gy", "gz"), P("gx", "gy", "gz"), P("gx", "gy", "gz"))
    return jax.shard_map(body, mesh=mesh, in_specs=in_specs, out_specs=out_specs, check_vma=False)
```

```python
import jax
import jax.numpy as jnp
import numpy as np
from jax import lax
from jax.experimental import pallas as pl
from jax.experimental.pallas import tpu as pltpu
from jax.sharding import PartitionSpec as P

S = 4
BASIS = 9
RECYCLED = 16
LANES = 128
TILE = 8
AXES = ("gx", "gy", "gz")

RIM = 2 * S
SIDE = RIM * S


center = 7.25
half_width = 6.75


def lanes_of(rows):
    return lax.broadcasted_iota(jnp.int32, (rows, LANES), 1)


def rows_of(rows):
    return lax.broadcasted_iota(jnp.int32, (rows, LANES), 0)


def turn(values, shift, axis):
    shift = shift % values.shape[axis]
    return pltpu.roll(values, shift, axis) if shift else values


def load_kernel(
    direction_in, residual_in, diagonal_in, coupling_in, direction, residual, diagonal, upper, lower, coupling, done
):
    pairs = (
        (direction_in, direction, S),
        (residual_in, residual, S - 1),
        (diagonal_in, diagonal, S - 1),
        (coupling_in, coupling, 0),
    )
    copies = [pltpu.make_async_copy(source, kept, done.at[index]) for index, (source, kept, _) in enumerate(pairs)]
    for copy in copies:
        copy.start()
    planes = direction.shape[0]
    at = 0
    for copy, (_, kept, width) in zip(copies, pairs):
        copy.wait()
        if not width:
            continue
        upper[at : at + width] = kept[planes - width :]
        lower[at : at + width] = kept[:width]
        at += width


def rim_kernel(parity, direction, residual, diagonal, coupling, rim_out, outward_out, inward_out, coupling_out):
    planes, rows, _ = direction.shape
    slot = lanes_of(rows) // RIM
    after = jnp.zeros((rows, LANES), jnp.float32)
    before = jnp.zeros((rows, LANES), jnp.float32)
    source = lax.broadcasted_iota(jnp.int32, (LANES, LANES), 0)
    target = lax.broadcasted_iota(jnp.int32, (LANES, LANES), 1) % RIM
    ends = (source == jnp.where(target < S, target, LANES - RIM + target)).astype(jnp.float32).astype(jnp.bfloat16)
    ends = jnp.concatenate([ends, ends], axis=0)
    for field, values in enumerate((direction, residual, diagonal)):
        values = values[...].reshape(planes * rows, LANES)
        copies = jnp.dot(jnp.concatenate(split(values), axis=1), ends, preferred_element_type=jnp.float32)
        rim = jnp.zeros((rows, LANES), jnp.float32)
        for plane in range(planes):
            here = copies[rows * plane : rows * (plane + 1)]
            rim = jnp.where(slot == plane + S, here, rim)
            if plane < S:
                before = jnp.where(slot == S * field + plane, here, before)
            if plane >= planes - S:
                after = jnp.where(slot == S * field + plane - planes + S, here, after)
        rim_out[field] = rim
    even = parity[0] < 2
    outward_out[...] = jnp.where(even, before, after)
    inward_out[...] = jnp.where(even, after, before)
    vector = lax.broadcasted_iota(jnp.int32, (RECYCLED, LANES), 0)
    spread = (lanes_of(RECYCLED) // TILE == vector).astype(jnp.float32)
    coupling_out[...] = jnp.dot(
        coupling[...], spread, precision=lax.Precision.HIGHEST, preferred_element_type=jnp.float32
    )


def plane_of(own, low, high, field, x):
    planes = own.shape[0]
    first = (0, S, 2 * S - 1)[field]
    width = (S, S - 1, S - 1)[field]
    if x < 0:
        return low[first + width + x]
    if x >= planes:
        return high[first + x - planes]
    return own[x]


def packing(planes):
    pieces = []
    for field in range(3):
        reach = (S, S - 1, S - 1)[field]
        for x in range(1 - reach, planes + reach - 1):
            pieces.append((reach - max(0, -x, x - planes + 1), field, x))
        pieces.append((reach - 1, field, None))
    pieces.sort(key=lambda piece: -piece[0])
    tiles = []
    for count, field, x in pieces:
        for tile in tiles:
            used = sum(piece[0] for piece in tile)
            if used + count <= TILE:
                tile.append((count, field, x, used))
                break
        else:
            tiles.append([(count, field, x, 0)])
    return tiles


def edge_kernel(
    parity, direction, residual, diagonal, low, high, rim_next, rim_before, outward_next, outward_before, inward_next, inward_before, first_out, second_out, rim_out
):
    planes, rows, _ = direction.shape
    lane = lanes_of(rows)
    nearer = lane % RIM < S
    outward = jnp.where(nearer, outward_next[...], outward_before[...])
    inward = jnp.where(nearer, inward_next[...], inward_before[...])
    low_rim = jnp.where(parity[0] < 2, outward, inward)
    high_rim = jnp.where(parity[0] < 2, inward, outward)
    for field in range(3):
        rim = jnp.where(nearer, rim_next[field], rim_before[field])
        rim = jnp.where(lane < SIDE, turn(low_rim, -SIDE * field, 1), rim)
        rim = jnp.where(lane >= SIDE + RIM * planes, turn(high_rim, SIDE + RIM * planes - SIDE * field, 1), rim)
        rim_out[field] = rim
    fields = (direction, residual, diagonal)
    row = rows_of(TILE)

    even = parity[0] & 1 == 0
    for index, tile in enumerate(packing(planes)):
        lower = jnp.zeros((TILE, LANES), jnp.float32)
        upper = jnp.zeros((TILE, LANES), jnp.float32)
        for count, field, x, offset in tile:
            values = rim_out[field] if x is None else plane_of(fields[field], low, high, field, x)
            mine = (row >= offset) & (row < offset + count)
            lower = jnp.where(mine, turn(values[:TILE], offset, 0), lower)
            upper = jnp.where(mine, turn(values[rows - TILE :], offset + count, 0), upper)
        first_out[index] = jnp.where(even, upper, lower)
        second_out[index] = jnp.where(even, lower, upper)


def shift_matrices():
    source = np.arange(LANES)[:, None]
    target = np.arange(LANES)[None, :]
    along = np.abs(source - target) == 1
    last = (target % RIM == 0) & (source == LANES - 1)
    ends = last | ((target % RIM == RIM - 1) & (source == 0))
    facing = ((target == 0) & (source % RIM == RIM - 1)) | ((target == LANES - 1) & (source % RIM == 0))
    around = (np.abs(source - target) == RIM) | (along & (source // RIM == target // RIM))
    groups = np.arange(2 * TILE * RECYCLED)[:, None] // (2 * TILE) == target // TILE
    inner = np.concatenate([along, ends], 1)
    outer = np.concatenate([facing, np.zeros_like(facing)], 1)
    matrices = ([inner, inner, outer, outer], [around, around], [groups, groups, groups])
    return [jnp.asarray(np.concatenate(parts), jnp.bfloat16) for parts in matrices]


def split(values, count=2):
    terms = []
    for index in range(count):
        terms.append(values.astype(jnp.bfloat16))
        if index + 1 < count:
            values = values - terms[-1].astype(jnp.float32)
    return terms


def products():
    found = []
    for one, other, count in ((0, 0, 2 * S + 1), (S + 1, S + 1, 2 * S - 1), (0, S + 1, 2 * S)):
        found.append([(one + (m + 1) // 2, other + m // 2) for m in range(count)])
    return found


def march(load, vertical, planes, ring, walk, trail, weight, left, shifts, rim_shifts, emit, keep):
    slot = lanes_of(ring) // RIM

    def scaled(values):
        return (values - (center - 6.0)) * (2.0 / half_width)

    for x in range(1 - S, planes + S - 1):
        weight[x + S] = scaled(load(2, x))
    weight_rim = scaled(load(2, None))
    chains = ((0, walk, 0, S), (1, trail, S, S - 1))
    rim_levels = {}
    for field, history, offset, length in chains:
        for x in range(-length, planes + length):
            history[0, x + S] = load(field, x)
        rim_levels[field] = [load(field, None)]
        keep(field, 0, rim_levels[field][0])

    def advance(values, before, factor, beside):
        following = factor * values - (2.0 / half_width) * beside
        return 0.5 * following if before is None else following - before

    for level in range(S):
        work = []
        for field, history, offset, length in chains:
            reach = length - 1 - level
            if reach < 0:
                continue
            facing = [part.astype(jnp.float32) for part in split(rim_levels[field][level])]
            for x in range(-reach, planes + reach):
                parts = list(split(history[level, x + S]))
                parts += [jnp.where(slot == x + S, part, 0.0).astype(jnp.bfloat16) for part in facing]
                for index, part in enumerate(parts):
                    left[ring * len(work) : ring * (len(work) + 1), LANES * index : LANES * (index + 1)] = part
                work.append((field, history, offset, reach, x))
        moved = jnp.dot(left[: ring * len(work)], shifts[...], preferred_element_type=jnp.float32)
        gathered = {}
        for index, (field, history, offset, reach, x) in enumerate(work):
            at = x + S
            here = moved[ring * index : ring * (index + 1)]
            values = history[level, at]
            beside = here[:, :LANES] + (history[level, at - 1] + history[level, at + 1])
            beside = beside + vertical(values, field, level, x)
            before = None if level == 0 else history[level - 1, at]
            following = advance(values, before, weight[at], beside)
            if 0 <= x < planes:
                emit(offset + level, x, following)
            if reach:
                history[level + 1, at] = following
                gathered[field] = jnp.where(slot == at, here[:, LANES:], gathered.get(field, 0.0))
        for field in gathered:
            levels = rim_levels[field]
            rim = levels[level]
            beside = jnp.dot(
                jnp.concatenate(split(rim), axis=1), rim_shifts[...], preferred_element_type=jnp.float32
            )
            beside = beside + vertical(rim, field, level, None) + gathered[field]
            levels.append(advance(rim, None if level == 0 else levels[level - 1], weight_rim, beside))
            keep(field, level + 1, levels[-1])


def inner_products(planes, tiles_of, images_of):
    families = products()
    sums = {}
    half = 2 * TILE
    total = jnp.zeros((BASIS * half, RECYCLED * half), jnp.float32)
    rounded = []
    against = []
    for x in range(planes):
        values = [tiles_of(index, x) for index in range(BASIS)]
        for tile in range(len(values[0])):
            if values[0][tile] is None:
                continue
            for family in families:
                for i, j in family:
                    product = values[i][tile] * values[j][tile]
                    sums[i, j] = sums[i, j] + product if (i, j) in sums else product
        nothing = jnp.zeros((TILE, LANES), jnp.float32)
        for block, images in enumerate(images_of(x)):
            pieces = [value[2 * block : 2 * block + 2] for value in values]
            pieces = [nothing if piece is None else piece for pair in pieces for piece in pair]
            rounded.append(jnp.concatenate(pieces, axis=0).astype(jnp.bfloat16))
            against.append(images.reshape(RECYCLED * half, LANES))
        if len(rounded) == 2:
            total = total + lax.dot_general(
                jnp.concatenate(rounded, axis=1),
                jnp.concatenate(against, axis=1),
                (((1,), (1,)), ((), ())),
                preferred_element_type=jnp.float32,
            )
            rounded = []
            against = []
    return sums, total


def inner_kernel(
    direction, residual, diagonal, low, high, rims, shifts, rim_shifts, images_in, basis_out, sums_out, total_out, walk, trail, rim_walk, rim_trail, images, weight, left, done
):
    planes, rows, _ = direction.shape
    fields = (direction, residual, diagonal)
    row = rows_of(TILE)
    copy = pltpu.make_async_copy(images_in, images, done)
    copy.start()

    def load(field, x):
        return rims[field] if x is None else plane_of(fields[field], low, high, field, x)

    def vertical(values, field, level, x):
        return turn(values, 1, 0) + turn(values, -1, 0)

    def emit(index, x, values):
        basis_out[index, x] = values

    def keep(field, level, values):
        (rim_trail if field else rim_walk)[level] = values

    march(load, vertical, planes, rows, walk, trail, weight, left, shifts, rim_shifts, emit, keep)

    def tiles_of(index, x):
        if index in (0, S + 1):
            values = fields[index > 0][x]
        else:
            values = basis_out[index - 1 if index <= S else index - 2, x]
        tiles = [values[start : start + TILE] for start in range(0, rows, TILE)]
        tiles[0] = jnp.where(row < S, 0.0, tiles[0])
        tiles[-1] = jnp.where(row < S, tiles[-1], 0.0)
        return tiles

    copy.wait()

    def images_of(x):
        return [images[:, x, start : start + 2 * TILE] for start in range(0, rows, 2 * TILE)]

    sums, total = inner_products(planes, tiles_of, images_of)
    for index, pair in enumerate(sorted(sums)):
        sums_out[index] = sums[pair]
    total_out[...] = total


def caps_kernel(
    parity, direction, residual, diagonal, low, high, rims, first, second, images, shifts, rim_shifts, groups, sums_in, total_in, inner_walk, inner_trail, inner_rim_walk, inner_rim_trail, caps_out, parts_out, walk, trail, weight, left
):
    planes, rows, _ = direction.shape
    ring = 2 * TILE
    fields = (direction, residual, diagonal)
    row = rows_of(TILE)
    near = row < S
    even = parity[0] & 1 == 0
    halo = {}
    for index, tile in enumerate(packing(planes)):
        above = jnp.where(even, first[index], second[index])
        below = jnp.where(even, second[index], first[index])
        for count, field, x, offset in tile:
            halo[field, x] = jnp.where(near, turn(above, -offset, 0), turn(below, -offset - count, 0))
    nothing = jnp.zeros((TILE, LANES), jnp.float32)

    def load(field, x):
        values = rims[field] if x is None else plane_of(fields[field], low, high, field, x)
        beyond = halo.get((field, x), nothing)
        return jnp.concatenate(
            [jnp.where(near, beyond, values[rows - TILE :]), jnp.where(near, values[:TILE], beyond)], axis=0
        )

    def vertical(values, field, level, x):
        if x is None:
            known = (inner_rim_trail if field else inner_rim_walk)[level]
        else:
            known = (inner_trail if field else inner_walk)[level, x + S]
        top = values[:TILE]
        bottom = values[TILE:]
        top_sum = turn(top, -1, 0) + turn(jnp.where(row == S - 1, known[rows - TILE :], top), 1, 0)
        bottom_sum = turn(jnp.where(row == S, known[:TILE], bottom), -1, 0) + turn(bottom, 1, 0)
        return jnp.concatenate([top_sum, bottom_sum], axis=0)

    def emit(index, x, values):
        caps_out[index, x] = jnp.where(near, values[TILE:], values[:TILE])

    march(load, vertical, planes, ring, walk, trail, weight, left, shifts, rim_shifts, emit, lambda *_: None)

    def tile_of(index, x):
        if index in (0, S + 1):
            values = fields[index > 0][x]
            return jnp.where(near, values[:TILE], values[rows - TILE :])
        return caps_out[index - 1 if index <= S else index - 2, x]

    upper = lax.broadcasted_iota(jnp.int32, (RECYCLED, 2 * TILE, LANES), 1) < TILE
    families = products()
    sums = {}
    half = 2 * TILE
    total = total_in[...]
    for x in range(0, planes, 2):
        rounded = []
        against = []
        for k in range(2):
            values = [tile_of(index, x + k) for index in range(BASIS)]
            for family in families:
                for i, j in family:
                    product = values[i] * values[j]
                    sums[i, j] = sums[i, j] + product if (i, j) in sums else product
            pieces = [
                piece for value in values for piece in (jnp.where(near, value, 0.0), jnp.where(near, 0.0, value))
            ]
            rounded.append(jnp.concatenate(pieces, axis=0).astype(jnp.bfloat16))
            images_here = jnp.where(upper, images[:, x + k, :half], images[:, x + k, rows - half :])
            against.append(images_here.reshape(RECYCLED * half, LANES))
        total = total + lax.dot_general(
            jnp.concatenate(rounded, axis=1),
            jnp.concatenate(against, axis=1),
            (((1,), (1,)), ((), ())),
            preferred_element_type=jnp.float32,
        )
    spot = lanes_of(TILE)
    columns = [list(families[0][:TILE]), list(families[1]) + [families[0][TILE]], list(families[2])]
    order = {pair: index for index, pair in enumerate(sorted(sums))}
    scalars = jnp.zeros((TILE, LANES), jnp.float32)
    for place, column in enumerate(columns):
        values = jnp.zeros((TILE, LANES), jnp.float32)
        for index, pair in enumerate(column):
            whole = sums[pair] + sums_in[order[pair]]
            values = jnp.where(row == index, jnp.sum(whole, axis=0, keepdims=True), values)
        values = jnp.sum(values, axis=1, keepdims=True)
        scalars = jnp.where((spot // TILE == row) & (spot % TILE == place + 1), values, scalars)
    wide = (BASIS * half, RECYCLED * half)
    same = lax.broadcasted_iota(jnp.int32, wide, 0) % half == lax.broadcasted_iota(jnp.int32, wide, 1) % half
    total = jnp.where(same, total, 0.0).reshape(BASIS, 2, TILE, RECYCLED * half)
    total = (total[:, 0] + total[:, 1]).reshape(BASIS * TILE, RECYCLED * half)
    lines = jnp.dot(jnp.concatenate(split(total, 3), axis=1), groups[...], preferred_element_type=jnp.float32)
    mixed = jnp.zeros((TILE, LANES), jnp.float32)
    for index in range(TILE):
        mixed = jnp.where(spot % TILE == index, lines[TILE * index : TILE * (index + 1)], mixed)
    extra = jnp.where(spot % TILE == 0, lines[TILE * TILE :], scalars)
    table = jnp.concatenate(
        [jnp.sum(mixed, axis=0, keepdims=True), jnp.sum(extra, axis=0, keepdims=True)], axis=0
    )
    for device in range(parts_out.shape[0]):
        parts_out[device] = table


def moments_of(values):
    first = values[:2]
    return first + [2.0 * value - first[index % 2] for index, value in enumerate(values[2:])]


def finish_kernel(
    parts, coupling, direction, residual, basis, caps, recycled, delta_out, residual_out, direction_out
):
    table = jnp.sum(parts[...], axis=0)
    spot = lanes_of(TILE)
    row = rows_of(TILE)
    mixed = jnp.broadcast_to(table[:1], (TILE, LANES))
    extra = jnp.broadcast_to(table[1:], (TILE, LANES))
    columns = []
    for place in range(3):
        mine = (spot // TILE == row) & (spot % TILE == place + 1)
        column = jnp.sum(jnp.where(mine, extra, 0.0), axis=1, keepdims=True)
        columns.append(jnp.broadcast_to(column, (TILE, LANES)))

    def spread(column, index):
        return jnp.broadcast_to(columns[column][index : index + 1], (TILE, LANES))

    walk = moments_of([spread(0, index) for index in range(TILE)] + [spread(1, TILE - 1)])
    trail = moments_of([spread(1, index) for index in range(2 * S - 1)])
    cross = moments_of([spread(2, index) for index in range(2 * S)])
    gram = {}
    for i in range(BASIS):
        for j in range(i, BASIS):
            source = walk if j <= S else (cross if i <= S else trail)
            one = i if i <= S else i - S - 1
            two = j if j <= S else j - S - 1
            gram[i, j] = gram[j, i] = 0.5 * (source[one + two] + source[abs(one - two)])

    def dot(one, other):
        terms = [one[i] * other[i] for i in one if i in other]
        while len(terms) > 1:
            terms = [a + b for a, b in zip(terms[::2], terms[1::2])] + terms[len(terms) // 2 * 2 :]
        return terms[0]

    def applied(values):
        return {i: dot({j: gram[i, j] for j in values}, values) for i in range(BASIS)}

    def mapped_by(values):
        found = {}
        for j, value in values.items():
            first, length = (0, S + 1) if j <= S else (S + 1, S)
            k = j - first
            if k == 0:
                entries = ((j, center), (j + 1, half_width))
            elif k < length - 1:
                entries = ((j - 1, half_width / 2), (j, center), (j + 1, half_width / 2))
            else:
                entries = ()
            for i, factor in entries:
                found[i] = found[i] + factor * value if i in found else factor * value
        return found

    def plus(one, factor, other):
        found = dict(one)
        for i, value in other.items():
            found[i] = found[i] + factor * value if i in found else factor * value
        return found

    unit = jnp.ones((TILE, LANES), jnp.float32)
    residue = {S + 1: unit}
    search = {0: unit}
    update = {}
    norm_now = dot(residue, applied(residue))
    for _ in range(S):
        mapped = mapped_by(search)
        step_size = norm_now / dot(search, applied(mapped))
        update = plus(update, step_size, search)
        residue = plus(residue, -step_size, mapped)
        norm_next = dot(residue, applied(residue))
        search = plus(residue, norm_next / norm_now, search)
        norm_now = norm_next
    across = residue[0]
    for index in range(1, TILE):
        across = jnp.where(spot % TILE == index, residue[index], across)
    projected = mixed * across + jnp.where(spot % TILE == 0, extra * residue[BASIS - 1], 0.0)
    projected = projected[:1]
    weights = jnp.sum(coupling[...] * projected, axis=1, keepdims=True)
    weights = jnp.broadcast_to(weights.astype(jnp.bfloat16).astype(jnp.float32), (RECYCLED, LANES))
    planes, rows, _ = direction.shape
    near = row < S
    for plane in range(planes):
        for start in range(0, rows, 2 * TILE):
            part = slice(start, start + 2 * TILE)
            found = [0.0, 0.0, 0.0]
            for field in range(BASIS):
                if field in (0, S + 1):
                    values = (residual if field else direction)[plane, part]
                else:
                    at = field - 1 if field <= S else field - 2
                    pieces = [basis[at, plane, start : start + TILE], basis[at, plane, start + TILE : start + 2 * TILE]]
                    if start == 0:
                        pieces[0] = jnp.where(near, caps[at, plane], pieces[0])
                    if start + 2 * TILE == rows:
                        pieces[1] = jnp.where(near, pieces[1], caps[at, plane])
                    values = jnp.concatenate(pieces, axis=0)
                for index, coefficients in enumerate((update, residue, search)):
                    if field in coefficients:
                        factor = jnp.concatenate([coefficients[field]] * 2, axis=0)
                        found[index] = found[index] + factor * values
            correction = 0.0
            for vector in range(RECYCLED):
                correction = correction + weights[vector : vector + 1] * recycled[vector, plane, part].astype(
                    jnp.float32
                )
            delta_out[plane, part] = found[0]
            residual_out[plane, part] = found[1]
            direction_out[plane, part] = found[2] - correction


def onward(step):
    return lambda index, count: (index + step) % count


def inward(index, count):
    return index ^ 1


def outward(index, count):
    return (index - 1 + 2 * (index % 2)) % count


def moved(values, moves):
    axes = tuple(moves)
    pairs = [(0, 0)]
    for axis in axes:
        count = lax.axis_size(axis)
        pairs = [
            (source * count + i, target * count + moves[axis](i, count)) for source, target in pairs for i in range(count)
        ]
    return lax.ppermute(values, axes, pairs)


def call(kernel, out_shape, operands, scratch=(), limit=16, in_hbm=()):
    in_vmem = pl.BlockSpec(memory_space=pltpu.VMEM)
    in_smem = pl.BlockSpec(memory_space=pltpu.SMEM)
    in_place = pl.BlockSpec(memory_space=pltpu.HBM)
    in_hbm = [pltpu.with_memory_space_constraint(operand, pltpu.HBM) for operand in in_hbm]
    out_shape = [shape if isinstance(shape, jax.ShapeDtypeStruct) else jax.ShapeDtypeStruct(shape, jnp.float32) for shape in out_shape]
    return pl.pallas_call(
        kernel,
        out_shape=tuple(out_shape),
        in_specs=[in_smem if operand.dtype == jnp.int32 else in_vmem for operand in operands] + [in_place] * len(in_hbm),
        out_specs=(in_vmem,) * len(out_shape),
        scratch_shapes=list(scratch),
        compiler_params=pltpu.CompilerParams(vmem_limit_bytes=limit * 1024 * 1024),
    )(*operands, *in_hbm)


def body(residual, direction, diagonal, recycled, recycled_images, coupling_inverse):
    planes, rows, columns = residual.shape
    if columns != LANES or rows != 4 * TILE or RIM * (planes + 2 * S) != LANES or lax.axis_size("gx") % 2 or lax.axis_size("gy") % 2:
        raise ValueError("unsupported block")
    shape = residual.shape
    shifts, rim_shifts, groups = shift_matrices()
    slab = (3 * S - 2, rows, LANES)
    *fields, upper, lower, coupling = call(
        load_kernel,
        [shape] * 3 + [slab] * 2 + [coupling_inverse.shape],
        (),
        [pltpu.SemaphoreType.DMA((4,))],
        in_hbm=(direction, residual, diagonal, coupling_inverse),
    )
    parity = ((lax.axis_index("gy") & 1) + 2 * (lax.axis_index("gx") & 1)).astype(jnp.int32).reshape(1)
    low = moved(upper, {"gx": onward(1)})
    high = moved(lower, {"gx": onward(-1)})
    rim, rim_outward, rim_inward, coupling = call(
        rim_kernel, [(3, rows, LANES), (rows, LANES), (rows, LANES), (RECYCLED, LANES)], (parity, *fields, coupling)
    )
    sides = [onward(-1)] if lax.axis_size("gz") == 2 else [onward(-1), onward(1)]
    outward_rims = [moved(rim_outward, {"gx": outward, "gz": side}) for side in sides]
    rims = [moved(rim, {"gz": side}) for side in sides]
    inward_rims = [moved(rim_inward, {"gx": inward, "gz": side}) for side in sides]
    tiles = len(packing(planes))
    first, second, whole_rims = call(
        edge_kernel,
        [(tiles, TILE, LANES), (tiles, TILE, LANES), (3, rows, LANES)],
        (parity, *fields, low, high, rims[0], rims[-1], outward_rims[0], outward_rims[-1])
        + (inward_rims[0], inward_rims[-1]),
    )
    second = moved(second, {"gy": outward})
    first = moved(first, {"gy": inward})
    devices = lax.axis_size(AXES)
    wide = planes + 2 * S
    worked = 2 * planes + 2 * (S - 1) + 2 * (S - 2)

    def weights_and_left(ring):
        return [pltpu.VMEM((wide, ring, LANES), jnp.float32), pltpu.VMEM((worked * ring, 4 * LANES), jnp.bfloat16)]

    count = sum(len(family) for family in products())
    block = 2 * TILE
    basis, sums, total, *levels, images = call(
        inner_kernel,
        [
            (BASIS - 2, *shape),
            (count, TILE, LANES),
            (BASIS * block, RECYCLED * block),
            (S, wide, rows, LANES),
            (S - 1, wide, rows, LANES),
            (S, rows, LANES),
            (S - 1, rows, LANES),
            jax.ShapeDtypeStruct(recycled_images.shape, recycled_images.dtype),
        ],
        (*fields, low, high, whole_rims, shifts, rim_shifts),
        weights_and_left(rows) + [pltpu.SemaphoreType.DMA],
        in_hbm=(recycled_images,),
    )
    caps, parts = call(
        caps_kernel,
        [(BASIS - 2, planes, TILE, LANES), (devices, 2, LANES)],
        (parity, *fields, low, high, whole_rims, first, second, images)
        + (shifts, rim_shifts, groups, sums, total, *levels),
        [pltpu.VMEM((S, wide, block, LANES), jnp.float32), pltpu.VMEM((S - 1, wide, block, LANES), jnp.float32)]
        + weights_and_left(block),
    )
    parts = lax.all_to_all(parts, AXES, 0, 0)
    return call(finish_kernel, [shape] * 3, (parts, coupling, fields[0], fields[1], basis, caps, recycled))


def solution(mesh):
    in_specs = (
        P("gx", "gy", "gz"),
        P("gx", "gy", "gz"),
        P("gx", "gy", "gz"),
        P(None, "gx", "gy", "gz"),
        P(None, "gx", "gy", "gz"),
        P(),
    )
    out_specs = (P("gx", "gy", "gz"), P("gx", "gy", "gz"), P("gx", "gy", "gz"))
    return jax.shard_map(body, mesh=mesh, in_specs=in_specs, out_specs=out_specs, check_vma=False)
```

```python
import jax
import jax.numpy as jnp
import numpy as np
from jax import lax
from jax.experimental import pallas as pl
from jax.experimental.pallas import tpu as pltpu
from jax.sharding import PartitionSpec as P

S = 4
BASIS = 9
RECYCLED = 16
LANES = 128
TILE = 8
AXES = ("gx", "gy", "gz")

RIM = 2 * S
SIDE = RIM * S


center = 7.25
half_width = 6.75


def lanes_of(rows):
    return lax.broadcasted_iota(jnp.int32, (rows, LANES), 1)


def rows_of(rows):
    return lax.broadcasted_iota(jnp.int32, (rows, LANES), 0)


def turn(values, shift, axis):
    shift = shift % values.shape[axis]
    return pltpu.roll(values, shift, axis) if shift else values


def load_kernel(
    direction_in, residual_in, diagonal_in, coupling_in, direction, residual, diagonal, upper, lower, coupling, done
):
    pairs = (
        (direction_in, direction, S),
        (residual_in, residual, S - 1),
        (diagonal_in, diagonal, S - 1),
        (coupling_in, coupling, 0),
    )
    copies = [pltpu.make_async_copy(source, kept, done.at[index]) for index, (source, kept, _) in enumerate(pairs)]
    for copy in copies:
        copy.start()
    planes = direction.shape[0]
    at = 0
    for copy, (_, kept, width) in zip(copies, pairs):
        copy.wait()
        if not width:
            continue
        upper[at : at + width] = kept[planes - width :]
        lower[at : at + width] = kept[:width]
        at += width


def rim_kernel(parity, direction, residual, diagonal, coupling, rim_out, outward_out, inward_out, coupling_out):
    planes, rows, _ = direction.shape
    slot = lanes_of(rows) // RIM
    after = jnp.zeros((rows, LANES), jnp.float32)
    before = jnp.zeros((rows, LANES), jnp.float32)
    source = lax.broadcasted_iota(jnp.int32, (LANES, LANES), 0)
    target = lax.broadcasted_iota(jnp.int32, (LANES, LANES), 1) % RIM
    ends = (source == jnp.where(target < S, target, LANES - RIM + target)).astype(jnp.float32).astype(jnp.bfloat16)
    ends = jnp.concatenate([ends, ends], axis=0)
    for field, values in enumerate((direction, residual, diagonal)):
        values = values[...].reshape(planes * rows, LANES)
        copies = jnp.dot(jnp.concatenate(split(values), axis=1), ends, preferred_element_type=jnp.float32)
        rim = jnp.zeros((rows, LANES), jnp.float32)
        for plane in range(planes):
            here = copies[rows * plane : rows * (plane + 1)]
            rim = jnp.where(slot == plane + S, here, rim)
            if plane < S:
                before = jnp.where(slot == S * field + plane, here, before)
            if plane >= planes - S:
                after = jnp.where(slot == S * field + plane - planes + S, here, after)
        rim_out[field] = rim
    even = parity[0] & 2 == 0
    outward_out[...] = jnp.where(even, before, after)
    inward_out[...] = jnp.where(even, after, before)
    vector = lax.broadcasted_iota(jnp.int32, (RECYCLED, LANES), 0)
    spread = (lanes_of(RECYCLED) // TILE == vector).astype(jnp.float32)
    coupling_out[...] = jnp.dot(
        coupling[...], spread, precision=lax.Precision.HIGHEST, preferred_element_type=jnp.float32
    )


def plane_of(own, low, high, field, x):
    planes = own.shape[0]
    first = (0, S, 2 * S - 1)[field]
    width = (S, S - 1, S - 1)[field]
    if x < 0:
        return low[first + width + x]
    if x >= planes:
        return high[first + x - planes]
    return own[x]


def packing(planes):
    pieces = []
    for field in range(3):
        reach = (S, S - 1, S - 1)[field]
        for x in range(1 - reach, planes + reach - 1):
            pieces.append((reach - max(0, -x, x - planes + 1), field, x))
        pieces.append((reach - 1, field, None))
    pieces.sort(key=lambda piece: -piece[0])
    tiles = []
    for count, field, x in pieces:
        for tile in tiles:
            used = sum(piece[0] for piece in tile)
            if used + count <= TILE:
                tile.append((count, field, x, used))
                break
        else:
            tiles.append([(count, field, x, 0)])
    return tiles


def edge_kernel(
    parity, direction, residual, diagonal, low, high, rim_next, rim_before, outward_next, outward_before, inward_next, inward_before, first_out, second_out, rim_out
):
    planes, rows, _ = direction.shape
    lane = lanes_of(rows)
    nearer = lane % RIM < S
    outward = jnp.where(nearer, outward_next[...], outward_before[...])
    inward = jnp.where(nearer, inward_next[...], inward_before[...])
    low_rim = jnp.where(parity[0] & 2 == 0, outward, inward)
    high_rim = jnp.where(parity[0] & 2 == 0, inward, outward)
    for field in range(3):
        rim = jnp.where(nearer, rim_next[field], rim_before[field])
        rim = jnp.where(lane < SIDE, turn(low_rim, -SIDE * field, 1), rim)
        rim = jnp.where(lane >= SIDE + RIM * planes, turn(high_rim, SIDE + RIM * planes - SIDE * field, 1), rim)
        rim_out[field] = rim
    fields = (direction, residual, diagonal)
    row = rows_of(TILE)

    even = parity[0] & 1 == 0
    for index, tile in enumerate(packing(planes)):
        lower = jnp.zeros((TILE, LANES), jnp.float32)
        upper = jnp.zeros((TILE, LANES), jnp.float32)
        for count, field, x, offset in tile:
            values = rim_out[field] if x is None else plane_of(fields[field], low, high, field, x)
            mine = (row >= offset) & (row < offset + count)
            lower = jnp.where(mine, turn(values[:TILE], offset, 0), lower)
            upper = jnp.where(mine, turn(values[rows - TILE :], offset + count, 0), upper)
        first_out[index] = jnp.where(even, upper, lower)
        second_out[index] = jnp.where(even, lower, upper)


def shift_matrices():
    source = np.arange(LANES)[:, None]
    target = np.arange(LANES)[None, :]
    along = np.abs(source - target) == 1
    last = (target % RIM == 0) & (source == LANES - 1)
    ends = last | ((target % RIM == RIM - 1) & (source == 0))
    facing = ((target == 0) & (source % RIM == RIM - 1)) | ((target == LANES - 1) & (source % RIM == 0))
    around = (np.abs(source - target) == RIM) | (along & (source // RIM == target // RIM))
    groups = np.arange(2 * TILE * RECYCLED)[:, None] // (2 * TILE) == target // TILE
    inner = np.concatenate([along, ends], 1)
    outer = np.concatenate([facing, np.zeros_like(facing)], 1)
    matrices = ([inner, inner, outer, outer], [around, around], [groups, groups, groups])
    return [jnp.asarray(np.concatenate(parts), jnp.bfloat16) for parts in matrices]


def split(values, count=2):
    terms = []
    for index in range(count):
        terms.append(values.astype(jnp.bfloat16))
        if index + 1 < count:
            values = values - terms[-1].astype(jnp.float32)
    return terms


def products():
    found = []
    for one, other, count in ((0, 0, 2 * S + 1), (S + 1, S + 1, 2 * S - 1), (0, S + 1, 2 * S)):
        found.append([(one + (m + 1) // 2, other + m // 2) for m in range(count)])
    return found


def march(load, vertical, planes, ring, walk, trail, weight, left, shifts, rim_shifts, emit, keep):
    slot = lanes_of(ring) // RIM

    def scaled(values):
        return (values - (center - 6.0)) * (2.0 / half_width)

    for x in range(1 - S, planes + S - 1):
        weight[x + S] = scaled(load(2, x))
    weight_rim = scaled(load(2, None))
    chains = ((0, walk, 0, S), (1, trail, S, S - 1))
    rim_levels = {}
    for field, history, offset, length in chains:
        for x in range(-length, planes + length):
            history[0, x + S] = load(field, x)
        rim_levels[field] = [load(field, None)]
        keep(field, 0, rim_levels[field][0])

    def advance(values, before, factor, beside):
        following = factor * values - (2.0 / half_width) * beside
        return 0.5 * following if before is None else following - before

    for level in range(S):
        work = []
        for field, history, offset, length in chains:
            reach = length - 1 - level
            if reach < 0:
                continue
            facing = [part.astype(jnp.float32) for part in split(rim_levels[field][level])]
            for x in range(-reach, planes + reach):
                parts = list(split(history[level, x + S]))
                parts += [jnp.where(slot == x + S, part, 0.0).astype(jnp.bfloat16) for part in facing]
                for index, part in enumerate(parts):
                    left[ring * len(work) : ring * (len(work) + 1), LANES * index : LANES * (index + 1)] = part
                work.append((field, history, offset, reach, x))
        moved = jnp.dot(left[: ring * len(work)], shifts[...], preferred_element_type=jnp.float32)
        gathered = {}
        for index, (field, history, offset, reach, x) in enumerate(work):
            at = x + S
            here = moved[ring * index : ring * (index + 1)]
            values = history[level, at]
            beside = here[:, :LANES] + (history[level, at - 1] + history[level, at + 1])
            beside = beside + vertical(values, field, level, x)
            before = None if level == 0 else history[level - 1, at]
            following = advance(values, before, weight[at], beside)
            if 0 <= x < planes:
                emit(offset + level, x, following)
            if reach:
                history[level + 1, at] = following
                gathered[field] = jnp.where(slot == at, here[:, LANES:], gathered.get(field, 0.0))
        for field in gathered:
            levels = rim_levels[field]
            rim = levels[level]
            beside = jnp.dot(
                jnp.concatenate(split(rim), axis=1), rim_shifts[...], preferred_element_type=jnp.float32
            )
            beside = beside + vertical(rim, field, level, None) + gathered[field]
            levels.append(advance(rim, None if level == 0 else levels[level - 1], weight_rim, beside))
            keep(field, level + 1, levels[-1])


def inner_products(planes, tiles_of, images_of):
    families = products()
    sums = {}
    half = 2 * TILE
    total = jnp.zeros((BASIS * half, RECYCLED * half), jnp.float32)
    rounded = []
    against = []
    for x in range(planes):
        values = [tiles_of(index, x) for index in range(BASIS)]
        for tile in range(len(values[0])):
            if values[0][tile] is None:
                continue
            for family in families:
                for i, j in family:
                    product = values[i][tile] * values[j][tile]
                    sums[i, j] = sums[i, j] + product if (i, j) in sums else product
        nothing = jnp.zeros((TILE, LANES), jnp.float32)
        for block, images in enumerate(images_of(x)):
            pieces = [value[2 * block : 2 * block + 2] for value in values]
            pieces = [nothing if piece is None else piece for pair in pieces for piece in pair]
            rounded.append(jnp.concatenate(pieces, axis=0).astype(jnp.bfloat16))
            against.append(images.reshape(RECYCLED * half, LANES))
        if len(rounded) == 2:
            total = total + lax.dot_general(
                jnp.concatenate(rounded, axis=1),
                jnp.concatenate(against, axis=1),
                (((1,), (1,)), ((), ())),
                preferred_element_type=jnp.float32,
            )
            rounded = []
            against = []
    return sums, total


def steps_kernel(
    direction, residual, diagonal, low, high, rims, shifts, rim_shifts, images_in, basis_out, walk, trail, rim_walk, rim_trail, images, weight, left, done
):
    planes, rows, _ = direction.shape
    fields = (direction, residual, diagonal)
    copy = pltpu.make_async_copy(images_in, images, done)
    copy.start()

    def load(field, x):
        return rims[field] if x is None else plane_of(fields[field], low, high, field, x)

    def vertical(values, field, level, x):
        return turn(values, 1, 0) + turn(values, -1, 0)

    def emit(index, x, values):
        basis_out[index, x] = values

    def keep(field, level, values):
        (rim_trail if field else rim_walk)[level] = values

    march(load, vertical, planes, rows, walk, trail, weight, left, shifts, rim_shifts, emit, keep)
    copy.wait()


def products_kernel(direction, residual, basis, images, sums_out, total_out):
    planes, rows, _ = direction.shape
    row = rows_of(TILE)

    def tiles_of(index, x):
        if index in (0, S + 1):
            values = (residual if index else direction)[x]
        else:
            values = basis[index - 1 if index <= S else index - 2, x]
        tiles = [values[start : start + TILE] for start in range(0, rows, TILE)]
        tiles[0] = jnp.where(row < S, 0.0, tiles[0])
        tiles[-1] = jnp.where(row < S, tiles[-1], 0.0)
        return tiles

    def images_of(x):
        return [images[:, x, start : start + 2 * TILE] for start in range(0, rows, 2 * TILE)]

    sums, total = inner_products(planes, tiles_of, images_of)
    for index, pair in enumerate(sorted(sums)):
        sums_out[index] = sums[pair]
    total_out[...] = total


def caps_kernel(
    parity, direction, residual, diagonal, low, high, rims, first, second, wrapped, images, shifts, rim_shifts, groups, sums_in, total_in, inner_walk, inner_trail, inner_rim_walk, inner_rim_trail, caps_out, parts_out, walk, trail, weight, left
):
    planes, rows, _ = direction.shape
    ring = 2 * TILE
    fields = (direction, residual, diagonal)
    row = rows_of(TILE)
    near = row < S
    even = parity[0] & 1 == 0
    halo = {}
    at_end = parity[0] >= 4
    for index, tile in enumerate(packing(planes)):
        other = jnp.where(at_end, wrapped[index], second[index])
        above = jnp.where(even, first[index], other)
        below = jnp.where(even, other, first[index])
        for count, field, x, offset in tile:
            halo[field, x] = jnp.where(near, turn(above, -offset, 0), turn(below, -offset - count, 0))
    nothing = jnp.zeros((TILE, LANES), jnp.float32)

    def load(field, x):
        values = rims[field] if x is None else plane_of(fields[field], low, high, field, x)
        beyond = halo.get((field, x), nothing)
        return jnp.concatenate(
            [jnp.where(near, beyond, values[rows - TILE :]), jnp.where(near, values[:TILE], beyond)], axis=0
        )

    def vertical(values, field, level, x):
        if x is None:
            known = (inner_rim_trail if field else inner_rim_walk)[level]
        else:
            known = (inner_trail if field else inner_walk)[level, x + S]
        top = values[:TILE]
        bottom = values[TILE:]
        top_sum = turn(top, -1, 0) + turn(jnp.where(row == S - 1, known[rows - TILE :], top), 1, 0)
        bottom_sum = turn(jnp.where(row == S, known[:TILE], bottom), -1, 0) + turn(bottom, 1, 0)
        return jnp.concatenate([top_sum, bottom_sum], axis=0)

    def emit(index, x, values):
        caps_out[index, x] = jnp.where(near, values[TILE:], values[:TILE])

    march(load, vertical, planes, ring, walk, trail, weight, left, shifts, rim_shifts, emit, lambda *_: None)

    def tile_of(index, x):
        if index in (0, S + 1):
            values = fields[index > 0][x]
            return jnp.where(near, values[:TILE], values[rows - TILE :])
        return caps_out[index - 1 if index <= S else index - 2, x]

    upper = lax.broadcasted_iota(jnp.int32, (RECYCLED, 2 * TILE, LANES), 1) < TILE
    families = products()
    sums = {}
    half = 2 * TILE
    total = total_in[...]
    for x in range(0, planes, 2):
        rounded = []
        against = []
        for k in range(2):
            values = [tile_of(index, x + k) for index in range(BASIS)]
            for family in families:
                for i, j in family:
                    product = values[i] * values[j]
                    sums[i, j] = sums[i, j] + product if (i, j) in sums else product
            pieces = [
                piece for value in values for piece in (jnp.where(near, value, 0.0), jnp.where(near, 0.0, value))
            ]
            rounded.append(jnp.concatenate(pieces, axis=0).astype(jnp.bfloat16))
            images_here = jnp.where(upper, images[:, x + k, :half], images[:, x + k, rows - half :])
            against.append(images_here.reshape(RECYCLED * half, LANES))
        total = total + lax.dot_general(
            jnp.concatenate(rounded, axis=1),
            jnp.concatenate(against, axis=1),
            (((1,), (1,)), ((), ())),
            preferred_element_type=jnp.float32,
        )
    spot = lanes_of(TILE)
    columns = [list(families[0][:TILE]), list(families[1]) + [families[0][TILE]], list(families[2])]
    order = {pair: index for index, pair in enumerate(sorted(sums))}
    scalars = jnp.zeros((TILE, LANES), jnp.float32)
    for place, column in enumerate(columns):
        values = jnp.zeros((TILE, LANES), jnp.float32)
        for index, pair in enumerate(column):
            whole = sums[pair] + sums_in[order[pair]]
            values = jnp.where(row == index, jnp.sum(whole, axis=0, keepdims=True), values)
        values = jnp.sum(values, axis=1, keepdims=True)
        scalars = jnp.where((spot // TILE == row) & (spot % TILE == place + 1), values, scalars)
    wide = (BASIS * half, RECYCLED * half)
    same = lax.broadcasted_iota(jnp.int32, wide, 0) % half == lax.broadcasted_iota(jnp.int32, wide, 1) % half
    total = jnp.where(same, total, 0.0).reshape(BASIS, 2, TILE, RECYCLED * half)
    total = (total[:, 0] + total[:, 1]).reshape(BASIS * TILE, RECYCLED * half)
    lines = jnp.dot(jnp.concatenate(split(total, 3), axis=1), groups[...], preferred_element_type=jnp.float32)
    mixed = jnp.zeros((TILE, LANES), jnp.float32)
    for index in range(TILE):
        mixed = jnp.where(spot % TILE == index, lines[TILE * index : TILE * (index + 1)], mixed)
    extra = jnp.where(spot % TILE == 0, lines[TILE * TILE :], scalars)
    table = jnp.concatenate(
        [jnp.sum(mixed, axis=0, keepdims=True), jnp.sum(extra, axis=0, keepdims=True)], axis=0
    )
    for device in range(parts_out.shape[0]):
        parts_out[device] = table


def moments_of(values):
    first = values[:2]
    return first + [2.0 * value - first[index % 2] for index, value in enumerate(values[2:])]


def finish_kernel(
    parts, coupling, direction, residual, basis, caps, recycled, delta_out, residual_out, direction_out
):
    table = jnp.sum(parts[...], axis=0)
    spot = lanes_of(TILE)
    row = rows_of(TILE)
    mixed = jnp.broadcast_to(table[:1], (TILE, LANES))
    extra = jnp.broadcast_to(table[1:], (TILE, LANES))
    columns = []
    for place in range(3):
        mine = (spot // TILE == row) & (spot % TILE == place + 1)
        column = jnp.sum(jnp.where(mine, extra, 0.0), axis=1, keepdims=True)
        columns.append(jnp.broadcast_to(column, (TILE, LANES)))

    def spread(column, index):
        return jnp.broadcast_to(columns[column][index : index + 1], (TILE, LANES))

    walk = moments_of([spread(0, index) for index in range(TILE)] + [spread(1, TILE - 1)])
    trail = moments_of([spread(1, index) for index in range(2 * S - 1)])
    cross = moments_of([spread(2, index) for index in range(2 * S)])
    gram = {}
    for i in range(BASIS):
        for j in range(i, BASIS):
            source = walk if j <= S else (cross if i <= S else trail)
            one = i if i <= S else i - S - 1
            two = j if j <= S else j - S - 1
            gram[i, j] = gram[j, i] = 0.5 * (source[one + two] + source[abs(one - two)])

    def dot(one, other):
        terms = [one[i] * other[i] for i in one if i in other]
        while len(terms) > 1:
            terms = [a + b for a, b in zip(terms[::2], terms[1::2])] + terms[len(terms) // 2 * 2 :]
        return terms[0]

    def applied(values):
        return {i: dot({j: gram[i, j] for j in values}, values) for i in range(BASIS)}

    def mapped_by(values):
        found = {}
        for j, value in values.items():
            first, length = (0, S + 1) if j <= S else (S + 1, S)
            k = j - first
            if k == 0:
                entries = ((j, center), (j + 1, half_width))
            elif k < length - 1:
                entries = ((j - 1, half_width / 2), (j, center), (j + 1, half_width / 2))
            else:
                entries = ()
            for i, factor in entries:
                found[i] = found[i] + factor * value if i in found else factor * value
        return found

    def plus(one, factor, other):
        found = dict(one)
        for i, value in other.items():
            found[i] = found[i] + factor * value if i in found else factor * value
        return found

    unit = jnp.ones((TILE, LANES), jnp.float32)
    residue = {S + 1: unit}
    search = {0: unit}
    update = {}
    norm_now = dot(residue, applied(residue))
    for _ in range(S):
        mapped = mapped_by(search)
        step_size = norm_now / dot(search, applied(mapped))
        update = plus(update, step_size, search)
        residue = plus(residue, -step_size, mapped)
        norm_next = dot(residue, applied(residue))
        search = plus(residue, norm_next / norm_now, search)
        norm_now = norm_next
    across = residue[0]
    for index in range(1, TILE):
        across = jnp.where(spot % TILE == index, residue[index], across)
    projected = mixed * across + jnp.where(spot % TILE == 0, extra * residue[BASIS - 1], 0.0)
    projected = projected[:1]
    weights = jnp.sum(coupling[...] * projected, axis=1, keepdims=True)
    weights = jnp.broadcast_to(weights.astype(jnp.bfloat16).astype(jnp.float32), (RECYCLED, LANES))
    planes, rows, _ = direction.shape
    near = row < S
    for plane in range(planes):
        for start in range(0, rows, 2 * TILE):
            part = slice(start, start + 2 * TILE)
            found = [0.0, 0.0, 0.0]
            for field in range(BASIS):
                if field in (0, S + 1):
                    values = (residual if field else direction)[plane, part]
                else:
                    at = field - 1 if field <= S else field - 2
                    pieces = [basis[at, plane, start : start + TILE], basis[at, plane, start + TILE : start + 2 * TILE]]
                    if start == 0:
                        pieces[0] = jnp.where(near, caps[at, plane], pieces[0])
                    if start + 2 * TILE == rows:
                        pieces[1] = jnp.where(near, pieces[1], caps[at, plane])
                    values = jnp.concatenate(pieces, axis=0)
                for index, coefficients in enumerate((update, residue, search)):
                    if field in coefficients:
                        factor = jnp.concatenate([coefficients[field]] * 2, axis=0)
                        found[index] = found[index] + factor * values
            correction = 0.0
            for vector in range(RECYCLED):
                correction = correction + weights[vector : vector + 1] * recycled[vector, plane, part].astype(
                    jnp.float32
                )
            delta_out[plane, part] = found[0]
            residual_out[plane, part] = found[1]
            direction_out[plane, part] = found[2] - correction


def onward(step):
    return lambda index, count: (index + step) % count


def inward(index, count):
    return index ^ 1


def outward(index, count):
    return (index - 1 + 2 * (index % 2)) % count


def moved(values, moves):
    axes = tuple(moves)
    pairs = [(0, 0)]
    for axis in axes:
        count = lax.axis_size(axis)
        pairs = [
            (source * count + i, target * count + moves[axis](i, count)) for source, target in pairs for i in range(count)
        ]
    return lax.ppermute(values, axes, pairs)


def call(kernel, out_shape, operands, scratch=(), limit=16, in_hbm=()):
    in_vmem = pl.BlockSpec(memory_space=pltpu.VMEM)
    in_smem = pl.BlockSpec(memory_space=pltpu.SMEM)
    in_place = pl.BlockSpec(memory_space=pltpu.HBM)
    in_hbm = [pltpu.with_memory_space_constraint(operand, pltpu.HBM) for operand in in_hbm]
    out_shape = [shape if isinstance(shape, jax.ShapeDtypeStruct) else jax.ShapeDtypeStruct(shape, jnp.float32) for shape in out_shape]
    return pl.pallas_call(
        kernel,
        out_shape=tuple(out_shape),
        in_specs=[in_smem if operand.dtype == jnp.int32 else in_vmem for operand in operands] + [in_place] * len(in_hbm),
        out_specs=(in_vmem,) * len(out_shape),
        scratch_shapes=list(scratch),
        compiler_params=pltpu.CompilerParams(vmem_limit_bytes=limit * 1024 * 1024),
    )(*operands, *in_hbm)


def body(residual, direction, diagonal, recycled, recycled_images, coupling_inverse):
    planes, rows, columns = residual.shape
    if columns != LANES or rows != 4 * TILE or RIM * (planes + 2 * S) != LANES or lax.axis_size("gx") % 2 or lax.axis_size("gy") % 4:
        raise ValueError("unsupported block")
    shape = residual.shape
    shifts, rim_shifts, groups = shift_matrices()
    slab = (3 * S - 2, rows, LANES)
    *fields, upper, lower, coupling = call(
        load_kernel,
        [shape] * 3 + [slab] * 2 + [coupling_inverse.shape],
        (),
        [pltpu.SemaphoreType.DMA((4,))],
        in_hbm=(direction, residual, diagonal, coupling_inverse),
    )
    count = lax.axis_size("gy")
    y = lax.axis_index("gy")
    at_end = 4 * ((y == 0) | (y == count - 1)).astype(jnp.int32)
    parity = ((y & 1) + 2 * (lax.axis_index("gx") & 1) + at_end).astype(jnp.int32).reshape(1)
    low = moved(upper, {"gx": onward(1)})
    high = moved(lower, {"gx": onward(-1)})
    rim, rim_outward, rim_inward, coupling = call(
        rim_kernel, [(3, rows, LANES), (rows, LANES), (rows, LANES), (RECYCLED, LANES)], (parity, *fields, coupling)
    )
    sides = [onward(-1)] if lax.axis_size("gz") == 2 else [onward(-1), onward(1)]
    outward_rims = [moved(rim_outward, {"gx": outward, "gz": side}) for side in sides]
    rims = [moved(rim, {"gz": side}) for side in sides]
    inward_rims = [moved(rim_inward, {"gx": inward, "gz": side}) for side in sides]
    tiles = len(packing(planes))
    first, second, whole_rims = call(
        edge_kernel,
        [(tiles, TILE, LANES), (tiles, TILE, LANES), (3, rows, LANES)],
        (parity, *fields, low, high, rims[0], rims[-1], outward_rims[0], outward_rims[-1])
        + (inward_rims[0], inward_rims[-1]),
    )
    wide = planes + 2 * S
    worked = 2 * planes + 2 * (S - 1) + 2 * (S - 2)

    def weights_and_left(ring):
        return [pltpu.VMEM((wide, ring, LANES), jnp.float32), pltpu.VMEM((worked * ring, 4 * LANES), jnp.bfloat16)]

    wrapped = lax.ppermute(second, "gy", [(0, count - 1), (count - 1, 0)])
    basis, *levels, images = call(
        steps_kernel,
        [
            (BASIS - 2, *shape),
            (S, wide, rows, LANES),
            (S - 1, wide, rows, LANES),
            (S, rows, LANES),
            (S - 1, rows, LANES),
            jax.ShapeDtypeStruct(recycled_images.shape, recycled_images.dtype),
        ],
        (*fields, low, high, whole_rims, shifts, rim_shifts),
        weights_and_left(rows) + [pltpu.SemaphoreType.DMA],
        in_hbm=(recycled_images,),
    )
    first = moved(first, {"gy": inward})
    second = lax.ppermute(second, "gy", [(i, outward(i, count)) for i in range(1, count - 1)])
    block = 2 * TILE
    sums, total = call(
        products_kernel,
        [(sum(len(family) for family in products()), TILE, LANES), (BASIS * block, RECYCLED * block)],
        (*fields[:2], basis, images),
    )
    caps, parts = call(
        caps_kernel,
        [(BASIS - 2, planes, TILE, LANES), (lax.axis_size(AXES), 2, LANES)],
        (parity, *fields, low, high, whole_rims, first, second, wrapped, images)
        + (shifts, rim_shifts, groups, sums, total, *levels),
        [pltpu.VMEM((S, wide, block, LANES), jnp.float32), pltpu.VMEM((S - 1, wide, block, LANES), jnp.float32)]
        + weights_and_left(block),
    )
    parts = lax.all_to_all(parts, AXES, 0, 0)
    return call(finish_kernel, [shape] * 3, (parts, coupling, fields[0], fields[1], basis, caps, recycled))


def solution(mesh):
    in_specs = (
        P("gx", "gy", "gz"),
        P("gx", "gy", "gz"),
        P("gx", "gy", "gz"),
        P(None, "gx", "gy", "gz"),
        P(None, "gx", "gy", "gz"),
        P(),
    )
    out_specs = (P("gx", "gy", "gz"), P("gx", "gy", "gz"), P("gx", "gy", "gz"))
    return jax.shard_map(body, mesh=mesh, in_specs=in_specs, out_specs=out_specs, check_vma=False)
```

```python
import jax
import jax.numpy as jnp
import numpy as np
from jax import lax
from jax.experimental import pallas as pl
from jax.experimental.pallas import tpu as pltpu
from jax.sharding import PartitionSpec as P

S = 4
BASIS = 9
RECYCLED = 16
LANES = 128
TILE = 8
AXES = ("gx", "gy", "gz")

RIM = 2 * S
SIDE = RIM * S


center = 7.25
half_width = 6.75


def lanes_of(rows):
    return lax.broadcasted_iota(jnp.int32, (rows, LANES), 1)


def rows_of(rows):
    return lax.broadcasted_iota(jnp.int32, (rows, LANES), 0)


def turn(values, shift, axis):
    shift = shift % values.shape[axis]
    return pltpu.roll(values, shift, axis) if shift else values


def load_kernel(
    direction_in, residual_in, diagonal_in, coupling_in, direction, residual, diagonal, upper, lower, coupling, done
):
    pairs = (
        (direction_in, direction, S),
        (residual_in, residual, S - 1),
        (diagonal_in, diagonal, S - 1),
        (coupling_in, coupling, 0),
    )
    copies = [pltpu.make_async_copy(source, kept, done.at[index]) for index, (source, kept, _) in enumerate(pairs)]
    for copy in copies:
        copy.start()
    planes = direction.shape[0]
    at = 0
    for copy, (_, kept, width) in zip(copies, pairs):
        copy.wait()
        if not width:
            continue
        upper[at : at + width] = kept[planes - width :]
        lower[at : at + width] = kept[:width]
        at += width


def rim_kernel(parity, direction, residual, diagonal, coupling, rim_out, outward_out, inward_out, coupling_out):
    planes, rows, _ = direction.shape
    slot = lanes_of(rows) // RIM
    after = jnp.zeros((rows, LANES), jnp.float32)
    before = jnp.zeros((rows, LANES), jnp.float32)
    source = lax.broadcasted_iota(jnp.int32, (LANES, LANES), 0)
    target = lax.broadcasted_iota(jnp.int32, (LANES, LANES), 1) % RIM
    ends = (source == jnp.where(target < S, target, LANES - RIM + target)).astype(jnp.float32).astype(jnp.bfloat16)
    ends = jnp.concatenate([ends, ends], axis=0)
    for field, values in enumerate((direction, residual, diagonal)):
        values = values[...].reshape(planes * rows, LANES)
        copies = jnp.dot(jnp.concatenate(split(values), axis=1), ends, preferred_element_type=jnp.float32)
        rim = jnp.zeros((rows, LANES), jnp.float32)
        for plane in range(planes):
            here = copies[rows * plane : rows * (plane + 1)]
            rim = jnp.where(slot == plane + S, here, rim)
            if plane < S:
                before = jnp.where(slot == S * field + plane, here, before)
            if plane >= planes - S:
                after = jnp.where(slot == S * field + plane - planes + S, here, after)
        rim_out[field] = rim
    even = parity[0] < 2
    outward_out[...] = jnp.where(even, before, after)
    inward_out[...] = jnp.where(even, after, before)
    vector = lax.broadcasted_iota(jnp.int32, (RECYCLED, LANES), 0)
    spread = (lanes_of(RECYCLED) // TILE == vector).astype(jnp.float32)
    coupling_out[...] = jnp.dot(
        coupling[...], spread, precision=lax.Precision.HIGHEST, preferred_element_type=jnp.float32
    )


def plane_of(own, low, high, field, x, part=slice(None)):
    planes = own.shape[0]
    first = (0, S, 2 * S - 1)[field]
    width = (S, S - 1, S - 1)[field]
    if x < 0:
        return low[first + width + x, part]
    if x >= planes:
        return high[first + x - planes, part]
    return own[x, part]


def packing(planes):
    pieces = []
    for field in range(3):
        reach = (S, S - 1, S - 1)[field]
        for x in range(1 - reach, planes + reach - 1):
            pieces.append((reach - max(0, -x, x - planes + 1), field, x))
        pieces.append((reach - 1, field, None))
    pieces.sort(key=lambda piece: -piece[0])
    tiles = []
    for count, field, x in pieces:
        for tile in tiles:
            used = sum(piece[0] for piece in tile)
            if used + count <= TILE:
                tile.append((count, field, x, used))
                break
        else:
            tiles.append([(count, field, x, 0)])
    return tiles


def edge_kernel(
    parity, direction, residual, diagonal, low, high, rim_next, rim_before, outward_next, outward_before, inward_next, inward_before, first_out, second_out, rim_out
):
    planes, rows, _ = direction.shape
    lane = lanes_of(rows)
    nearer = lane % RIM < S
    outward = jnp.where(nearer, outward_next[...], outward_before[...])
    inward = jnp.where(nearer, inward_next[...], inward_before[...])
    low_rim = jnp.where(parity[0] < 2, outward, inward)
    high_rim = jnp.where(parity[0] < 2, inward, outward)
    for field in range(3):
        rim = jnp.where(nearer, rim_next[field], rim_before[field])
        rim = jnp.where(lane < SIDE, turn(low_rim, -SIDE * field, 1), rim)
        rim = jnp.where(lane >= SIDE + RIM * planes, turn(high_rim, SIDE + RIM * planes - SIDE * field, 1), rim)
        rim_out[field] = rim
    fields = (direction, residual, diagonal)
    row = rows_of(TILE)

    even = parity[0] & 1 == 0
    for index, tile in enumerate(packing(planes)):
        lower = jnp.zeros((TILE, LANES), jnp.float32)
        upper = jnp.zeros((TILE, LANES), jnp.float32)
        for count, field, x, offset in tile:
            values = rim_out[field] if x is None else plane_of(fields[field], low, high, field, x)
            mine = (row >= offset) & (row < offset + count)
            lower = jnp.where(mine, turn(values[:TILE], offset, 0), lower)
            upper = jnp.where(mine, turn(values[rows - TILE :], offset + count, 0), upper)
        first_out[index] = jnp.where(even, upper, lower)
        second_out[index] = jnp.where(even, lower, upper)


def shift_matrices():
    source = np.arange(LANES)[:, None]
    target = np.arange(LANES)[None, :]
    along = np.abs(source - target) == 1
    last = (target % RIM == 0) & (source == LANES - 1)
    ends = last | ((target % RIM == RIM - 1) & (source == 0))
    facing = ((target == 0) & (source % RIM == RIM - 1)) | ((target == LANES - 1) & (source % RIM == 0))
    around = (np.abs(source - target) == RIM) | (along & (source // RIM == target // RIM))
    groups = np.arange(2 * TILE * RECYCLED)[:, None] // (2 * TILE) == target // TILE
    inner = np.concatenate([along, ends], 1)
    outer = np.concatenate([facing, np.zeros_like(facing)], 1)
    matrices = ([inner, inner, outer, outer], [around, around], [groups, groups, groups])
    return [jnp.asarray(np.concatenate(parts), jnp.bfloat16) for parts in matrices]


def split(values, count=2):
    terms = []
    for index in range(count):
        terms.append(values.astype(jnp.bfloat16))
        if index + 1 < count:
            values = values - terms[-1].astype(jnp.float32)
    return terms


def products():
    found = []
    for one, other, count in ((0, 0, 2 * S + 1), (S + 1, S + 1, 2 * S - 1), (0, S + 1, 2 * S)):
        found.append([(one + (m + 1) // 2, other + m // 2) for m in range(count)])
    return found


def march(load, vertical, planes, ring, walk, trail, weight, left, shifts, rim_shifts, emit, keep):
    slot = lanes_of(ring) // RIM

    def scaled(values):
        return (values - (center - 6.0)) * (2.0 / half_width)

    for x in range(1 - S, planes + S - 1):
        weight[x + S] = scaled(load(2, x))
    weight_rim = scaled(load(2, None))
    chains = ((0, walk, 0, S), (1, trail, S, S - 1))
    rim_levels = {}
    for field, history, offset, length in chains:
        for x in range(-length, planes + length):
            history[0, x + S] = load(field, x)
        rim_levels[field] = [load(field, None)]
        keep(field, 0, rim_levels[field][0])

    def advance(values, before, factor, beside):
        following = factor * values - (2.0 / half_width) * beside
        return 0.5 * following if before is None else following - before

    for level in range(S):
        work = []
        for field, history, offset, length in chains:
            reach = length - 1 - level
            if reach < 0:
                continue
            facing = [part.astype(jnp.float32) for part in split(rim_levels[field][level])]
            for x in range(-reach, planes + reach, 2):
                both = (x, x + 1)
                parts = split(jnp.concatenate([history[level, one + S] for one in both], axis=0))
                for part in facing:
                    slots = [jnp.where(slot == one + S, part, 0.0) for one in both]
                    parts.append(jnp.concatenate(slots, axis=0).astype(jnp.bfloat16))
                for index, part in enumerate(parts):
                    left[ring * len(work) : ring * (len(work) + 2), LANES * index : LANES * (index + 1)] = part
                work += [(field, history, offset, reach, one) for one in both]
        moved = jnp.dot(left[: ring * len(work)], shifts[...], preferred_element_type=jnp.float32)
        gathered = {}
        for index, (field, history, offset, reach, x) in enumerate(work):
            at = x + S
            here = moved[ring * index : ring * (index + 1)]
            values = history[level, at]
            beside = here[:, :LANES] + (history[level, at - 1] + history[level, at + 1])
            beside = beside + vertical(values, field, level, x)
            before = None if level == 0 else history[level - 1, at]
            following = advance(values, before, weight[at], beside)
            if 0 <= x < planes:
                emit(offset + level, x, following)
            if reach:
                history[level + 1, at] = following
                gathered[field] = jnp.where(slot == at, here[:, LANES:], gathered.get(field, 0.0))
        for field in gathered:
            levels = rim_levels[field]
            rim = levels[level]
            beside = jnp.dot(
                jnp.concatenate(split(rim), axis=1), rim_shifts[...], preferred_element_type=jnp.float32
            )
            beside = beside + vertical(rim, field, level, None) + gathered[field]
            levels.append(advance(rim, None if level == 0 else levels[level - 1], weight_rim, beside))
            keep(field, level + 1, levels[-1])


def inner_products(planes, tiles_of, images_of):
    families = products()
    sums = {}
    half = 2 * TILE
    total = jnp.zeros((BASIS * half, RECYCLED * half), jnp.float32)
    rounded = []
    against = []
    for x in range(planes):
        values = [tiles_of(index, x) for index in range(BASIS)]
        for tile in range(len(values[0])):
            if values[0][tile] is None:
                continue
            for family in families:
                for i, j in family:
                    product = values[i][tile] * values[j][tile]
                    sums[i, j] = sums[i, j] + product if (i, j) in sums else product
        nothing = jnp.zeros((TILE, LANES), jnp.float32)
        for block, images in enumerate(images_of(x)):
            pieces = [value[2 * block : 2 * block + 2] for value in values]
            pieces = [nothing if piece is None else piece for pair in pieces for piece in pair]
            rounded.append(jnp.concatenate(pieces, axis=0).astype(jnp.bfloat16))
            against.append(images.reshape(RECYCLED * half, LANES))
        if len(rounded) == 2:
            total = total + lax.dot_general(
                jnp.concatenate(rounded, axis=1),
                jnp.concatenate(against, axis=1),
                (((1,), (1,)), ((), ())),
                preferred_element_type=jnp.float32,
            )
            rounded = []
            against = []
    return sums, total


def inner_kernel(
    direction, residual, diagonal, low, high, rims, shifts, rim_shifts, images_in, basis_out, sums_out, total_out, walk, trail, rim_walk, rim_trail, images, weight, left, done
):
    planes, rows, _ = direction.shape
    fields = (direction, residual, diagonal)
    row = rows_of(TILE)
    copy = pltpu.make_async_copy(images_in, images, done)
    copy.start()

    def load(field, x):
        return rims[field] if x is None else plane_of(fields[field], low, high, field, x)

    def vertical(values, field, level, x):
        return turn(values, 1, 0) + turn(values, -1, 0)

    def emit(index, x, values):
        basis_out[index, x] = values

    def keep(field, level, values):
        (rim_trail if field else rim_walk)[level] = values

    march(load, vertical, planes, rows, walk, trail, weight, left, shifts, rim_shifts, emit, keep)

    def tiles_of(index, x):
        if index in (0, S + 1):
            values = fields[index > 0][x]
        else:
            values = basis_out[index - 1 if index <= S else index - 2, x]
        tiles = [values[start : start + TILE] for start in range(0, rows, TILE)]
        tiles[0] = jnp.where(row < S, 0.0, tiles[0])
        tiles[-1] = jnp.where(row < S, tiles[-1], 0.0)
        return tiles

    copy.wait()

    def images_of(x):
        return [images[:, x, start : start + 2 * TILE] for start in range(0, rows, 2 * TILE)]

    sums, total = inner_products(planes, tiles_of, images_of)
    for index, pair in enumerate(sorted(sums)):
        sums_out[index] = sums[pair]
    total_out[...] = total


def cap_steps(
    high_side, arrived, fields, low, high, rims, shifts, rim_shifts, inner_walk, inner_trail, inner_rim_walk, inner_rim_trail, walk, trail, weight, left, emit
):
    planes, rows, _ = fields[0].shape
    row = rows_of(TILE)
    near = row < S
    side = jnp.where(high_side, 1, 0)
    beyond_here = near == (jnp.zeros((TILE, LANES), jnp.int32) + side == 1)
    from_above = (row == S) & (jnp.zeros((TILE, LANES), jnp.int32) + side == 0)
    from_below = (row == S - 1) & (jnp.zeros((TILE, LANES), jnp.int32) + side == 1)
    start = pl.multiple_of(side * (rows - TILE), TILE)
    part = pl.ds(start, TILE)
    halo = {}
    for tile, pieces in enumerate(packing(planes)):
        for count, field, x, offset in pieces:
            message = arrived(tile)
            halo[field, x] = jnp.where(high_side, turn(message, -offset, 0), turn(message, -offset - count, 0))
    nothing = jnp.zeros((TILE, LANES), jnp.float32)

    def load(field, x):
        if x is None:
            values = rims[field, part]
        else:
            values = plane_of(fields[field], low, high, field, x, part)
        return jnp.where(beyond_here, halo.get((field, x), nothing), values)

    def vertical(values, field, level, x):
        if x is None:
            known = (inner_rim_trail if field else inner_rim_walk)[level, part]
        else:
            known = (inner_trail if field else inner_walk)[level, x + S, part]
        after = turn(jnp.where(from_above, known, values), -1, 0)
        return after + turn(jnp.where(from_below, known, values), 1, 0)

    march(load, vertical, planes, TILE, walk, trail, weight, left, shifts, rim_shifts, emit, lambda *_: None)


def first_cap_kernel(
    parity, direction, residual, diagonal, low, high, rims, first, shifts, rim_shifts, inner_walk, inner_trail, inner_rim_walk, inner_rim_trail, cap_out, walk, trail, weight, left
):
    def emit(index, x, values):
        cap_out[index, x] = values

    cap_steps(
        parity[0] & 1 == 0, lambda tile: first[tile], (direction, residual, diagonal), low, high, rims, shifts, rim_shifts, inner_walk, inner_trail, inner_rim_walk, inner_rim_trail, walk, trail, weight, left, emit
    )


def caps_kernel(
    parity, direction, residual, diagonal, low, high, rims, second, cap, images, shifts, rim_shifts, groups, sums_in, total_in, inner_walk, inner_trail, inner_rim_walk, inner_rim_trail, caps_out, parts_out, walk, trail, weight, left
):
    planes, rows, _ = direction.shape
    fields = (direction, residual, diagonal)
    row = rows_of(TILE)
    near = row < S
    odd = parity[0] & 1
    ours = near == (jnp.zeros((TILE, LANES), jnp.int32) + odd == 0)

    def emit(index, x, values):
        caps_out[index, x] = jnp.where(ours, values, cap[index, x])

    cap_steps(
        odd == 1, lambda tile: second[tile], fields, low, high, rims, shifts, rim_shifts, inner_walk, inner_trail, inner_rim_walk, inner_rim_trail, walk, trail, weight, left, emit
    )

    def tile_of(index, x):
        if index in (0, S + 1):
            values = fields[index > 0][x]
            return jnp.where(near, values[:TILE], values[rows - TILE :])
        return caps_out[index - 1 if index <= S else index - 2, x]

    upper = lax.broadcasted_iota(jnp.int32, (RECYCLED, 2 * TILE, LANES), 1) < TILE
    families = products()
    sums = {}
    half = 2 * TILE
    total = total_in[...]
    for x in range(0, planes, 2):
        rounded = []
        against = []
        for k in range(2):
            values = [tile_of(index, x + k) for index in range(BASIS)]
            for family in families:
                for i, j in family:
                    product = values[i] * values[j]
                    sums[i, j] = sums[i, j] + product if (i, j) in sums else product
            pieces = [
                piece for value in values for piece in (jnp.where(near, value, 0.0), jnp.where(near, 0.0, value))
            ]
            rounded.append(jnp.concatenate(pieces, axis=0).astype(jnp.bfloat16))
            images_here = jnp.where(upper, images[:, x + k, :half], images[:, x + k, rows - half :])
            against.append(images_here.reshape(RECYCLED * half, LANES))
        total = total + lax.dot_general(
            jnp.concatenate(rounded, axis=1),
            jnp.concatenate(against, axis=1),
            (((1,), (1,)), ((), ())),
            preferred_element_type=jnp.float32,
        )
    spot = lanes_of(TILE)
    columns = [list(families[0][:TILE]), list(families[1]) + [families[0][TILE]], list(families[2])]
    order = {pair: index for index, pair in enumerate(sorted(sums))}
    scalars = jnp.zeros((TILE, LANES), jnp.float32)
    for place, column in enumerate(columns):
        values = jnp.zeros((TILE, LANES), jnp.float32)
        for index, pair in enumerate(column):
            whole = sums[pair] + sums_in[order[pair]]
            values = jnp.where(row == index, jnp.sum(whole, axis=0, keepdims=True), values)
        values = jnp.sum(values, axis=1, keepdims=True)
        scalars = jnp.where((spot // TILE == row) & (spot % TILE == place + 1), values, scalars)
    wide = (BASIS * half, RECYCLED * half)
    same = lax.broadcasted_iota(jnp.int32, wide, 0) % half == lax.broadcasted_iota(jnp.int32, wide, 1) % half
    total = jnp.where(same, total, 0.0).reshape(BASIS, 2, TILE, RECYCLED * half)
    total = (total[:, 0] + total[:, 1]).reshape(BASIS * TILE, RECYCLED * half)
    lines = jnp.dot(jnp.concatenate(split(total, 3), axis=1), groups[...], preferred_element_type=jnp.float32)
    mixed = jnp.zeros((TILE, LANES), jnp.float32)
    for index in range(TILE):
        mixed = jnp.where(spot % TILE == index, lines[TILE * index : TILE * (index + 1)], mixed)
    extra = jnp.where(spot % TILE == 0, lines[TILE * TILE :], scalars)
    table = jnp.concatenate(
        [jnp.sum(mixed, axis=0, keepdims=True), jnp.sum(extra, axis=0, keepdims=True)], axis=0
    )
    table = jnp.concatenate([table] * (TILE // 2), axis=0)
    for start in range(0, parts_out.shape[0], TILE):
        parts_out[start : start + TILE] = table


def moments_of(values):
    first = values[:2]
    return first + [2.0 * value - first[index % 2] for index, value in enumerate(values[2:])]


def finish_kernel(
    parts, coupling, direction, residual, basis, caps, recycled, delta_out, residual_out, direction_out
):
    pieces = [parts[start : start + TILE] for start in range(0, parts.shape[0], TILE)]
    while len(pieces) > 1:
        pieces = [a + b for a, b in zip(pieces[::2], pieces[1::2])] + pieces[len(pieces) // 2 * 2 :]
    table = pieces[0]
    for shift in (4, 2):
        table = table + turn(table, shift, 0)
    spot = lanes_of(TILE)
    row = rows_of(TILE)
    mixed = jnp.broadcast_to(table[:1], (TILE, LANES))
    extra = jnp.broadcast_to(table[1:2], (TILE, LANES))
    columns = []
    for place in range(3):
        mine = (spot // TILE == row) & (spot % TILE == place + 1)
        column = jnp.sum(jnp.where(mine, extra, 0.0), axis=1, keepdims=True)
        columns.append(jnp.broadcast_to(column, (TILE, LANES)))

    def spread(column, index):
        return jnp.broadcast_to(columns[column][index : index + 1], (TILE, LANES))

    walk = moments_of([spread(0, index) for index in range(TILE)] + [spread(1, TILE - 1)])
    trail = moments_of([spread(1, index) for index in range(2 * S - 1)])
    cross = moments_of([spread(2, index) for index in range(2 * S)])
    gram = {}
    for i in range(BASIS):
        for j in range(i, BASIS):
            source = walk if j <= S else (cross if i <= S else trail)
            one = i if i <= S else i - S - 1
            two = j if j <= S else j - S - 1
            gram[i, j] = gram[j, i] = 0.5 * (source[one + two] + source[abs(one - two)])

    def dot(one, other):
        terms = [one[i] * other[i] for i in one if i in other]
        while len(terms) > 1:
            terms = [a + b for a, b in zip(terms[::2], terms[1::2])] + terms[len(terms) // 2 * 2 :]
        return terms[0]

    def applied(values):
        return {i: dot({j: gram[i, j] for j in values}, values) for i in range(BASIS)}

    def mapped_by(values):
        found = {}
        for j, value in values.items():
            first, length = (0, S + 1) if j <= S else (S + 1, S)
            k = j - first
            if k == 0:
                entries = ((j, center), (j + 1, half_width))
            elif k < length - 1:
                entries = ((j - 1, half_width / 2), (j, center), (j + 1, half_width / 2))
            else:
                entries = ()
            for i, factor in entries:
                found[i] = found[i] + factor * value if i in found else factor * value
        return found

    def plus(one, factor, other):
        found = dict(one)
        for i, value in other.items():
            found[i] = found[i] + factor * value if i in found else factor * value
        return found

    unit = jnp.ones((TILE, LANES), jnp.float32)
    residue = {S + 1: unit}
    search = {0: unit}
    update = {}
    norm_now = dot(residue, applied(residue))
    for _ in range(S):
        mapped = mapped_by(search)
        step_size = norm_now / dot(search, applied(mapped))
        update = plus(update, step_size, search)
        residue = plus(residue, -step_size, mapped)
        norm_next = dot(residue, applied(residue))
        search = plus(residue, norm_next / norm_now, search)
        norm_now = norm_next
    across = residue[0]
    for index in range(1, TILE):
        across = jnp.where(spot % TILE == index, residue[index], across)
    projected = mixed * across + jnp.where(spot % TILE == 0, extra * residue[BASIS - 1], 0.0)
    projected = projected[:1]
    weights = jnp.sum(coupling[...] * projected, axis=1, keepdims=True)
    weights = jnp.broadcast_to(weights.astype(jnp.bfloat16).astype(jnp.float32), (RECYCLED, 2 * LANES))
    wide = (2 * TILE, 2 * TILE * RECYCLED)
    index = lax.broadcasted_iota(jnp.int32, wide, 0)
    slot = lax.broadcasted_iota(jnp.int32, wide, 1)
    spread_weights = jnp.sum(jnp.where(slot // (2 * TILE) == index, weights, 0.0), axis=0, keepdims=True)
    mixing = jnp.where(slot % (2 * TILE) == index, spread_weights, 0.0).astype(jnp.bfloat16)
    planes, rows, _ = direction.shape
    near = row < S
    for plane in range(planes):
        for start in range(0, rows, 2 * TILE):
            part = slice(start, start + 2 * TILE)
            found = [0.0, 0.0, 0.0]
            for field in range(BASIS):
                if field in (0, S + 1):
                    values = (residual if field else direction)[plane, part]
                else:
                    at = field - 1 if field <= S else field - 2
                    pieces = [basis[at, plane, start : start + TILE], basis[at, plane, start + TILE : start + 2 * TILE]]
                    if start == 0:
                        pieces[0] = jnp.where(near, caps[at, plane], pieces[0])
                    if start + 2 * TILE == rows:
                        pieces[1] = jnp.where(near, pieces[1], caps[at, plane])
                    values = jnp.concatenate(pieces, axis=0)
                for index, coefficients in enumerate((update, residue, search)):
                    if field in coefficients:
                        factor = jnp.concatenate([coefficients[field]] * 2, axis=0)
                        found[index] = found[index] + factor * values
            vectors = recycled[:, plane, part].reshape(RECYCLED * 2 * TILE, LANES)
            correction = jnp.dot(mixing, vectors, preferred_element_type=jnp.float32)
            delta_out[plane, part] = found[0]
            residual_out[plane, part] = found[1]
            direction_out[plane, part] = found[2] - correction


def onward(step):
    return lambda index, count: (index + step) % count


def inward(index, count):
    return index ^ 1


def outward(index, count):
    return (index - 1 + 2 * (index % 2)) % count


def moved(values, moves):
    axes = tuple(moves)
    pairs = [(0, 0)]
    for axis in axes:
        count = lax.axis_size(axis)
        pairs = [
            (source * count + i, target * count + moves[axis](i, count)) for source, target in pairs for i in range(count)
        ]
    return lax.ppermute(values, axes, pairs)


def call(kernel, out_shape, operands, scratch=(), limit=16, in_hbm=()):
    in_vmem = pl.BlockSpec(memory_space=pltpu.VMEM)
    in_smem = pl.BlockSpec(memory_space=pltpu.SMEM)
    in_place = pl.BlockSpec(memory_space=pltpu.HBM)
    in_hbm = [pltpu.with_memory_space_constraint(operand, pltpu.HBM) for operand in in_hbm]
    out_shape = [shape if isinstance(shape, jax.ShapeDtypeStruct) else jax.ShapeDtypeStruct(shape, jnp.float32) for shape in out_shape]
    return pl.pallas_call(
        kernel,
        out_shape=tuple(out_shape),
        in_specs=[in_smem if operand.dtype == jnp.int32 else in_vmem for operand in operands] + [in_place] * len(in_hbm),
        out_specs=(in_vmem,) * len(out_shape),
        scratch_shapes=list(scratch),
        compiler_params=pltpu.CompilerParams(vmem_limit_bytes=limit * 1024 * 1024),
    )(*operands, *in_hbm)


def body(residual, direction, diagonal, recycled, recycled_images, coupling_inverse):
    planes, rows, columns = residual.shape
    if columns != LANES or rows != 4 * TILE or RIM * (planes + 2 * S) != LANES or lax.axis_size("gx") % 2 or lax.axis_size("gy") % 2:
        raise ValueError("unsupported block")
    shape = residual.shape
    shifts, rim_shifts, groups = shift_matrices()
    slab = (3 * S - 2, rows, LANES)
    *fields, upper, lower, coupling = call(
        load_kernel,
        [shape] * 3 + [slab] * 2 + [coupling_inverse.shape],
        (),
        [pltpu.SemaphoreType.DMA((4,))],
        in_hbm=(direction, residual, diagonal, coupling_inverse),
    )
    parity = ((lax.axis_index("gy") & 1) + 2 * (lax.axis_index("gx") & 1)).astype(jnp.int32).reshape(1)
    low = moved(upper, {"gx": onward(1)})
    high = moved(lower, {"gx": onward(-1)})
    rim, rim_outward, rim_inward, coupling = call(
        rim_kernel, [(3, rows, LANES), (rows, LANES), (rows, LANES), (RECYCLED, LANES)], (parity, *fields, coupling)
    )
    sides = [onward(-1)] if lax.axis_size("gz") == 2 else [onward(-1), onward(1)]
    outward_rims = [moved(rim_outward, {"gx": outward, "gz": side}) for side in sides]
    rims = [moved(rim, {"gz": side}) for side in sides]
    inward_rims = [moved(rim_inward, {"gx": inward, "gz": side}) for side in sides]
    tiles = len(packing(planes))
    first, second, whole_rims = call(
        edge_kernel,
        [(tiles, TILE, LANES), (tiles, TILE, LANES), (3, rows, LANES)],
        (parity, *fields, low, high, rims[0], rims[-1], outward_rims[0], outward_rims[-1])
        + (inward_rims[0], inward_rims[-1]),
    )
    second = moved(second, {"gy": outward})
    first = moved(first, {"gy": inward})
    devices = lax.axis_size(AXES)
    wide = planes + 2 * S
    worked = 2 * planes + 2 * (S - 1) + 2 * (S - 2)

    def weights_and_left(ring):
        return [pltpu.VMEM((wide, ring, LANES), jnp.float32), pltpu.VMEM((worked * ring, 4 * LANES), jnp.bfloat16)]

    count = sum(len(family) for family in products())
    block = 2 * TILE
    basis, sums, total, *levels, images = call(
        inner_kernel,
        [
            (BASIS - 2, *shape),
            (count, TILE, LANES),
            (BASIS * block, RECYCLED * block),
            (S, wide, rows, LANES),
            (S - 1, wide, rows, LANES),
            (S, rows, LANES),
            (S - 1, rows, LANES),
            jax.ShapeDtypeStruct(recycled_images.shape, recycled_images.dtype),
        ],
        (*fields, low, high, whole_rims, shifts, rim_shifts),
        weights_and_left(rows) + [pltpu.SemaphoreType.DMA],
        in_hbm=(recycled_images,),
    )
    tall = [pltpu.VMEM((S, wide, TILE, LANES), jnp.float32), pltpu.VMEM((S - 1, wide, TILE, LANES), jnp.float32)]
    cap_shape = (BASIS - 2, planes, TILE, LANES)
    (cap,) = call(
        first_cap_kernel,
        [cap_shape],
        (parity, *fields, low, high, whole_rims, first, shifts, rim_shifts, *levels),
        tall + weights_and_left(TILE),
    )
    caps, parts = call(
        caps_kernel,
        [cap_shape, (2 * devices, LANES)],
        (parity, *fields, low, high, whole_rims, second, cap, images)
        + (shifts, rim_shifts, groups, sums, total, *levels),
        tall + weights_and_left(TILE),
    )
    parts = lax.all_to_all(parts, AXES, 0, 0, tiled=True)
    return call(finish_kernel, [shape] * 3, (parts, coupling, fields[0], fields[1], basis, caps, recycled))


def solution(mesh):
    in_specs = (
        P("gx", "gy", "gz"),
        P("gx", "gy", "gz"),
        P("gx", "gy", "gz"),
        P(None, "gx", "gy", "gz"),
        P(None, "gx", "gy", "gz"),
        P(),
    )
    out_specs = (P("gx", "gy", "gz"), P("gx", "gy", "gz"), P("gx", "gy", "gz"))
    return jax.shard_map(body, mesh=mesh, in_specs=in_specs, out_specs=out_specs, check_vma=False)
```

```python
import jax
import jax.numpy as jnp
import numpy as np
from jax import lax
from jax.experimental import pallas as pl
from jax.experimental.pallas import tpu as pltpu
from jax.sharding import PartitionSpec as P

S = 4
BASIS = 9
RECYCLED = 16
LANES = 128
TILE = 8
AXES = ("gx", "gy", "gz")

RIM = 2 * S
SIDE = RIM * S


center = 7.25
half_width = 6.75


def lanes_of(rows):
    return lax.broadcasted_iota(jnp.int32, (rows, LANES), 1)


def rows_of(rows):
    return lax.broadcasted_iota(jnp.int32, (rows, LANES), 0)


def turn(values, shift, axis):
    shift = shift % values.shape[axis]
    return pltpu.roll(values, shift, axis) if shift else values


def load_kernel(
    direction_in, residual_in, diagonal_in, coupling_in, direction, residual, diagonal, upper, lower, coupling, done
):
    pairs = (
        (direction_in, direction, S),
        (residual_in, residual, S - 1),
        (diagonal_in, diagonal, S - 1),
        (coupling_in, coupling, 0),
    )
    copies = [pltpu.make_async_copy(source, kept, done.at[index]) for index, (source, kept, _) in enumerate(pairs)]
    for copy in copies:
        copy.start()
    planes = direction.shape[0]
    at = 0
    for copy, (_, kept, width) in zip(copies, pairs):
        copy.wait()
        if not width:
            continue
        upper[at : at + width] = kept[planes - width :]
        lower[at : at + width] = kept[:width]
        at += width


def rim_kernel(parity, direction, residual, diagonal, coupling, rim_out, outward_out, inward_out, coupling_out):
    planes, rows, _ = direction.shape
    slot = lanes_of(rows) // RIM
    after = jnp.zeros((rows, LANES), jnp.float32)
    before = jnp.zeros((rows, LANES), jnp.float32)
    source = lax.broadcasted_iota(jnp.int32, (LANES, LANES), 0)
    target = lax.broadcasted_iota(jnp.int32, (LANES, LANES), 1) % RIM
    ends = (source == jnp.where(target < S, target, LANES - RIM + target)).astype(jnp.float32).astype(jnp.bfloat16)
    ends = jnp.concatenate([ends, ends], axis=0)
    for field, values in enumerate((direction, residual, diagonal)):
        values = values[...].reshape(planes * rows, LANES)
        copies = jnp.dot(jnp.concatenate(split(values), axis=1), ends, preferred_element_type=jnp.float32)
        rim = jnp.zeros((rows, LANES), jnp.float32)
        for plane in range(planes):
            here = copies[rows * plane : rows * (plane + 1)]
            rim = jnp.where(slot == plane + S, here, rim)
            if plane < S:
                before = jnp.where(slot == S * field + plane, here, before)
            if plane >= planes - S:
                after = jnp.where(slot == S * field + plane - planes + S, here, after)
        rim_out[field] = rim
    even = parity[0] < 2
    outward_out[...] = jnp.where(even, before, after)
    inward_out[...] = jnp.where(even, after, before)
    vector = lax.broadcasted_iota(jnp.int32, (RECYCLED, LANES), 0)
    spread = (lanes_of(RECYCLED) // TILE == vector).astype(jnp.float32)
    coupling_out[...] = jnp.dot(
        coupling[...], spread, precision=lax.Precision.HIGHEST, preferred_element_type=jnp.float32
    )


def plane_of(own, low, high, field, x, part=slice(None)):
    planes = own.shape[0]
    first = (0, S, 2 * S - 1)[field]
    width = (S, S - 1, S - 1)[field]
    if x < 0:
        return low[first + width + x, part]
    if x >= planes:
        return high[first + x - planes, part]
    return own[x, part]


def packing(planes):
    pieces = []
    for field in range(3):
        reach = (S, S - 1, S - 1)[field]
        for x in range(1 - reach, planes + reach - 1):
            pieces.append((reach - max(0, -x, x - planes + 1), field, x))
        pieces.append((reach - 1, field, None))
    pieces.sort(key=lambda piece: -piece[0])
    tiles = []
    for count, field, x in pieces:
        for tile in tiles:
            used = sum(piece[0] for piece in tile)
            if used + count <= TILE:
                tile.append((count, field, x, used))
                break
        else:
            tiles.append([(count, field, x, 0)])
    return tiles


def edge_kernel(
    parity, direction, residual, diagonal, low, high, rim_next, rim_before, outward_next, outward_before, inward_next, inward_before, first_out, second_out, rim_out
):
    planes, rows, _ = direction.shape
    lane = lanes_of(rows)
    nearer = lane % RIM < S
    outward = jnp.where(nearer, outward_next[...], outward_before[...])
    inward = jnp.where(nearer, inward_next[...], inward_before[...])
    low_rim = jnp.where(parity[0] < 2, outward, inward)
    high_rim = jnp.where(parity[0] < 2, inward, outward)
    for field in range(3):
        rim = jnp.where(nearer, rim_next[field], rim_before[field])
        rim = jnp.where(lane < SIDE, turn(low_rim, -SIDE * field, 1), rim)
        rim = jnp.where(lane >= SIDE + RIM * planes, turn(high_rim, SIDE + RIM * planes - SIDE * field, 1), rim)
        rim_out[field] = rim
    fields = (direction, residual, diagonal)
    row = rows_of(TILE)

    even = parity[0] & 1 == 0
    for index, tile in enumerate(packing(planes)):
        lower = jnp.zeros((TILE, LANES), jnp.float32)
        upper = jnp.zeros((TILE, LANES), jnp.float32)
        for count, field, x, offset in tile:
            values = rim_out[field] if x is None else plane_of(fields[field], low, high, field, x)
            mine = (row >= offset) & (row < offset + count)
            lower = jnp.where(mine, turn(values[:TILE], offset, 0), lower)
            upper = jnp.where(mine, turn(values[rows - TILE :], offset + count, 0), upper)
        first_out[index] = jnp.where(even, upper, lower)
        second_out[index] = jnp.where(even, lower, upper)


def shift_matrices():
    source = np.arange(LANES)[:, None]
    target = np.arange(LANES)[None, :]
    along = np.abs(source - target) == 1
    last = (target % RIM == 0) & (source == LANES - 1)
    ends = last | ((target % RIM == RIM - 1) & (source == 0))
    facing = ((target == 0) & (source % RIM == RIM - 1)) | ((target == LANES - 1) & (source % RIM == 0))
    around = (np.abs(source - target) == RIM) | (along & (source // RIM == target // RIM))
    groups = np.arange(2 * TILE * RECYCLED)[:, None] // (2 * TILE) == target // TILE
    inner = np.concatenate([along, ends], 1)
    outer = np.concatenate([facing, np.zeros_like(facing)], 1)
    matrices = ([inner, inner, outer, outer], [around, around], [groups, groups, groups])
    return [jnp.asarray(np.concatenate(parts), jnp.bfloat16) for parts in matrices]


def split(values, count=2):
    terms = []
    for index in range(count):
        terms.append(values.astype(jnp.bfloat16))
        if index + 1 < count:
            values = values - terms[-1].astype(jnp.float32)
    return terms


def products():
    found = []
    for one, other, count in ((0, 0, 2 * S + 1), (S + 1, S + 1, 2 * S - 1), (0, S + 1, 2 * S)):
        found.append([(one + (m + 1) // 2, other + m // 2) for m in range(count)])
    return found


def march(load, vertical, planes, ring, walk, trail, weight, left, shifts, rim_shifts, emit, keep):
    slot = lanes_of(ring) // RIM

    def scaled(values):
        return (values - (center - 6.0)) * (2.0 / half_width)

    for x in range(1 - S, planes + S - 1):
        weight[x + S] = scaled(load(2, x))
    weight_rim = scaled(load(2, None))
    chains = ((0, walk, 0, S), (1, trail, S, S - 1))
    rim_levels = {}
    for field, history, offset, length in chains:
        for x in range(-length, planes + length):
            history[0, x + S] = load(field, x)
        rim_levels[field] = [load(field, None)]
        keep(field, 0, rim_levels[field][0])

    def advance(values, before, factor, beside):
        following = factor * values - (2.0 / half_width) * beside
        return 0.5 * following if before is None else following - before

    for level in range(S):
        work = []
        for field, history, offset, length in chains:
            reach = length - 1 - level
            if reach < 0:
                continue
            facing = [part.astype(jnp.float32) for part in split(rim_levels[field][level])]
            for x in range(-reach, planes + reach, 2):
                both = (x, x + 1)
                parts = split(jnp.concatenate([history[level, one + S] for one in both], axis=0))
                for part in facing:
                    slots = [jnp.where(slot == one + S, part, 0.0) for one in both]
                    parts.append(jnp.concatenate(slots, axis=0).astype(jnp.bfloat16))
                for index, part in enumerate(parts):
                    left[ring * len(work) : ring * (len(work) + 2), LANES * index : LANES * (index + 1)] = part
                work += [(field, history, offset, reach, one) for one in both]
        moved = jnp.dot(left[: ring * len(work)], shifts[...], preferred_element_type=jnp.float32)
        gathered = {}
        for index, (field, history, offset, reach, x) in enumerate(work):
            at = x + S
            here = moved[ring * index : ring * (index + 1)]
            values = history[level, at]
            beside = here[:, :LANES] + (history[level, at - 1] + history[level, at + 1])
            beside = beside + vertical(values, field, level, x)
            before = None if level == 0 else history[level - 1, at]
            following = advance(values, before, weight[at], beside)
            if 0 <= x < planes:
                emit(offset + level, x, following)
            if reach:
                history[level + 1, at] = following
                gathered[field] = jnp.where(slot == at, here[:, LANES:], gathered.get(field, 0.0))
        for field in gathered:
            levels = rim_levels[field]
            rim = levels[level]
            beside = jnp.dot(
                jnp.concatenate(split(rim), axis=1), rim_shifts[...], preferred_element_type=jnp.float32
            )
            beside = beside + vertical(rim, field, level, None) + gathered[field]
            levels.append(advance(rim, None if level == 0 else levels[level - 1], weight_rim, beside))
            keep(field, level + 1, levels[-1])


def inner_products(planes, tiles_of, images_of):
    families = products()
    sums = {}
    half = 2 * TILE
    total = jnp.zeros((BASIS * half, RECYCLED * half), jnp.float32)
    rounded = []
    against = []
    for x in range(planes):
        values = [tiles_of(index, x) for index in range(BASIS)]
        for tile in range(len(values[0])):
            if values[0][tile] is None:
                continue
            for family in families:
                for i, j in family:
                    product = values[i][tile] * values[j][tile]
                    sums[i, j] = sums[i, j] + product if (i, j) in sums else product
        nothing = jnp.zeros((TILE, LANES), jnp.float32)
        for block, images in enumerate(images_of(x)):
            pieces = [value[2 * block : 2 * block + 2] for value in values]
            pieces = [nothing if piece is None else piece for pair in pieces for piece in pair]
            rounded.append(jnp.concatenate(pieces, axis=0).astype(jnp.bfloat16))
            against.append(images.reshape(RECYCLED * half, LANES))
        if len(rounded) == 2:
            total = total + lax.dot_general(
                jnp.concatenate(rounded, axis=1),
                jnp.concatenate(against, axis=1),
                (((1,), (1,)), ((), ())),
                preferred_element_type=jnp.float32,
            )
            rounded = []
            against = []
    return sums, total


def inner_kernel(
    direction, residual, diagonal, low, high, rims, shifts, rim_shifts, images_in, basis_out, sums_out, total_out, walk, trail, rim_walk, rim_trail, images, weight, left, done
):
    planes, rows, _ = direction.shape
    fields = (direction, residual, diagonal)
    row = rows_of(TILE)
    copy = pltpu.make_async_copy(images_in, images, done)
    copy.start()

    def load(field, x):
        return rims[field] if x is None else plane_of(fields[field], low, high, field, x)

    def vertical(values, field, level, x):
        return turn(values, 1, 0) + turn(values, -1, 0)

    def emit(index, x, values):
        basis_out[index, x] = values

    def keep(field, level, values):
        (rim_trail if field else rim_walk)[level] = values

    march(load, vertical, planes, rows, walk, trail, weight, left, shifts, rim_shifts, emit, keep)

    def tiles_of(index, x):
        if index in (0, S + 1):
            values = fields[index > 0][x]
        else:
            values = basis_out[index - 1 if index <= S else index - 2, x]
        tiles = [values[start : start + TILE] for start in range(0, rows, TILE)]
        tiles[0] = jnp.where(row < S, 0.0, tiles[0])
        tiles[-1] = jnp.where(row < S, tiles[-1], 0.0)
        return tiles

    copy.wait()

    def images_of(x):
        return [images[:, x, start : start + 2 * TILE] for start in range(0, rows, 2 * TILE)]

    sums, total = inner_products(planes, tiles_of, images_of)
    for index, pair in enumerate(sorted(sums)):
        sums_out[index] = sums[pair]
    total_out[...] = total


def cap_steps(
    high_side, arrived, fields, low, high, rims, shifts, rim_shifts, inner_walk, inner_trail, inner_rim_walk, inner_rim_trail, walk, trail, weight, left, emit
):
    planes, rows, _ = fields[0].shape
    row = rows_of(TILE)
    near = row < S
    side = jnp.where(high_side, 1, 0)
    beyond_here = near == (jnp.zeros((TILE, LANES), jnp.int32) + side == 1)
    from_above = (row == S) & (jnp.zeros((TILE, LANES), jnp.int32) + side == 0)
    from_below = (row == S - 1) & (jnp.zeros((TILE, LANES), jnp.int32) + side == 1)
    start = pl.multiple_of(side * (rows - TILE), TILE)
    part = pl.ds(start, TILE)
    halo = {}
    for tile, pieces in enumerate(packing(planes)):
        for count, field, x, offset in pieces:
            message = arrived(tile)
            halo[field, x] = jnp.where(high_side, turn(message, -offset, 0), turn(message, -offset - count, 0))
    nothing = jnp.zeros((TILE, LANES), jnp.float32)

    def load(field, x):
        if x is None:
            values = rims[field, part]
        else:
            values = plane_of(fields[field], low, high, field, x, part)
        return jnp.where(beyond_here, halo.get((field, x), nothing), values)

    def vertical(values, field, level, x):
        if x is None:
            known = (inner_rim_trail if field else inner_rim_walk)[level, part]
        else:
            known = (inner_trail if field else inner_walk)[level, x + S, part]
        after = turn(jnp.where(from_above, known, values), -1, 0)
        return after + turn(jnp.where(from_below, known, values), 1, 0)

    march(load, vertical, planes, TILE, walk, trail, weight, left, shifts, rim_shifts, emit, lambda *_: None)


def first_cap_kernel(
    parity, direction, residual, diagonal, low, high, rims, first, images, shifts, rim_shifts, inner_walk, inner_trail, inner_rim_walk, inner_rim_trail, cap_out, images_out, walk, trail, weight, left
):
    planes, rows, _ = direction.shape
    half = 2 * TILE
    upper = lax.broadcasted_iota(jnp.int32, (RECYCLED, half, LANES), 1) < TILE
    for x in range(planes):
        chosen = jnp.where(upper, images[:, x, :half], images[:, x, rows - half :])
        images_out[x] = chosen.reshape(RECYCLED * half, LANES)

    def emit(index, x, values):
        cap_out[index, x] = values

    cap_steps(
        parity[0] & 1 == 0, lambda tile: first[tile], (direction, residual, diagonal), low, high, rims, shifts, rim_shifts, inner_walk, inner_trail, inner_rim_walk, inner_rim_trail, walk, trail, weight, left, emit
    )


def caps_kernel(
    parity, direction, residual, diagonal, low, high, rims, second, cap, images, shifts, rim_shifts, groups, sums_in, total_in, inner_walk, inner_trail, inner_rim_walk, inner_rim_trail, caps_out, parts_out, walk, trail, weight, left
):
    planes, rows, _ = direction.shape
    fields = (direction, residual, diagonal)
    row = rows_of(TILE)
    near = row < S
    odd = parity[0] & 1
    ours = near == (jnp.zeros((TILE, LANES), jnp.int32) + odd == 0)

    def emit(index, x, values):
        caps_out[index, x] = jnp.where(ours, values, cap[index, x])

    cap_steps(
        odd == 1, lambda tile: second[tile], fields, low, high, rims, shifts, rim_shifts, inner_walk, inner_trail, inner_rim_walk, inner_rim_trail, walk, trail, weight, left, emit
    )

    def tile_of(index, x):
        if index in (0, S + 1):
            values = fields[index > 0][x]
            return jnp.where(near, values[:TILE], values[rows - TILE :])
        return caps_out[index - 1 if index <= S else index - 2, x]

    families = products()
    sums = {}
    half = 2 * TILE
    total = total_in[...]
    for x in range(0, planes, 2):
        rounded = []
        against = []
        for k in range(2):
            values = [tile_of(index, x + k) for index in range(BASIS)]
            for family in families:
                for i, j in family:
                    product = values[i] * values[j]
                    sums[i, j] = sums[i, j] + product if (i, j) in sums else product
            pieces = [
                piece for value in values for piece in (jnp.where(near, value, 0.0), jnp.where(near, 0.0, value))
            ]
            rounded.append(jnp.concatenate(pieces, axis=0).astype(jnp.bfloat16))
            against.append(images[x + k])
        total = total + lax.dot_general(
            jnp.concatenate(rounded, axis=1),
            jnp.concatenate(against, axis=1),
            (((1,), (1,)), ((), ())),
            preferred_element_type=jnp.float32,
        )
    spot = lanes_of(TILE)
    columns = [list(families[0][:TILE]), list(families[1]) + [families[0][TILE]], list(families[2])]
    order = {pair: index for index, pair in enumerate(sorted(sums))}
    scalars = jnp.zeros((TILE, LANES), jnp.float32)
    for place, column in enumerate(columns):
        values = jnp.zeros((TILE, LANES), jnp.float32)
        for index, pair in enumerate(column):
            whole = sums[pair] + sums_in[order[pair]]
            values = jnp.where(row == index, jnp.sum(whole, axis=0, keepdims=True), values)
        values = jnp.sum(values, axis=1, keepdims=True)
        scalars = jnp.where((spot // TILE == row) & (spot % TILE == place + 1), values, scalars)
    wide = (BASIS * half, RECYCLED * half)
    same = lax.broadcasted_iota(jnp.int32, wide, 0) % half == lax.broadcasted_iota(jnp.int32, wide, 1) % half
    total = jnp.where(same, total, 0.0).reshape(BASIS, 2, TILE, RECYCLED * half)
    total = (total[:, 0] + total[:, 1]).reshape(BASIS * TILE, RECYCLED * half)
    lines = jnp.dot(jnp.concatenate(split(total, 3), axis=1), groups[...], preferred_element_type=jnp.float32)
    mixed = jnp.zeros((TILE, LANES), jnp.float32)
    for index in range(TILE):
        mixed = jnp.where(spot % TILE == index, lines[TILE * index : TILE * (index + 1)], mixed)
    extra = jnp.where(spot % TILE == 0, lines[TILE * TILE :], scalars)
    table = jnp.concatenate(
        [jnp.sum(mixed, axis=0, keepdims=True), jnp.sum(extra, axis=0, keepdims=True)], axis=0
    )
    table = jnp.concatenate([table] * (TILE // 2), axis=0)
    for start in range(0, parts_out.shape[0], TILE):
        parts_out[start : start + TILE] = table


def moments_of(values):
    first = values[:2]
    return first + [2.0 * value - first[index % 2] for index, value in enumerate(values[2:])]


def finish_kernel(
    parts, coupling, direction, residual, basis, caps, recycled, delta_out, residual_out, direction_out
):
    pieces = [parts[start : start + TILE] for start in range(0, parts.shape[0], TILE)]
    while len(pieces) > 1:
        pieces = [a + b for a, b in zip(pieces[::2], pieces[1::2])] + pieces[len(pieces) // 2 * 2 :]
    table = pieces[0]
    for shift in (4, 2):
        table = table + turn(table, shift, 0)
    spot = lanes_of(TILE)
    row = rows_of(TILE)
    mixed = jnp.broadcast_to(table[:1], (TILE, LANES))
    extra = jnp.broadcast_to(table[1:2], (TILE, LANES))
    columns = []
    for place in range(3):
        mine = (spot // TILE == row) & (spot % TILE == place + 1)
        column = jnp.sum(jnp.where(mine, extra, 0.0), axis=1, keepdims=True)
        columns.append(jnp.broadcast_to(column, (TILE, LANES)))

    def spread(column, index):
        return jnp.broadcast_to(columns[column][index : index + 1], (TILE, LANES))

    walk = moments_of([spread(0, index) for index in range(TILE)] + [spread(1, TILE - 1)])
    trail = moments_of([spread(1, index) for index in range(2 * S - 1)])
    cross = moments_of([spread(2, index) for index in range(2 * S)])
    gram = {}
    for i in range(BASIS):
        for j in range(i, BASIS):
            source = walk if j <= S else (cross if i <= S else trail)
            one = i if i <= S else i - S - 1
            two = j if j <= S else j - S - 1
            gram[i, j] = gram[j, i] = 0.5 * (source[one + two] + source[abs(one - two)])

    def dot(one, other):
        terms = [one[i] * other[i] for i in one if i in other]
        while len(terms) > 1:
            terms = [a + b for a, b in zip(terms[::2], terms[1::2])] + terms[len(terms) // 2 * 2 :]
        return terms[0]

    def applied(values):
        return {i: dot({j: gram[i, j] for j in values}, values) for i in range(BASIS)}

    def mapped_by(values):
        found = {}
        for j, value in values.items():
            first, length = (0, S + 1) if j <= S else (S + 1, S)
            k = j - first
            if k == 0:
                entries = ((j, center), (j + 1, half_width))
            elif k < length - 1:
                entries = ((j - 1, half_width / 2), (j, center), (j + 1, half_width / 2))
            else:
                entries = ()
            for i, factor in entries:
                found[i] = found[i] + factor * value if i in found else factor * value
        return found

    def plus(one, factor, other):
        found = dict(one)
        for i, value in other.items():
            found[i] = found[i] + factor * value if i in found else factor * value
        return found

    unit = jnp.ones((TILE, LANES), jnp.float32)
    residue = {S + 1: unit}
    search = {0: unit}
    update = {}
    norm_now = dot(residue, applied(residue))
    for _ in range(S):
        mapped = mapped_by(search)
        step_size = norm_now / dot(search, applied(mapped))
        update = plus(update, step_size, search)
        residue = plus(residue, -step_size, mapped)
        norm_next = dot(residue, applied(residue))
        search = plus(residue, norm_next / norm_now, search)
        norm_now = norm_next
    across = residue[0]
    for index in range(1, TILE):
        across = jnp.where(spot % TILE == index, residue[index], across)
    projected = mixed * across + jnp.where(spot % TILE == 0, extra * residue[BASIS - 1], 0.0)
    projected = projected[:1]
    weights = jnp.sum(coupling[...] * projected, axis=1, keepdims=True)
    weights = jnp.broadcast_to(weights.astype(jnp.bfloat16).astype(jnp.float32), (RECYCLED, 2 * LANES))
    wide = (2 * TILE, 2 * TILE * RECYCLED)
    index = lax.broadcasted_iota(jnp.int32, wide, 0)
    slot = lax.broadcasted_iota(jnp.int32, wide, 1)
    spread_weights = jnp.sum(jnp.where(slot // (2 * TILE) == index, weights, 0.0), axis=0, keepdims=True)
    mixing = jnp.where(slot % (2 * TILE) == index, spread_weights, 0.0).astype(jnp.bfloat16)
    planes, rows, _ = direction.shape
    near = row < S
    for plane in range(planes):
        for start in range(0, rows, 2 * TILE):
            part = slice(start, start + 2 * TILE)
            found = [0.0, 0.0, 0.0]
            for field in range(BASIS):
                if field in (0, S + 1):
                    values = (residual if field else direction)[plane, part]
                else:
                    at = field - 1 if field <= S else field - 2
                    pieces = [basis[at, plane, start : start + TILE], basis[at, plane, start + TILE : start + 2 * TILE]]
                    if start == 0:
                        pieces[0] = jnp.where(near, caps[at, plane], pieces[0])
                    if start + 2 * TILE == rows:
                        pieces[1] = jnp.where(near, pieces[1], caps[at, plane])
                    values = jnp.concatenate(pieces, axis=0)
                for index, coefficients in enumerate((update, residue, search)):
                    if field in coefficients:
                        factor = jnp.concatenate([coefficients[field]] * 2, axis=0)
                        found[index] = found[index] + factor * values
            vectors = recycled[:, plane, part].reshape(RECYCLED * 2 * TILE, LANES)
            correction = jnp.dot(mixing, vectors, preferred_element_type=jnp.float32)
            delta_out[plane, part] = found[0]
            residual_out[plane, part] = found[1]
            direction_out[plane, part] = found[2] - correction


def onward(step):
    return lambda index, count: (index + step) % count


def inward(index, count):
    return index ^ 1


def outward(index, count):
    return (index - 1 + 2 * (index % 2)) % count


def moved(values, moves):
    axes = tuple(moves)
    pairs = [(0, 0)]
    for axis in axes:
        count = lax.axis_size(axis)
        pairs = [
            (source * count + i, target * count + moves[axis](i, count)) for source, target in pairs for i in range(count)
        ]
    return lax.ppermute(values, axes, pairs)


def call(kernel, out_shape, operands, scratch=(), limit=16, in_hbm=()):
    in_vmem = pl.BlockSpec(memory_space=pltpu.VMEM)
    in_smem = pl.BlockSpec(memory_space=pltpu.SMEM)
    in_place = pl.BlockSpec(memory_space=pltpu.HBM)
    in_hbm = [pltpu.with_memory_space_constraint(operand, pltpu.HBM) for operand in in_hbm]
    out_shape = [shape if isinstance(shape, jax.ShapeDtypeStruct) else jax.ShapeDtypeStruct(shape, jnp.float32) for shape in out_shape]
    return pl.pallas_call(
        kernel,
        out_shape=tuple(out_shape),
        in_specs=[in_smem if operand.dtype == jnp.int32 else in_vmem for operand in operands] + [in_place] * len(in_hbm),
        out_specs=(in_vmem,) * len(out_shape),
        scratch_shapes=list(scratch),
        compiler_params=pltpu.CompilerParams(vmem_limit_bytes=limit * 1024 * 1024),
    )(*operands, *in_hbm)


def body(residual, direction, diagonal, recycled, recycled_images, coupling_inverse):
    planes, rows, columns = residual.shape
    if columns != LANES or rows != 4 * TILE or RIM * (planes + 2 * S) != LANES or lax.axis_size("gx") % 2 or lax.axis_size("gy") % 2:
        raise ValueError("unsupported block")
    shape = residual.shape
    shifts, rim_shifts, groups = shift_matrices()
    slab = (3 * S - 2, rows, LANES)
    *fields, upper, lower, coupling = call(
        load_kernel,
        [shape] * 3 + [slab] * 2 + [coupling_inverse.shape],
        (),
        [pltpu.SemaphoreType.DMA((4,))],
        in_hbm=(direction, residual, diagonal, coupling_inverse),
    )
    parity = ((lax.axis_index("gy") & 1) + 2 * (lax.axis_index("gx") & 1)).astype(jnp.int32).reshape(1)
    low = moved(upper, {"gx": onward(1)})
    high = moved(lower, {"gx": onward(-1)})
    rim, rim_outward, rim_inward, coupling = call(
        rim_kernel, [(3, rows, LANES), (rows, LANES), (rows, LANES), (RECYCLED, LANES)], (parity, *fields, coupling)
    )
    sides = [onward(-1)] if lax.axis_size("gz") == 2 else [onward(-1), onward(1)]
    outward_rims = [moved(rim_outward, {"gx": outward, "gz": side}) for side in sides]
    rims = [moved(rim, {"gz": side}) for side in sides]
    inward_rims = [moved(rim_inward, {"gx": inward, "gz": side}) for side in sides]
    tiles = len(packing(planes))
    first, second, whole_rims = call(
        edge_kernel,
        [(tiles, TILE, LANES), (tiles, TILE, LANES), (3, rows, LANES)],
        (parity, *fields, low, high, rims[0], rims[-1], outward_rims[0], outward_rims[-1])
        + (inward_rims[0], inward_rims[-1]),
    )
    second = moved(second, {"gy": outward})
    first = moved(first, {"gy": inward})
    devices = lax.axis_size(AXES)
    wide = planes + 2 * S
    worked = 2 * planes + 2 * (S - 1) + 2 * (S - 2)

    def weights_and_left(ring):
        return [pltpu.VMEM((wide, ring, LANES), jnp.float32), pltpu.VMEM((worked * ring, 4 * LANES), jnp.bfloat16)]

    count = sum(len(family) for family in products())
    block = 2 * TILE
    basis, sums, total, *levels, images = call(
        inner_kernel,
        [
            (BASIS - 2, *shape),
            (count, TILE, LANES),
            (BASIS * block, RECYCLED * block),
            (S, wide, rows, LANES),
            (S - 1, wide, rows, LANES),
            (S, rows, LANES),
            (S - 1, rows, LANES),
            jax.ShapeDtypeStruct(recycled_images.shape, recycled_images.dtype),
        ],
        (*fields, low, high, whole_rims, shifts, rim_shifts),
        weights_and_left(rows) + [pltpu.SemaphoreType.DMA],
        in_hbm=(recycled_images,),
    )
    tall = [pltpu.VMEM((S, wide, TILE, LANES), jnp.float32), pltpu.VMEM((S - 1, wide, TILE, LANES), jnp.float32)]
    cap_shape = (BASIS - 2, planes, TILE, LANES)
    cap, chosen = call(
        first_cap_kernel,
        [cap_shape, jax.ShapeDtypeStruct((planes, RECYCLED * block, LANES), images.dtype)],
        (parity, *fields, low, high, whole_rims, first, images, shifts, rim_shifts, *levels),
        tall + weights_and_left(TILE),
    )
    caps, parts = call(
        caps_kernel,
        [cap_shape, (2 * devices, LANES)],
        (parity, *fields, low, high, whole_rims, second, cap, chosen)
        + (shifts, rim_shifts, groups, sums, total, *levels),
        tall + weights_and_left(TILE),
    )
    parts = lax.all_to_all(parts, AXES, 0, 0, tiled=True)
    return call(finish_kernel, [shape] * 3, (parts, coupling, fields[0], fields[1], basis, caps, recycled))


def solution(mesh):
    in_specs = (
        P("gx", "gy", "gz"),
        P("gx", "gy", "gz"),
        P("gx", "gy", "gz"),
        P(None, "gx", "gy", "gz"),
        P(None, "gx", "gy", "gz"),
        P(),
    )
    out_specs = (P("gx", "gy", "gz"), P("gx", "gy", "gz"), P("gx", "gy", "gz"))
    return jax.shard_map(body, mesh=mesh, in_specs=in_specs, out_specs=out_specs, check_vma=False)
```
